32 devices in a mesh: tm: 8 (over z, y), space: 4 (over x, core).
Axes of the slice: x: 2, y: 2, z: 4, core: 2. Of those that a mesh axis runs over, the one named last changes fastest.
Arguments:
- starts: float32 [8, 5, 16, 64, 128], P('tm', None, 'space'), may hold values from -4 to 4
- source: float32 [5, 16, 64, 128], P(None, 'space'), may hold values from -4 to 4
Outputs:
- ends: float32 [8, 5, 16, 64, 128], P('tm', None, 'space')
- slice_norms: float32 [8], P('tm')
- total_norm: float32 [1], replicated
The draws below stay inside these ranges and needn't reach their ends.
All inputs are finite; a program needn't handle non-finite values.
Results may differ from the reference program's by a relative error of at most 0.0003.
Values sent between devices are 32-bit elements; how exact they have to be, the bound alone decides.
A program may use at most 64 MiB of HBM per device.

```python
import math
import jax
import jax.numpy as jnp
from jax import lax

FIELDS = 5
NX = 128
NY = 64
STEPS = 1
NZ = 16
SLICES = 8


def block_levels(rng, dims, cuts, least, top_value):
    gain, own = 1.0, jax.random.fold_in(rng, 6)
    for position, parts in cuts:
        draws = jnp.exp(jax.random.uniform(jax.random.fold_in(own, position), (parts,), jnp.float32, least / len(cuts), top_value / len(cuts)))
        gain = gain * jnp.repeat(draws, dims[position] // parts).reshape([-1 if axis == position else 1 for axis in range(len(dims))])
    return gain


def normal_values(stream_key, extent, deviation, reach, split=(), kind=jnp.bfloat16):
    entries = jax.random.normal(stream_key, extent, jnp.float32) * deviation
    if len(split) > 0:
        entries = block_levels(stream_key, extent, split, -0.22, 0.18) * entries
    return jnp.clip(entries, min=-reach, max=reach).astype(kind)


def setup_inputs(seed: int = 0) -> dict:
    key_of = jax.random.split(jax.random.key(seed), 3)
    return {
        "starts": normal_values(key_of[0], (SLICES, FIELDS, NZ, NY, NX), 0.3, 4.0, ((0, 8), (2, 4)), jnp.float32),
        "source": normal_values(key_of[1], (FIELDS, NZ, NY, NX), 0.3, 4.0, ((1, 4),), jnp.float32),
    }


viscosity = 0.08
diffusivity = 0.05
compress_rate = 0.25
time_step = 0.5
diffusion_number = 0.08
advect_xaxis = 0.2
advect_yaxis = 0.15
advect_zaxis = 0.1
epsilon = 1e-06

def central(values, axis):
    return 0.5 * (jnp.roll(values, -1, axis) - jnp.roll(values, 1, axis))

def laplace(values):
    summed = -6.0 * values
    for axis in (0, 1, 2):
        summed = summed + jnp.roll(values, -1, axis) + jnp.roll(values, 1, axis)
    return summed

def tendency(state_now, source):
    speed_xaxis = advect_xaxis + state_now[0]
    speed_yaxis = advect_yaxis + state_now[1]
    speed_zaxis = advect_zaxis + state_now[2]

    def transport(quantity):
        return central(speed_xaxis * quantity, 2) + central(speed_yaxis * quantity, 1) + central(speed_zaxis * quantity, 0)
    pressure = state_now[3]
    xmomentum = -transport(state_now[0]) - central(pressure, 2) + viscosity * laplace(state_now[0])
    ymomentum = -transport(state_now[1]) - central(pressure, 1) + viscosity * laplace(state_now[1])
    zmomentum = -transport(state_now[2]) - central(pressure, 0) + viscosity * laplace(state_now[2])
    pressure_rate = -compress_rate * (central(state_now[0], 2) + central(state_now[1], 1) + central(state_now[2], 0))
    scalar_rate = -transport(state_now[4]) + diffusivity * laplace(state_now[4])
    return jnp.stack([xmomentum, ymomentum, zmomentum, pressure_rate, scalar_rate]) + source

def fine_run(current, source):
    for repeat in range(STEPS):
        section_one = tendency(current, source)
        section_two = tendency(current + 0.5 * time_step * section_one, source)
        section_three = tendency(current + 0.5 * time_step * section_two, source)
        section_four = tendency(current + time_step * section_three, source)
        current = current + time_step / 6.0 * (section_one + 2.0 * section_two + 2.0 * section_three + section_four)
    return current

def signed_angle(length):
    cell_ids = jnp.arange(length, dtype=jnp.int32)
    signed = (cell_ids + length // 2) % length - length // 2
    return (signed, 2.0 * math.pi / length * signed.astype(jnp.float32))

def coarse_symbol():
    zsigned, zangles = signed_angle(NZ)
    ysigned, yangles = signed_angle(NY)
    xsigned, xangles = signed_angle(NX)
    keeper = ((jnp.abs(ysigned) < NY // 8)[:, None] & (jnp.abs(xsigned) < NX // 16)[None, :]).astype(jnp.float32)
    real_part = 1.0 + diffusion_number * ((2.0 * jnp.cos(zangles) - 2.0)[:, None, None] + (2.0 * jnp.cos(yangles) - 2.0)[None, :, None] + (2.0 * jnp.cos(xangles) - 2.0)[None, None, :])
    imag_part = -(advect_zaxis * jnp.sin(zangles)[:, None, None] + advect_yaxis * jnp.sin(yangles)[None, :, None] + advect_xaxis * jnp.sin(xangles)[None, None, :])
    return lax.complex(real_part * keeper[None], imag_part * keeper[None])

def coarse(values, symbol):
    spectrum = jnp.fft.fftn(values, axes=(1, 2, 3))
    return jnp.real(jnp.fft.ifftn(spectrum * symbol, axes=(1, 2, 3)))

def reference(starts, source):

    def run_slice(begin_state):
        return fine_run(begin_state, source)
    fine = lax.map(run_slice, starts)
    symbol = coarse_symbol()

    def advance(carried, inputs_pair):
        old_start, fine_end = inputs_pair
        end_state = fine_end + coarse(carried - old_start, symbol)
        jump_size = end_state - fine_end
        return (end_state, (end_state, jnp.sum(jump_size * jump_size)))
    unused, (ends, sums) = lax.scan(advance, starts[0], (starts, fine))
    cell_total = FIELDS * NZ * NY * NX
    slice_norms = jnp.sqrt(sums / cell_total + epsilon)
    total_norm = jnp.sqrt(jnp.sum(sums) / (cell_total * SLICES) + epsilon).reshape(1)
    return (ends, slice_norms, total_norm)
```

```python
import functools
import math

import jax
import jax.numpy as jnp
import numpy as np
from jax import lax
from jax.experimental import pallas as pl
from jax.experimental.pallas import tpu as pltpu
from jax.sharding import PartitionSpec as P

viscosity = 0.08
diffusivity = 0.05
compress_rate = 0.25
time_step = 0.5
diffusion_number = 0.08
advect_xaxis = 0.2
advect_yaxis = 0.15
advect_zaxis = 0.1
epsilon = 1e-06
MESH = pl.DeviceIdType.MESH
PAD = 8
CHUNK = 16
LANES = 128
VMEM_BYTES = 32 * 1024 * 1024


def tables(depth, rows, cols, spaces, steps):
    keep_y, keep_x = rows // 8, cols // 16
    slot = 2 * keep_x
    per = LANES // (slot * depth)
    full = depth * spaces
    k = np.arange(keep_x)
    x = np.arange(cols)
    ax = 2 * math.pi / cols * ((x[:, None] * k[None, :]) % cols)
    weight = np.where(k == 0, 1.0, 2.0) / (full * rows * cols)
    xf = np.zeros((2 * cols, LANES))
    xi = np.zeros((LANES, 2 * cols))
    for i in range(2):
        at = i * slot
        xf[i * cols : (i + 1) * cols, at : at + keep_x] = np.cos(ax)
        xf[i * cols : (i + 1) * cols, at + keep_x : at + slot] = -np.sin(ax)
        xi[at : at + keep_x, i * cols : (i + 1) * cols] = (np.cos(ax) * weight).T
        xi[at + keep_x : at + slot, i * cols : (i + 1) * cols] = (-np.sin(ax) * weight).T
    ky = np.arange(2 * keep_y)
    ky = np.where(ky < keep_y, ky, ky - 2 * keep_y)
    y = np.arange(rows)
    ay = 2 * math.pi / rows * ((ky[:, None] * y[None, :]) % rows)
    yf = np.concatenate([np.cos(ay), np.sin(ay)], axis=1)
    yi = np.concatenate([np.cos(ay).T, -np.sin(ay).T], axis=1)
    kz = np.arange(full)
    width = full * keep_x
    half = depth * slot
    zf = np.zeros((LANES, per * 2 * width))
    for fp in range(per):
        for z in range(depth):
            a = 2 * math.pi / full * ((kz * z) % full)
            for kk in range(keep_x):
                row = fp * half + z * slot + kk
                re = fp * 2 * width + kz * keep_x + kk
                im = re + width
                zf[row, re] = np.cos(a)
                zf[row, im] = -np.sin(a)
                zf[row + keep_x, re] = np.sin(a)
                zf[row + keep_x, im] = np.cos(a)
    zi = np.zeros((2 * width, full * slot))
    for z in range(full):
        a = 2 * math.pi / full * ((kz * z) % full)
        for kk in range(keep_x):
            re = kz * keep_x + kk
            im = re + width
            col = z * slot + kk
            zi[re, col] = np.cos(a)
            zi[im, col] = -np.sin(a)
            zi[re, col + keep_x] = np.sin(a)
            zi[im, col + keep_x] = np.cos(a)
    tz = 2 * math.pi / full * kz
    ty = 2 * math.pi / rows * ky
    tx = 2 * math.pi / cols * k
    live = (ky != -keep_y).astype(np.float64)[:, None, None]
    real = 1.0 + diffusion_number * (
        (2 * np.cos(ty) - 2)[:, None, None]
        + (2 * np.cos(tz) - 2)[None, :, None]
        + (2 * np.cos(tx) - 2)[None, None, :]
    )
    imag = -(
        advect_yaxis * np.sin(ty)[:, None, None]
        + advect_zaxis * np.sin(tz)[None, :, None]
        + advect_xaxis * np.sin(tx)[None, None, :]
    )
    symbol = (real + 1j * imag) * live
    powers = np.stack([symbol**p for p in range(1, max(steps, 2))])
    powers = np.stack([powers.real, powers.imag], axis=1).reshape(-1, 2, 2 * keep_y, width)
    return [xf, yf, zf, zi, yi, xi], powers.astype(np.float32)


def halves(table):
    high = table.astype(jnp.bfloat16)
    low = (table - high.astype(np.float64)).astype(jnp.bfloat16)
    return np.stack([high, low])


def split(values):
    high = values.astype(jnp.bfloat16)
    return high, (values - high.astype(jnp.float32)).astype(jnp.bfloat16)


def dot(a, b):
    return jnp.dot(a, b, preferred_element_type=jnp.float32)


def times(values, table):
    high, low = split(values)
    return dot(high, table[0]) + dot(low, table[0]) + dot(high, table[1])


def under(table, values):
    high, low = split(values)
    return dot(table[0], high) + dot(table[0], low) + dot(table[1], high)


def kernel(
    sizes, starts, source, xf_h, yf_h, zf_h, zi_h, yi_h, xi_h, sym_h,
    ends, norms,
    y1, y2, y3, y4, src, fine, halo, xf, yf, zf, zi, yi, xi, sym,
    own, jumps, ahead, mode_send, mode_recv, square_send, squares,
    load_sem, table_sem, halo_send, halo_recv, ahead_sems, jump_send, jump_recv,
    mode_ssem, mode_rsem, sq_send, sq_recv, relays,
):
    times_n, spaces, fields, depth, rows, cols = sizes
    keep_y, keep_x = rows // 8, cols // 16
    slot = 2 * keep_x
    ky = 2 * keep_y
    layers = fields * depth
    slots = LANES // slot
    groups = -(-layers // slots)
    per = LANES // (slot * depth)
    chunks = rows // CHUNK
    n = lax.axis_index("tm")
    s = lax.axis_index("space")
    me = n * spaces + s
    up = lax.rem(s + 1, spaces)
    down = lax.rem(s + spaces - 1, spaces)

    barrier = pltpu.get_barrier_semaphore()

    def near(distance, act):
        for side, target in enumerate((n - distance, n + distance)):
            pl.when((target >= 0) & (target < times_n))(functools.partial(act, side, target))

    def enter(target, where):
        pl.semaphore_signal(barrier, inc=1, device_id=(target, where), device_id_type=MESH)

    for offset in range(1, spaces):
        enter(n, lax.rem(s + offset, spaces))
    near(1, lambda side, target: enter(target, s))
    loads = [
        pltpu.make_async_copy(starts.at[0, :, 0], y1.at[:, 0, pl.ds(PAD, rows)], load_sem.at[0]),
        pltpu.make_async_copy(
            starts.at[0, :, depth - 1], y1.at[:, depth - 1, pl.ds(PAD, rows)], load_sem.at[4]
        ),
        pltpu.make_async_copy(
            starts.at[0, :, pl.ds(1, depth - 2)],
            y1.at[:, pl.ds(1, depth - 2), pl.ds(PAD, rows)],
            load_sem.at[5],
        ),
        pltpu.make_async_copy(
            starts.at[0, :, :, pl.ds(rows - PAD, PAD)], y1.at[:, :, pl.ds(0, PAD)], load_sem.at[1]
        ),
        pltpu.make_async_copy(
            starts.at[0, :, :, pl.ds(0, PAD)], y1.at[:, :, pl.ds(PAD + rows, PAD)], load_sem.at[2]
        ),
        pltpu.make_async_copy(source, src, load_sem.at[3]),
    ]
    for copy in loads:
        copy.start()
    fills = [
        pltpu.make_async_copy(a, b, table_sem.at[i])
        for i, (a, b) in enumerate(
            [(xf_h, xf), (yf_h, yf), (zf_h, zf), (zi_h, zi), (yi_h, yi), (xi_h, xi), (sym_h, sym)]
        )
    ]
    for copy in fills:
        copy.start()
    for copy in loads[:2]:
        copy.wait()
    beside = jnp.where(n > 0, 1, 0) + jnp.where(n < times_n - 1, 1, 0)
    pl.semaphore_wait(barrier, spaces - 1 + beside)

    def relay(level):
        near(
            2**level,
            lambda side, target: pl.semaphore_signal(
                relays.at[level, side], inc=1, device_id=(target, s), device_id_type=MESH
            ),
        )

    def heard(level):
        near(2**level, lambda side, target: pl.semaphore_wait(relays.at[level, 1 - side], 1))

    levels = (times_n - 1).bit_length()

    states = [y1, y2, y3, y4]

    def halo_copy(stage, side, chunk):
        r0 = pl.multiple_of(chunk * CHUNK, CHUNK)
        state = states[stage]
        layer = depth - 1 if side == 0 else 0
        return pltpu.make_async_remote_copy(
            src_ref=state.at[:, layer, pl.ds(pl.multiple_of(PAD + r0, 8), CHUNK)],
            dst_ref=halo.at[stage, side, :, pl.ds(r0, CHUNK)],
            send_sem=halo_send.at[stage, side, chunk],
            recv_sem=halo_recv.at[stage, side, chunk],
            device_id=(n, up if side == 0 else down),
            device_id_type=MESH,
        )

    def send_first(c, carry):
        for side in range(2):
            halo_copy(0, side, c).start()
        return carry

    lax.fori_loop(0, chunks, send_first, 0)
    relay(0)

    lane = lax.broadcasted_iota(jnp.int32, (1, LANES), 1)
    first = lax.rem(lane, slot) < keep_x

    def swapped(values):
        return jnp.where(
            first, pltpu.roll(values, LANES - keep_x, 1), -pltpu.roll(values, keep_x, 1)
        )

    def transform(layer_of):
        pairs = jnp.concatenate(
            [
                jnp.concatenate([layer_of(2 * p), layer_of(2 * p + 1)], axis=1)
                for p in range(layers // 2)
            ],
            axis=0,
        )
        packed = times(pairs, xf)
        result = []
        for g in range(groups):
            total = None
            for p in range(slots // 2):
                index = g * (slots // 2) + p
                if index < layers // 2:
                    piece = packed[index * rows : (index + 1) * rows]
                    if p > 0:
                        piece = pltpu.roll(piece, 2 * p * slot, 1)
                    total = piece if total is None else total + piece
            result.append(total)
        both = [jnp.concatenate([t, swapped(t)], axis=0) for t in result]
        spec = under(yf, jnp.concatenate(both, axis=1))
        return jnp.concatenate([spec[:, g * LANES : (g + 1) * LANES] for g in range(groups)], axis=0)

    for copy in loads[2:] + fills:
        copy.wait()

    own[...] = transform(lambda l: y1[l // depth, l % depth, pl.ds(PAD, rows)])
    ahead_copy = pltpu.make_async_remote_copy(
        src_ref=own,
        dst_ref=ahead,
        send_sem=ahead_sems.at[0],
        recv_sem=ahead_sems.at[1],
        device_id=(jnp.maximum(n - 1, 0), s),
        device_id_type=MESH,
    )

    @pl.when(n > 0)
    def _():
        ahead_copy.start()

    def update(stage, z, r0, below, above):
        state = states[stage]
        mid, xm, xp, ym, yp = [], [], [], [], []
        rolled = CHUNK + 2 * PAD
        for f in range(fields):
            wide = state[f, z, pl.ds(r0, rolled)]
            centre = wide[PAD : PAD + CHUNK]
            mid.append(centre)
            ym.append(pltpu.roll(wide, 1, 0)[PAD : PAD + CHUNK])
            yp.append(pltpu.roll(wide, rolled - 1, 0)[PAD : PAD + CHUNK])
            xm.append(pltpu.roll(centre, 1, 1))
            xp.append(pltpu.roll(centre, cols - 1, 1))
        zm = [below(f) for f in range(fields)]
        zp = [above(f) for f in range(fields)]
        sides = [xm, xp, ym, yp, zm, zp]
        factors = []
        for axis, speed in enumerate((advect_xaxis, advect_yaxis, advect_zaxis)):
            factors.append((viscosity + 0.5 * speed) + 0.5 * sides[2 * axis][axis])
            factors.append((viscosity - 0.5 * speed) - 0.5 * sides[2 * axis + 1][axis])
        shift = viscosity - diffusivity
        rates = []
        for f in range(fields):
            forcing = src[f, z, pl.ds(r0, CHUNK)]
            if f == 3:
                total = (
                    (xp[0] - xm[0]) + (yp[1] - ym[1]) + (zp[2] - zm[2])
                ) * (-0.5 * compress_rate)
            else:
                gain = viscosity if f < 3 else diffusivity
                total = (-6.0 * gain) * mid[f]
                for factor, side in zip(factors, sides):
                    total = total + (factor if f < 3 else factor - shift) * side[f]
                if f < 3:
                    total = total + 0.5 * (sides[2 * f][3] - sides[2 * f + 1][3])
            rates.append(total + forcing)
        share = time_step / 6.0 * (1.0, 2.0, 2.0, 1.0)[stage]
        for f in range(fields):
            at = f * depth + z
            here = pl.ds(r0, CHUNK)
            begin = y1[f, z, pl.ds(pl.multiple_of(r0 + PAD, 8), CHUNK)]
            done = begin if stage == 0 else fine[at, here]
            fine[at, here] = done + share * rates[f]
            if stage < 3:
                later = states[stage + 1]
                step = (0.5, 0.5, 1.0)[stage] * time_step
                value = begin + step * rates[f]
                later[f, z, pl.ds(pl.multiple_of(r0 + PAD, 8), CHUNK)] = value

                @pl.when(r0 == 0)
                def _():
                    later[f, z, pl.ds(PAD + rows, PAD)] = value[:PAD]

                @pl.when(r0 == rows - CHUNK)
                def _():
                    later[f, z, pl.ds(0, PAD)] = value[CHUNK - PAD :]

    for stage in range(4):
        state = states[stage]

        def inner(i, carry):
            z = 1 + i // chunks
            r0 = pl.multiple_of(lax.rem(i, chunks) * CHUNK, CHUNK)
            at = pl.ds(pl.multiple_of(r0 + PAD, 8), CHUNK)
            update(stage, z, r0, lambda f: state[f, z - 1, at], lambda f: state[f, z + 1, at])
            return carry

        def edge(c, carry):
            r0 = pl.multiple_of(c * CHUNK, CHUNK)
            at = pl.ds(pl.multiple_of(r0 + PAD, 8), CHUNK)
            for side in range(2):
                halo_copy(stage, side, c).wait_recv()
                here = lambda f: halo[stage, side, f, pl.ds(r0, CHUNK)]
                if side == 0:
                    update(stage, 0, r0, here, lambda f: state[f, 1, at])
                else:
                    update(stage, depth - 1, r0, lambda f: state[f, depth - 2, at], here)
                if stage < 3:
                    halo_copy(stage + 1, 1 - side, c).start()
            return carry

        lax.fori_loop(0, (depth - 2) * chunks, inner, 0)
        lax.fori_loop(0, chunks, edge, 0)
        for level in range(levels):
            if min(level, 2) == stage:
                heard(level)
                if level + 1 < levels:
                    relay(level + 1)

    spec = transform(lambda l: fine[l])

    @pl.when(n < times_n - 1)
    def _():
        ahead_copy.wait_recv()
        jumps[n] = spec - ahead[...]

    def jump_copy(slot_id, sem_id, target):
        return pltpu.make_async_remote_copy(
            src_ref=jumps.at[slot_id],
            dst_ref=jumps.at[slot_id],
            send_sem=jump_send.at[sem_id],
            recv_sem=jump_recv.at[slot_id],
            device_id=(target, s),
            device_id_type=MESH,
        )

    def send_jump(i, carry):
        target = times_n - 1 - i
        jump_copy(n, target, target).start()
        return carry

    lax.fori_loop(0, times_n - 1 - n, send_jump, 0)

    width = depth * spaces * keep_x

    def collect(i, carry):
        m = n - 1 - i
        jump_copy(m, m, n).wait_recv()
        fresh = times(jumps[m], zf)
        gain_re = jnp.concatenate([sym[i, 0]] * groups, axis=0)
        gain_im = jnp.concatenate([sym[i, 1]] * groups, axis=0)
        result = []
        for p in range(per):
            re = fresh[:, 2 * p * width : (2 * p + 1) * width]
            im = fresh[:, (2 * p + 1) * width : (2 * p + 2) * width]
            result.append(carry[2 * p] + (gain_re * re - gain_im * im))
            result.append(carry[2 * p + 1] + (gain_re * im + gain_im * re))
        return tuple(result)

    zero = jnp.zeros((groups * ky, width), jnp.float32)
    carry = lax.fori_loop(0, n, collect, (zero,) * (2 * per))
    stacked = jnp.concatenate(
        [jnp.concatenate([carry[2 * p], carry[2 * p + 1]], axis=1) for p in range(per)], axis=0
    )
    back = times(stacked, zi)
    half = depth * slot
    height = groups * ky

    def piece(offset):
        total = None
        at = offset * half
        tile, inside = at // LANES * LANES, at % LANES
        part = lax.broadcasted_iota(jnp.int32, (1, LANES), 1) // half
        for p in range(per):
            block = back[p * height : (p + 1) * height, tile : tile + LANES]
            move = (p * half - inside) % LANES
            if move:
                block = pltpu.roll(block, move, 1)
            total = block if total is None else jnp.where(part == p, block, total)
        return total

    def mode_copy(offset):
        return pltpu.make_async_remote_copy(
            src_ref=mode_send.at[offset - 1],
            dst_ref=mode_recv.at[offset - 1],
            send_sem=mode_ssem.at[offset - 1],
            recv_sem=mode_rsem.at[offset - 1],
            device_id=(n, lax.rem(s + offset, spaces)),
            device_id_type=MESH,
        )

    for offset in range(1, spaces):
        mode_send[offset - 1] = piece(offset)
        mode_copy(offset).start()
    modes = piece(0)
    for offset in range(1, spaces):
        mode_copy(offset).wait_recv()
        modes = modes + mode_recv[offset - 1]

    weight = jnp.where(lax.rem(lane, keep_x) == 0, 1.0, 2.0)
    scaled = modes * (1.0 / (depth * spaces * rows * cols))
    square = jnp.sum(
        jnp.sum(scaled * scaled * weight, axis=0, keepdims=True), axis=1, keepdims=True
    ) * float(rows * cols)
    square_send[...] = jnp.broadcast_to(square, (1, LANES))
    squares[me] = jnp.broadcast_to(square, (1, LANES))

    def square_copy(index, sem_id, target):
        return pltpu.make_async_remote_copy(
            src_ref=square_send,
            dst_ref=squares.at[index],
            send_sem=sq_send.at[sem_id],
            recv_sem=sq_recv.at[index],
            device_id=target,
            device_id_type=MESH,
        )

    def others(act):
        def body(dt, carry):
            t = n - dt
            t = jnp.where(t < 0, t + times_n, t)
            for ds in range(spaces):
                where = s + ds
                where = jnp.where(where >= spaces, where - spaces, where)
                run = functools.partial(act, dt * spaces + ds, t, where)
                if ds == 0:
                    pl.when(dt > 0)(run)
                else:
                    run()
            return carry

        if times_n <= 8:
            for dt in range(times_n):
                body(dt, 0)
        else:
            lax.fori_loop(0, times_n, body, 0)

    others(lambda k, t, where: square_copy(me, k, (t, where)).start())

    both = [
        jnp.concatenate([t, swapped(t)], axis=0)
        for t in (modes[g * ky : (g + 1) * ky] for g in range(groups))
    ]
    planes = under(yi, jnp.concatenate(both, axis=1))
    for g in range(groups):
        plane = planes[:, g * LANES : (g + 1) * LANES]
        count = min(slots, layers - g * slots) // 2
        shifted = [
            plane if p == 0 else pltpu.roll(plane, LANES - 2 * p * slot, 1) for p in range(count)
        ]
        fix = times(jnp.concatenate(shifted, axis=0), xi)
        for p in range(count):
            for i in range(2):
                l = g * slots + 2 * p + i
                ends[l] = fine[l] + fix[p * rows : (p + 1) * rows, i * cols : (i + 1) * cols]

    others(
        lambda k, t, where: square_copy(t * spaces + where, k, (t, where)).wait_recv()
    )
    cells = fields * depth * spaces * rows * cols
    mine = jnp.sum(squares[pl.ds(n * spaces, spaces)], axis=0)
    every = jnp.sum(squares[...], axis=0)
    norms[0] = jnp.sqrt(mine * (1.0 / cells) + epsilon)
    norms[1] = jnp.sqrt(every * (1.0 / (cells * times_n)) + epsilon)

    others(lambda k, t, where: square_copy(me, k, (t, where)).wait_send())

    def drain_jump(i, carry):
        target = times_n - 1 - i
        jump_copy(n, target, target).wait_send()
        return carry

    lax.fori_loop(0, times_n - 1 - n, drain_jump, 0)

    @pl.when(n > 0)
    def _():
        ahead_copy.wait_send()

    for stage in range(4):

        def drain_halo(c, carry):
            for side in range(2):
                halo_copy(stage, side, c).wait_send()
            return carry

        lax.fori_loop(0, chunks, drain_halo, 0)
    for offset in range(1, spaces):
        mode_copy(offset).wait_send()


def finish(ends, norms, out, slice_out, total_out, slice_held, total_held, sems):
    copies = [pltpu.make_async_copy(ends, out, sems.at[0])]
    copies[0].start()
    for i, (held, to) in enumerate(((slice_held, slice_out), (total_held, total_out))):
        held[0] = norms[i, 0, 0]
        copies.append(pltpu.make_async_copy(held, to, sems.at[1 + i]))
        copies[-1].start()
    for copy in copies:
        copy.wait()


def solution(mesh):
    times_n, spaces = mesh.shape["tm"], mesh.shape["space"]

    def step(starts, source):
        _, fields, depth, rows, cols = starts.shape
        keep_y, keep_x = rows // 8, cols // 16
        matrices, symbol = tables(depth, rows, cols, spaces, times_n)
        constants = [halves(t) for t in matrices] + [symbol]
        operands = [starts, source] + [jnp.asarray(c) for c in constants]
        ky, slot = 2 * keep_y, 2 * keep_x
        groups = -(-fields * depth // (LANES // slot))
        height = groups * ky
        chunks = rows // CHUNK
        devices = times_n * spaces
        state = pltpu.VMEM((fields, depth, rows + 2 * PAD, cols), jnp.float32)
        dma = pltpu.SemaphoreType.DMA
        layer_shape = (fields * depth, rows, cols)
        ends, norms = pl.pallas_call(
            functools.partial(kernel, (times_n, spaces, fields, depth, rows, cols)),
            out_shape=(
                pltpu.VMEM(layer_shape, jnp.float32),
                pltpu.VMEM((2, 1, LANES), jnp.float32),
            ),
            in_specs=[pl.BlockSpec(memory_space=pltpu.HBM)] * (2 + len(constants)),
            out_specs=(
                pl.BlockSpec(memory_space=pltpu.VMEM),
                pl.BlockSpec(memory_space=pltpu.VMEM),
            ),
            scratch_shapes=[
                state, state, state, state,
                pltpu.VMEM((fields, depth, rows, cols), jnp.float32),
                pltpu.VMEM(layer_shape, jnp.float32),
                pltpu.VMEM((4, 2, fields, rows, cols), jnp.float32),
                *[pltpu.VMEM(c.shape, c.dtype) for c in constants],
                pltpu.VMEM((height, LANES), jnp.float32),
                pltpu.VMEM((times_n, height, LANES), jnp.float32),
                pltpu.VMEM((height, LANES), jnp.float32),
                pltpu.VMEM((spaces - 1, height, LANES), jnp.float32),
                pltpu.VMEM((spaces - 1, height, LANES), jnp.float32),
                pltpu.VMEM((1, LANES), jnp.float32),
                pltpu.VMEM((devices, 1, LANES), jnp.float32),
                dma((6,)), dma((len(constants),)),
                dma((4, 2, chunks)), dma((4, 2, chunks)), dma((2,)),
                dma((times_n,)), dma((times_n,)),
                dma((spaces - 1,)), dma((spaces - 1,)),
                dma((devices,)), dma((devices,)),
                pltpu.SemaphoreType.REGULAR(((times_n - 1).bit_length(), 2)),
            ],
            compiler_params=pltpu.CompilerParams(
                collective_id=0, has_side_effects=True, vmem_limit_bytes=VMEM_BYTES
            ),
        )(*[pltpu.with_memory_space_constraint(a, pltpu.HBM) for a in operands])
        out, slice_norm, total_norm = pl.pallas_call(
            finish,
            out_shape=(
                jax.ShapeDtypeStruct(layer_shape, jnp.float32),
                jax.ShapeDtypeStruct((1,), jnp.float32),
                jax.ShapeDtypeStruct((1,), jnp.float32),
            ),
            in_specs=[pl.BlockSpec(memory_space=pltpu.VMEM)] * 2,
            out_specs=[pl.BlockSpec(memory_space=pltpu.HBM)] * 3,
            scratch_shapes=[
                pltpu.SMEM((1,), jnp.float32), pltpu.SMEM((1,), jnp.float32), dma((3,)),
            ],
            compiler_params=pltpu.CompilerParams(vmem_limit_bytes=VMEM_BYTES // 2),
        )(
            pltpu.with_memory_space_constraint(ends, pltpu.VMEM),
            pltpu.with_memory_space_constraint(norms, pltpu.VMEM),
        )
        return out.reshape(starts.shape), slice_norm, total_norm

    return jax.shard_map(
        step,
        mesh=mesh,
        in_specs=(P("tm", None, "space", None, None), P(None, "space", None, None)),
        out_specs=(P("tm", None, "space", None, None), P("tm"), P()),
        check_vma=False,
    )
```

```python
import functools
import math

import jax
import jax.numpy as jnp
import numpy as np
from jax import lax
from jax.experimental import pallas as pl
from jax.experimental.pallas import tpu as pltpu
from jax.sharding import PartitionSpec as P

viscosity = 0.08
diffusivity = 0.05
compress_rate = 0.25
time_step = 0.5
diffusion_number = 0.08
advect_xaxis = 0.2
advect_yaxis = 0.15
advect_zaxis = 0.1
epsilon = 1e-06
MESH = pl.DeviceIdType.MESH
PAD = 8
CHUNK = 16
LANES = 128
SUBLANES = 8
PAIR = 2
VMEM_BYTES = 32 * 1024 * 1024


def layout(fields, depth, rows, cols, times_n, spaces):
    keep_y, keep_x = rows // 8, cols // 16
    groups = -(-fields * depth // (LANES // (2 * keep_x)))
    pair = PAIR if times_n % PAIR == 0 else 1
    owners = spaces * pair
    share = 2 * keep_y // owners
    used = groups * share
    height = -(-(used + 1) // SUBLANES) * SUBLANES
    return groups, pair, owners, share, used, height


def tables(fields, depth, rows, cols, times_n, spaces):
    groups, pair, owners, share, used, height = layout(fields, depth, rows, cols, times_n, spaces)
    keep_y, keep_x = rows // 8, cols // 16
    slot = 2 * keep_x
    full = depth * spaces
    k = np.arange(keep_x)
    x = np.arange(cols)
    ax = 2 * math.pi / cols * ((x[:, None] * k[None, :]) % cols)
    weight = np.where(k == 0, 1.0, 2.0) / (full * rows * cols)
    xf = np.zeros((2 * cols, LANES))
    xi = np.zeros((LANES, 2 * cols))
    for i in range(2):
        at = i * slot
        xf[i * cols : (i + 1) * cols, at : at + keep_x] = np.cos(ax)
        xf[i * cols : (i + 1) * cols, at + keep_x : at + slot] = -np.sin(ax)
        xi[at : at + keep_x, i * cols : (i + 1) * cols] = (np.cos(ax) * weight).T
        xi[at + keep_x : at + slot, i * cols : (i + 1) * cols] = (-np.sin(ax) * weight).T
    ky = np.arange(2 * keep_y)
    ky = np.where(ky < keep_y, ky, ky - 2 * keep_y)
    y = np.arange(rows)
    ay = 2 * math.pi / rows * ((ky[:, None] * y[None, :]) % rows)
    kz = np.arange(full)
    width = full * keep_x
    block = owners * height
    yf = np.zeros((block, groups * 2 * rows))
    yi = np.zeros((groups * rows, 2 * block))
    for g in range(groups):
        for at in range(2 * keep_y):
            row = at // share * height + g * share + at % share
            yf[row, g * 2 * rows : (g + 1) * 2 * rows] = np.concatenate([np.cos(ay[at]), np.sin(ay[at])])
            yi[g * rows : (g + 1) * rows, row] = np.cos(ay[at])
            yi[g * rows : (g + 1) * rows, block + row] = -np.sin(ay[at])
    zf = np.zeros((full * slot, 2 * width))
    for z in range(full):
        a = 2 * math.pi / full * ((kz * z) % full)
        for kk in range(keep_x):
            row = z * slot + kk
            re = kz * keep_x + kk
            im = re + width
            zf[row, re] = np.cos(a)
            zf[row, im] = -np.sin(a)
            zf[row + keep_x, re] = np.sin(a)
            zf[row + keep_x, im] = np.cos(a)
    zi = np.zeros((2 * width, full * slot))
    for z in range(full):
        a = 2 * math.pi / full * ((kz * z) % full)
        for kk in range(keep_x):
            re = kz * keep_x + kk
            im = re + width
            col = z * slot + kk
            zi[re, col] = np.cos(a)
            zi[im, col] = -np.sin(a)
            zi[re, col + keep_x] = np.sin(a)
            zi[im, col + keep_x] = np.cos(a)
    tz = 2 * math.pi / full * kz
    ty = 2 * math.pi / rows * ky
    tx = 2 * math.pi / cols * k
    live = (ky != -keep_y).astype(np.float64)[:, None, None]
    real = 1.0 + diffusion_number * (
        (2 * np.cos(ty) - 2)[:, None, None]
        + (2 * np.cos(tz) - 2)[None, :, None]
        + (2 * np.cos(tx) - 2)[None, None, :]
    )
    imag = -(
        advect_yaxis * np.sin(ty)[:, None, None]
        + advect_zaxis * np.sin(tz)[None, :, None]
        + advect_xaxis * np.sin(tx)[None, None, :]
    )
    symbol = (real + 1j * imag) * live
    symbol = symbol.reshape(owners, share, width)
    gains = np.zeros((owners, 2, height, width), np.float32)
    for g in range(groups):
        gains[:, 0, g * share : (g + 1) * share] = symbol.real
        gains[:, 1, g * share : (g + 1) * share] = symbol.imag
    return [xf, yf, zf, zi, yi, xi], gains


def halves(table):
    high = table.astype(jnp.bfloat16)
    low = (table - high.astype(np.float64)).astype(jnp.bfloat16)
    return np.stack([high, low])


def split(values):
    high = values.astype(jnp.bfloat16)
    return high, (values - high.astype(jnp.float32)).astype(jnp.bfloat16)


def dot(a, b):
    return jnp.dot(a, b, preferred_element_type=jnp.float32)


def times(values, table):
    high, low = split(values)
    return dot(high, table[0]) + dot(low, table[0]) + dot(high, table[1])


def under(table, values):
    high, low = split(values)
    return dot(table[0], high) + dot(table[0], low) + dot(table[1], high)


def kernel(
    sizes, starts, source, xf_h, yf_h, zf_h, zi_h, yi_h, xi_h, sym_h,
    ends, norms,
    y1, y2, y3, y4, src, fine, halo, xf, yf, zf, zi, yi, xi, sym,
    own, jumps, ahead, gathered, corrections, pieces, modes,
    load_sem, table_sem, halo_send, halo_recv, ahead_sems, jump_send, jump_recv,
    mode_send, mode_recv, relays,
):
    times_n, spaces, fields, depth, rows, cols = sizes
    keep_y, keep_x = rows // 8, cols // 16
    slot = 2 * keep_x
    layers = fields * depth
    slots = LANES // slot
    per = LANES // (slot * depth)
    groups, pair, owners, share, used, height = layout(fields, depth, rows, cols, times_n, spaces)
    chunks = rows // CHUNK
    n = lax.axis_index("tm")
    s = lax.axis_index("space")
    place = lax.rem(n, pair)
    me = place * spaces + s
    base = n - place
    up = lax.rem(s + 1, spaces)
    down = lax.rem(s + spaces - 1, spaces)

    barrier = pltpu.get_barrier_semaphore()

    def near(distance, act):
        for side, target in enumerate((n - distance, n + distance)):
            pl.when((target >= 0) & (target < times_n))(functools.partial(act, side, target))

    def enter(target, where):
        pl.semaphore_signal(barrier, inc=1, device_id=(target, where), device_id_type=MESH)

    for offset in range(1, spaces):
        enter(n, lax.rem(s + offset, spaces))
    near(1, lambda side, target: enter(target, s))
    loads = [
        pltpu.make_async_copy(starts.at[0, :, 0], y1.at[:, 0, pl.ds(PAD, rows)], load_sem.at[0]),
        pltpu.make_async_copy(
            starts.at[0, :, depth - 1], y1.at[:, depth - 1, pl.ds(PAD, rows)], load_sem.at[4]
        ),
        pltpu.make_async_copy(
            starts.at[0, :, pl.ds(1, depth - 2)],
            y1.at[:, pl.ds(1, depth - 2), pl.ds(PAD, rows)],
            load_sem.at[5],
        ),
        pltpu.make_async_copy(
            starts.at[0, :, :, pl.ds(rows - PAD, PAD)], y1.at[:, :, pl.ds(0, PAD)], load_sem.at[1]
        ),
        pltpu.make_async_copy(
            starts.at[0, :, :, pl.ds(0, PAD)], y1.at[:, :, pl.ds(PAD + rows, PAD)], load_sem.at[2]
        ),
        pltpu.make_async_copy(source, src, load_sem.at[3]),
    ]
    for copy in loads:
        copy.start()
    fills = [
        pltpu.make_async_copy(a, b, table_sem.at[i])
        for i, (a, b) in enumerate(
            [(xf_h, xf), (yf_h, yf), (zf_h, zf), (zi_h, zi), (yi_h, yi), (xi_h, xi), (sym_h, sym)]
        )
    ]
    for copy in fills:
        copy.start()
    for copy in loads[:2]:
        copy.wait()
    beside = jnp.where(n > 0, 1, 0) + jnp.where(n < times_n - 1, 1, 0)
    pl.semaphore_wait(barrier, spaces - 1 + beside)

    def relay(level):
        near(
            2**level,
            lambda side, target: pl.semaphore_signal(
                relays.at[level, side], inc=1, device_id=(target, s), device_id_type=MESH
            ),
        )

    def heard(level):
        near(2**level, lambda side, target: pl.semaphore_wait(relays.at[level, 1 - side], 1))

    levels = (times_n - 1).bit_length()

    states = [y1, y2, y3, y4]

    def halo_copy(stage, side, chunk):
        r0 = pl.multiple_of(chunk * CHUNK, CHUNK)
        state = states[stage]
        layer = depth - 1 if side == 0 else 0
        return pltpu.make_async_remote_copy(
            src_ref=state.at[:, layer, pl.ds(pl.multiple_of(PAD + r0, 8), CHUNK)],
            dst_ref=halo.at[stage, side, :, pl.ds(r0, CHUNK)],
            send_sem=halo_send.at[stage, side, chunk],
            recv_sem=halo_recv.at[stage, side, chunk],
            device_id=(n, up if side == 0 else down),
            device_id_type=MESH,
        )

    def send_first(c, carry):
        for side in range(2):
            halo_copy(0, side, c).start()
        return carry

    lax.fori_loop(0, chunks, send_first, 0)
    relay(0)

    lane = lax.broadcasted_iota(jnp.int32, (1, LANES), 1)
    first = lax.rem(lane, slot) < keep_x

    def swapped(values):
        return jnp.where(
            first, pltpu.roll(values, LANES - keep_x, 1), -pltpu.roll(values, keep_x, 1)
        )

    def transform(layer_of):
        pairs = jnp.concatenate(
            [
                jnp.concatenate([layer_of(2 * p), layer_of(2 * p + 1)], axis=1)
                for p in range(layers // 2)
            ],
            axis=0,
        )
        packed = times(pairs, xf)
        result = []
        for g in range(groups):
            total = None
            for p in range(slots // 2):
                index = g * (slots // 2) + p
                if index < layers // 2:
                    piece = packed[index * rows : (index + 1) * rows]
                    if p > 0:
                        piece = pltpu.roll(piece, 2 * p * slot, 1)
                    total = piece if total is None else total + piece
            result.append(total)
        both = jnp.concatenate([part for t in result for part in (t, swapped(t))], axis=0)
        return under(yf, both).reshape(owners, height, LANES)

    for copy in loads[2:] + fills:
        copy.wait()

    own[...] = transform(lambda l: y1[l // depth, l % depth, pl.ds(PAD, rows)])
    ahead_copy = pltpu.make_async_remote_copy(
        src_ref=own,
        dst_ref=ahead,
        send_sem=ahead_sems.at[0],
        recv_sem=ahead_sems.at[1],
        device_id=(jnp.maximum(n - 1, 0), s),
        device_id_type=MESH,
    )

    @pl.when(n > 0)
    def _():
        ahead_copy.start()

    def update(stage, z, r0, below, above):
        state = states[stage]
        mid, xm, xp, ym, yp = [], [], [], [], []
        rolled = CHUNK + 2 * PAD
        for f in range(fields):
            wide = state[f, z, pl.ds(r0, rolled)]
            centre = wide[PAD : PAD + CHUNK]
            mid.append(centre)
            ym.append(pltpu.roll(wide, 1, 0)[PAD : PAD + CHUNK])
            yp.append(pltpu.roll(wide, rolled - 1, 0)[PAD : PAD + CHUNK])
            xm.append(pltpu.roll(centre, 1, 1))
            xp.append(pltpu.roll(centre, cols - 1, 1))
        zm = [below(f) for f in range(fields)]
        zp = [above(f) for f in range(fields)]
        sides = [xm, xp, ym, yp, zm, zp]
        factors = []
        for axis, speed in enumerate((advect_xaxis, advect_yaxis, advect_zaxis)):
            factors.append((viscosity + 0.5 * speed) + 0.5 * sides[2 * axis][axis])
            factors.append((viscosity - 0.5 * speed) - 0.5 * sides[2 * axis + 1][axis])
        shift = viscosity - diffusivity
        rates = []
        for f in range(fields):
            forcing = src[f, z, pl.ds(r0, CHUNK)]
            if f == 3:
                total = (
                    (xp[0] - xm[0]) + (yp[1] - ym[1]) + (zp[2] - zm[2])
                ) * (-0.5 * compress_rate)
            else:
                gain = viscosity if f < 3 else diffusivity
                total = (-6.0 * gain) * mid[f]
                for factor, side in zip(factors, sides):
                    total = total + (factor if f < 3 else factor - shift) * side[f]
                if f < 3:
                    total = total + 0.5 * (sides[2 * f][3] - sides[2 * f + 1][3])
            rates.append(total + forcing)
        share = time_step / 6.0 * (1.0, 2.0, 2.0, 1.0)[stage]
        for f in range(fields):
            at = f * depth + z
            here = pl.ds(r0, CHUNK)
            begin = y1[f, z, pl.ds(pl.multiple_of(r0 + PAD, 8), CHUNK)]
            done = begin if stage == 0 else fine[at, here]
            fine[at, here] = done + share * rates[f]
            if stage < 3:
                later = states[stage + 1]
                step = (0.5, 0.5, 1.0)[stage] * time_step
                value = begin + step * rates[f]
                later[f, z, pl.ds(pl.multiple_of(r0 + PAD, 8), CHUNK)] = value

                @pl.when(r0 == 0)
                def _():
                    later[f, z, pl.ds(PAD + rows, PAD)] = value[:PAD]

                @pl.when(r0 == rows - CHUNK)
                def _():
                    later[f, z, pl.ds(0, PAD)] = value[CHUNK - PAD :]

    for stage in range(4):
        state = states[stage]

        def inner(i, carry):
            z = 1 + i // chunks
            r0 = pl.multiple_of(lax.rem(i, chunks) * CHUNK, CHUNK)
            at = pl.ds(pl.multiple_of(r0 + PAD, 8), CHUNK)
            update(stage, z, r0, lambda f: state[f, z - 1, at], lambda f: state[f, z + 1, at])
            return carry

        def edge(c, carry):
            r0 = pl.multiple_of(c * CHUNK, CHUNK)
            at = pl.ds(pl.multiple_of(r0 + PAD, 8), CHUNK)
            for side in range(2):
                halo_copy(stage, side, c).wait_recv()
                here = lambda f: halo[stage, side, f, pl.ds(r0, CHUNK)]
                if side == 0:
                    update(stage, 0, r0, here, lambda f: state[f, 1, at])
                else:
                    update(stage, depth - 1, r0, lambda f: state[f, depth - 2, at], here)
                if stage < 3:
                    halo_copy(stage + 1, 1 - side, c).start()
            return carry

        lax.fori_loop(0, (depth - 2) * chunks, inner, 0)
        lax.fori_loop(0, chunks, edge, 0)
        for level in range(levels):
            if min(level, 2) == stage:
                heard(level)
                if level + 1 < levels:
                    relay(level + 1)

    spec = transform(lambda l: fine[l])

    def jump_copy(index, tile, target):
        return pltpu.make_async_remote_copy(
            src_ref=jumps.at[tile],
            dst_ref=gathered.at[index],
            send_sem=jump_send.at[target[0] * spaces + target[1]],
            recv_sem=jump_recv.at[index],
            device_id=target,
            device_id_type=MESH,
        )

    def others(act):
        def body(dt, carry):
            t = n + dt
            t = jnp.where(t >= times_n, t - times_n, t)
            for ds in reversed(range(spaces)):
                where = s + ds
                where = jnp.where(where >= spaces, where - spaces, where)
                run = functools.partial(act, t, where)
                if ds == 0:
                    pl.when(dt > 0)(run)
                else:
                    run()
            return carry

        if times_n <= 8:
            for dt in sorted(range(times_n), key=lambda d: -min(d, times_n - d)):
                body(dt, 0)
        else:
            lax.fori_loop(0, times_n, body, 0)

    sent = lambda t, where: jump_copy(
        n * spaces + s, lax.rem(t, pair) * spaces + where, (t, where)
    )

    @pl.when(n < times_n - 1)
    def _():
        ahead_copy.wait_recv()
        jumps[...] = spec - ahead[...]
        others(lambda t, where: sent(t, where).start())
        gathered[n * spaces + s] = jumps[me]

    def arrive(t, where):
        @pl.when(t < times_n - 1)
        def _():
            jump_copy(t * spaces + where, me, (t, where)).wait_recv()

    others(arrive)

    width = depth * spaces * keep_x
    half = depth * slot
    steps = times_n - 1
    part = lax.broadcasted_iota(jnp.int32, (1, LANES), 1) // half

    def turned(values, move):
        move = move % LANES
        return pltpu.roll(values, move, 1) if move else values

    def joined(blocks):
        total = None
        for i, block in enumerate(blocks):
            total = block if total is None else jnp.where(part == i, block, total)
        return total

    slabs = [
        jnp.concatenate([gathered[m * spaces + k] for m in range(steps)], axis=0)
        for k in range(spaces)
    ]
    lined = [
        jnp.concatenate(
            [
                joined([turned(slabs[at + i], (i - fp) * half) for i in range(per)])
                for at in range(0, spaces, per)
            ],
            axis=1,
        )
        for fp in range(per)
    ]
    fresh = times(jnp.concatenate(lined, axis=0), zf)
    gain_re, gain_im = sym[me, 0], sym[me, 1]
    weight = jnp.where(lax.rem(lane, keep_x) == 0, 1.0, 2.0)
    zero = jnp.zeros((height, width), jnp.float32)
    held = [(zero, zero)] * per
    sizes_of = [jnp.zeros((1, LANES), jnp.float32)]
    corrections[0] = jnp.zeros((per, height, 2 * width), jnp.float32)
    for m in range(steps):
        size = None
        for fp in range(per):
            at = (fp * steps + m) * height
            re = held[fp][0] + fresh[at : at + height, :width]
            im = held[fp][1] + fresh[at : at + height, width:]
            re, im = gain_re * re - gain_im * im, gain_re * im + gain_im * re
            held[fp] = (re, im)
            corrections[m + 1, fp, :, :width] = re
            corrections[m + 1, fp, :, width:] = im
            square = re * re + im * im
            size = square if size is None else size + square
        sizes_of.append(jnp.sum(size * weight, axis=0, keepdims=True))
    back = times(
        jnp.concatenate([corrections[base + j, fp] for j in range(pair) for fp in range(per)], axis=0), zi
    )
    column = jnp.sum(jnp.concatenate(sizes_of, axis=0), axis=1, keepdims=True)
    shape = (times_n, LANES)
    diagonal = lax.broadcasted_iota(jnp.int32, shape, 0) == lax.broadcasted_iota(jnp.int32, shape, 1)
    squares = jnp.sum(jnp.where(diagonal, column, 0.0), axis=0, keepdims=True) * (
        1.0 / (depth * spaces * rows * cols)
    )
    last = lax.broadcasted_iota(jnp.int32, (height, LANES), 0) == used
    for j in range(pair):
        for k in range(spaces):
            at = k * half
            tile, inside = at // LANES * LANES, at % LANES
            piece = joined(
                [
                    turned(
                        back[(j * per + fp) * height : (j * per + fp + 1) * height, tile : tile + LANES],
                        fp * half - inside,
                    )
                    for fp in range(per)
                ]
            )
            pieces[j * spaces + k] = jnp.where(last, squares, piece)

    def mode_copy(dj, dk):
        j, k = lax.rem(place + dj, pair), lax.rem(s + dk, spaces)
        return pltpu.make_async_remote_copy(
            src_ref=pieces.at[j * spaces + k],
            dst_ref=modes.at[me],
            send_sem=mode_send.at[j * spaces + k],
            recv_sem=mode_recv.at[me],
            device_id=(base + j, k),
            device_id_type=MESH,
        )

    def mode_arrival(dj, dk):
        j, k = lax.rem(place + dj, pair), lax.rem(s + dk, spaces)
        return pltpu.make_async_remote_copy(
            src_ref=pieces.at[me],
            dst_ref=modes.at[j * spaces + k],
            send_sem=mode_send.at[j * spaces + k],
            recv_sem=mode_recv.at[j * spaces + k],
            device_id=(base + j, k),
            device_id_type=MESH,
        )

    sharers = [(dj, dk) for dj in reversed(range(pair)) for dk in reversed(range(spaces)) if dj + dk]
    for dj, dk in sharers:
        mode_copy(dj, dk).start()
    modes[me] = pieces[me]
    for dj, dk in sharers:
        mode_arrival(dj, dk).wait_recv()
    found = modes[...].reshape(owners * height, LANES)
    total = None
    for o in range(owners):
        row = found[o * height + used : o * height + used + 1]
        total = row if total is None else total + row
    cells = fields * depth * spaces * rows * cols

    def norm(values, count):
        value = jnp.sqrt(jnp.sum(values, axis=1, keepdims=True) * (1.0 / count) + epsilon)
        return jnp.broadcast_to(value, (1, LANES))

    norms[0] = norm(jnp.where(lane == n, total, 0.0), cells)
    norms[1] = norm(total, cells * times_n)

    planes = under(yi, jnp.concatenate([found, swapped(found)], axis=0))
    for g in range(groups):
        plane = planes[g * rows : (g + 1) * rows]
        count = min(slots, layers - g * slots) // 2
        shifted = [
            plane if p == 0 else pltpu.roll(plane, LANES - 2 * p * slot, 1) for p in range(count)
        ]
        fix = times(jnp.concatenate(shifted, axis=0), xi)
        for p in range(count):
            for i in range(2):
                l = g * slots + 2 * p + i
                ends[l] = fine[l] + fix[p * rows : (p + 1) * rows, i * cols : (i + 1) * cols]

    @pl.when(n < times_n - 1)
    def _():
        others(lambda t, where: sent(t, where).wait_send())

    @pl.when(n > 0)
    def _():
        ahead_copy.wait_send()

    for stage in range(4):

        def drain_halo(c, carry):
            for side in range(2):
                halo_copy(stage, side, c).wait_send()
            return carry

        lax.fori_loop(0, chunks, drain_halo, 0)
    for dj, dk in sharers:
        mode_copy(dj, dk).wait_send()


def finish(ends, norms, out, slice_out, total_out, slice_held, total_held, sems):
    copies = [pltpu.make_async_copy(ends, out, sems.at[0])]
    copies[0].start()
    for i, (held, to) in enumerate(((slice_held, slice_out), (total_held, total_out))):
        held[0] = norms[i, 0, 0]
        copies.append(pltpu.make_async_copy(held, to, sems.at[1 + i]))
        copies[-1].start()
    for copy in copies:
        copy.wait()


def solution(mesh):
    times_n, spaces = mesh.shape["tm"], mesh.shape["space"]

    def step(starts, source):
        _, fields, depth, rows, cols = starts.shape
        matrices, symbol = tables(fields, depth, rows, cols, times_n, spaces)
        constants = [halves(t) for t in matrices] + [symbol]
        operands = [starts, source] + [jnp.asarray(c) for c in constants]
        _, pair, owners, _, _, height = layout(fields, depth, rows, cols, times_n, spaces)
        slot = cols // 16 * 2
        per = LANES // (slot * depth)
        chunks = rows // CHUNK
        devices = times_n * spaces
        state = pltpu.VMEM((fields, depth, rows + 2 * PAD, cols), jnp.float32)
        dma = pltpu.SemaphoreType.DMA
        layer_shape = (fields * depth, rows, cols)
        ends, norms = pl.pallas_call(
            functools.partial(kernel, (times_n, spaces, fields, depth, rows, cols)),
            out_shape=(
                pltpu.VMEM(layer_shape, jnp.float32),
                pltpu.VMEM((2, 1, LANES), jnp.float32),
            ),
            in_specs=[pl.BlockSpec(memory_space=pltpu.HBM)] * (2 + len(constants)),
            out_specs=(
                pl.BlockSpec(memory_space=pltpu.VMEM),
                pl.BlockSpec(memory_space=pltpu.VMEM),
            ),
            scratch_shapes=[
                state, state, state, state,
                pltpu.VMEM((fields, depth, rows, cols), jnp.float32),
                pltpu.VMEM(layer_shape, jnp.float32),
                pltpu.VMEM((4, 2, fields, rows, cols), jnp.float32),
                *[pltpu.VMEM(c.shape, c.dtype) for c in constants],
                *[pltpu.VMEM((owners, height, LANES), jnp.float32)] * 3,
                pltpu.VMEM((devices, height, LANES), jnp.float32),
                pltpu.VMEM((times_n, per, height, depth * spaces * slot), jnp.float32),
                *[pltpu.VMEM((owners, height, LANES), jnp.float32)] * 2,
                dma((6,)), dma((len(constants),)),
                dma((4, 2, chunks)), dma((4, 2, chunks)), dma((2,)),
                dma((devices,)), dma((devices,)), dma((owners,)), dma((owners,)),
                pltpu.SemaphoreType.REGULAR(((times_n - 1).bit_length(), 2)),
            ],
            compiler_params=pltpu.CompilerParams(
                collective_id=0, has_side_effects=True, vmem_limit_bytes=VMEM_BYTES
            ),
        )(*[pltpu.with_memory_space_constraint(a, pltpu.HBM) for a in operands])
        out, slice_norm, total_norm = pl.pallas_call(
            finish,
            out_shape=(
                jax.ShapeDtypeStruct(layer_shape, jnp.float32),
                jax.ShapeDtypeStruct((1,), jnp.float32),
                jax.ShapeDtypeStruct((1,), jnp.float32),
            ),
            in_specs=[pl.BlockSpec(memory_space=pltpu.VMEM)] * 2,
            out_specs=[pl.BlockSpec(memory_space=pltpu.HBM)] * 3,
            scratch_shapes=[
                pltpu.SMEM((1,), jnp.float32), pltpu.SMEM((1,), jnp.float32), dma((3,)),
            ],
            compiler_params=pltpu.CompilerParams(vmem_limit_bytes=VMEM_BYTES // 2),
        )(
            pltpu.with_memory_space_constraint(ends, pltpu.VMEM),
            pltpu.with_memory_space_constraint(norms, pltpu.VMEM),
        )
        return out.reshape(starts.shape), slice_norm, total_norm

    return jax.shard_map(
        step,
        mesh=mesh,
        in_specs=(P("tm", None, "space", None, None), P(None, "space", None, None)),
        out_specs=(P("tm", None, "space", None, None), P("tm"), P()),
        check_vma=False,
    )
```

```python
import functools
import math

import jax
import jax.numpy as jnp
import numpy as np
from jax import lax
from jax.experimental import pallas as pl
from jax.experimental.pallas import tpu as pltpu
from jax.sharding import PartitionSpec as P

viscosity = 0.08
diffusivity = 0.05
compress_rate = 0.25
time_step = 0.5
diffusion_number = 0.08
advect_xaxis = 0.2
advect_yaxis = 0.15
advect_zaxis = 0.1
epsilon = 1e-06
MESH = pl.DeviceIdType.MESH
PAD = 8
CHUNK = 16
LANES = 128
SUBLANES = 8
PAIR = 2
VMEM_BYTES = 32 * 1024 * 1024


def layout(fields, depth, rows, cols, times_n, spaces):
    keep_y, keep_x = rows // 8, cols // 16
    groups = -(-fields * depth // (LANES // (2 * keep_x)))
    pair = PAIR if times_n % PAIR == 0 else 1
    owners = spaces * pair
    share = 2 * keep_y // owners
    used = groups * share
    height = -(-(used + 1) // SUBLANES) * SUBLANES
    return groups, pair, owners, share, used, height


def tables(fields, depth, rows, cols, times_n, spaces):
    groups, pair, owners, share, used, height = layout(fields, depth, rows, cols, times_n, spaces)
    keep_y, keep_x = rows // 8, cols // 16
    slot = 2 * keep_x
    full = depth * spaces
    k = np.arange(keep_x)
    x = np.arange(cols)
    ax = 2 * math.pi / cols * ((x[:, None] * k[None, :]) % cols)
    weight = np.where(k == 0, 1.0, 2.0) / (full * rows * cols)
    xf = np.zeros((2 * cols, LANES))
    xi = np.zeros((LANES, 2 * cols))
    for i in range(2):
        at = i * slot
        xf[i * cols : (i + 1) * cols, at : at + keep_x] = np.cos(ax)
        xf[i * cols : (i + 1) * cols, at + keep_x : at + slot] = -np.sin(ax)
        xi[at : at + keep_x, i * cols : (i + 1) * cols] = (np.cos(ax) * weight).T
        xi[at + keep_x : at + slot, i * cols : (i + 1) * cols] = (-np.sin(ax) * weight).T
    ky = np.arange(2 * keep_y)
    ky = np.where(ky < keep_y, ky, ky - 2 * keep_y)
    y = np.arange(rows)
    ay = 2 * math.pi / rows * ((ky[:, None] * y[None, :]) % rows)
    kz = np.arange(full)
    width = full * keep_x
    block = owners * height
    yf = np.zeros((block, groups * 2 * rows))
    yi = np.zeros((groups * rows, 2 * block))
    for g in range(groups):
        for at in range(2 * keep_y):
            row = at // share * height + g * share + at % share
            yf[row, g * 2 * rows : (g + 1) * 2 * rows] = np.concatenate([np.cos(ay[at]), np.sin(ay[at])])
            yi[g * rows : (g + 1) * rows, row] = np.cos(ay[at])
            yi[g * rows : (g + 1) * rows, block + row] = -np.sin(ay[at])
    zf = np.zeros((full * slot, 2 * width))
    for z in range(full):
        a = 2 * math.pi / full * ((kz * z) % full)
        for kk in range(keep_x):
            row = z * slot + kk
            re = kz * keep_x + kk
            im = re + width
            zf[row, re] = np.cos(a)
            zf[row, im] = -np.sin(a)
            zf[row + keep_x, re] = np.sin(a)
            zf[row + keep_x, im] = np.cos(a)
    zi = np.zeros((2 * width, full * slot))
    for z in range(full):
        a = 2 * math.pi / full * ((kz * z) % full)
        for kk in range(keep_x):
            re = kz * keep_x + kk
            im = re + width
            col = z * slot + kk
            zi[re, col] = np.cos(a)
            zi[im, col] = -np.sin(a)
            zi[re, col + keep_x] = np.sin(a)
            zi[im, col + keep_x] = np.cos(a)
    tz = 2 * math.pi / full * kz
    ty = 2 * math.pi / rows * ky
    tx = 2 * math.pi / cols * k
    live = (ky != -keep_y).astype(np.float64)[:, None, None]
    real = 1.0 + diffusion_number * (
        (2 * np.cos(ty) - 2)[:, None, None]
        + (2 * np.cos(tz) - 2)[None, :, None]
        + (2 * np.cos(tx) - 2)[None, None, :]
    )
    imag = -(
        advect_yaxis * np.sin(ty)[:, None, None]
        + advect_zaxis * np.sin(tz)[None, :, None]
        + advect_xaxis * np.sin(tx)[None, None, :]
    )
    symbol = (real + 1j * imag) * live
    symbol = symbol.reshape(owners, share, width)
    gains = np.zeros((owners, 2, height, width), np.float32)
    for g in range(groups):
        gains[:, 0, g * share : (g + 1) * share] = symbol.real
        gains[:, 1, g * share : (g + 1) * share] = symbol.imag
    return [xf, yf, zf, zi, yi, xi], gains


def halves(table):
    high = table.astype(jnp.bfloat16)
    low = (table - high.astype(np.float64)).astype(jnp.bfloat16)
    return np.stack([high, low])


def split(values):
    high = values.astype(jnp.bfloat16)
    return high, (values - high.astype(jnp.float32)).astype(jnp.bfloat16)


def dot(a, b):
    return jnp.dot(a, b, preferred_element_type=jnp.float32)


def times(values, table):
    high, low = split(values)
    return dot(high, table[0]) + dot(low, table[0]) + dot(high, table[1])


def under(table, values):
    high, low = split(values)
    return dot(table[0], high) + dot(table[0], low) + dot(table[1], high)


def kernel(
    sizes, starts, source, xf_h, yf_h, zf_h, zi_h, yi_h, xi_h, sym_h,
    ends, norms,
    y1, y2, y3, y4, src, fine, halo, xf, yf, zf, zi, yi, xi, sym,
    own, jumps, ahead, gathered, corrections, pieces, modes,
    load_sem, table_sem, halo_send, halo_recv, ahead_sems, jump_send, jump_recv,
    mode_send, mode_recv, relays,
):
    times_n, spaces, fields, depth, rows, cols = sizes
    keep_y, keep_x = rows // 8, cols // 16
    slot = 2 * keep_x
    layers = fields * depth
    slots = LANES // slot
    per = LANES // (slot * depth)
    groups, pair, owners, share, used, height = layout(fields, depth, rows, cols, times_n, spaces)
    chunks = rows // CHUNK
    n = lax.axis_index("tm")
    s = lax.axis_index("space")
    place = lax.rem(n, pair)
    me = place * spaces + s
    base = n - place
    up = lax.rem(s + 1, spaces)
    down = lax.rem(s + spaces - 1, spaces)

    barrier = pltpu.get_barrier_semaphore()

    def near(distance, act):
        for side, target in enumerate((n - distance, n + distance)):
            pl.when((target >= 0) & (target < times_n))(functools.partial(act, side, target))

    def enter(target, where):
        pl.semaphore_signal(barrier, inc=1, device_id=(target, where), device_id_type=MESH)

    for offset in range(1, spaces):
        enter(n, lax.rem(s + offset, spaces))
    near(1, lambda side, target: enter(target, s))
    loads = [
        pltpu.make_async_copy(starts.at[0, :, 0], y1.at[:, 0, pl.ds(PAD, rows)], load_sem.at[0]),
        pltpu.make_async_copy(
            starts.at[0, :, depth - 1], y1.at[:, depth - 1, pl.ds(PAD, rows)], load_sem.at[4]
        ),
        pltpu.make_async_copy(
            starts.at[0, :, pl.ds(1, depth - 2)],
            y1.at[:, pl.ds(1, depth - 2), pl.ds(PAD, rows)],
            load_sem.at[5],
        ),
        pltpu.make_async_copy(
            starts.at[0, :, :, pl.ds(rows - PAD, PAD)], y1.at[:, :, pl.ds(0, PAD)], load_sem.at[1]
        ),
        pltpu.make_async_copy(
            starts.at[0, :, :, pl.ds(0, PAD)], y1.at[:, :, pl.ds(PAD + rows, PAD)], load_sem.at[2]
        ),
        pltpu.make_async_copy(source, src, load_sem.at[3]),
    ]
    for copy in loads:
        copy.start()
    fills = [
        pltpu.make_async_copy(a, b, table_sem.at[i])
        for i, (a, b) in enumerate(
            [(xf_h, xf), (yf_h, yf), (zf_h, zf), (zi_h, zi), (yi_h, yi), (xi_h, xi), (sym_h, sym)]
        )
    ]
    for copy in fills:
        copy.start()
    for copy in loads[:2]:
        copy.wait()
    beside = jnp.where(n > 0, 1, 0) + jnp.where(n < times_n - 1, 1, 0)
    pl.semaphore_wait(barrier, spaces - 1 + beside)

    def relay(level):
        near(
            2**level,
            lambda side, target: pl.semaphore_signal(
                relays.at[level, side], inc=1, device_id=(target, s), device_id_type=MESH
            ),
        )

    def heard(level):
        near(2**level, lambda side, target: pl.semaphore_wait(relays.at[level, 1 - side], 1))

    levels = (times_n - 1).bit_length()

    states = [y1, y2, y3, y4]

    def halo_copy(stage, side, chunk):
        r0 = pl.multiple_of(chunk * CHUNK, CHUNK)
        state = states[stage]
        layer = depth - 1 if side == 0 else 0
        return pltpu.make_async_remote_copy(
            src_ref=state.at[:, layer, pl.ds(pl.multiple_of(PAD + r0, 8), CHUNK)],
            dst_ref=halo.at[stage, side, :, pl.ds(r0, CHUNK)],
            send_sem=halo_send,
            recv_sem=halo_recv.at[stage % 2, side, chunk],
            device_id=(n, up if side == 0 else down),
            device_id_type=MESH,
        )

    def send_first(c, carry):
        for side in range(2):
            halo_copy(0, side, c).start()
        return carry

    lax.fori_loop(0, chunks, send_first, 0)
    relay(0)

    lane = lax.broadcasted_iota(jnp.int32, (1, LANES), 1)
    first = lax.rem(lane, slot) < keep_x

    def swapped(values):
        return jnp.where(
            first, pltpu.roll(values, LANES - keep_x, 1), -pltpu.roll(values, keep_x, 1)
        )

    def transform(layer_of):
        pairs = jnp.concatenate(
            [
                jnp.concatenate([layer_of(2 * p), layer_of(2 * p + 1)], axis=1)
                for p in range(layers // 2)
            ],
            axis=0,
        )
        packed = times(pairs, xf)
        result = []
        for g in range(groups):
            total = None
            for p in range(slots // 2):
                index = g * (slots // 2) + p
                if index < layers // 2:
                    piece = packed[index * rows : (index + 1) * rows]
                    if p > 0:
                        piece = pltpu.roll(piece, 2 * p * slot, 1)
                    total = piece if total is None else total + piece
            result.append(total)
        both = jnp.concatenate([part for t in result for part in (t, swapped(t))], axis=0)
        return under(yf, both).reshape(owners, height, LANES)

    for copy in loads[2:] + fills:
        copy.wait()

    own[...] = transform(lambda l: y1[l // depth, l % depth, pl.ds(PAD, rows)])
    ahead_copy = pltpu.make_async_remote_copy(
        src_ref=own,
        dst_ref=ahead,
        send_sem=ahead_sems.at[0],
        recv_sem=ahead_sems.at[1],
        device_id=(jnp.maximum(n - 1, 0), s),
        device_id_type=MESH,
    )

    @pl.when(n > 0)
    def _():
        ahead_copy.start()

    def update(stage, z, r0, below, above):
        state = states[stage]
        mid, xm, xp, ym, yp = [], [], [], [], []
        rolled = CHUNK + 2 * PAD
        for f in range(fields):
            wide = state[f, z, pl.ds(r0, rolled)]
            centre = wide[PAD : PAD + CHUNK]
            mid.append(centre)
            ym.append(pltpu.roll(wide, 1, 0)[PAD : PAD + CHUNK])
            yp.append(pltpu.roll(wide, rolled - 1, 0)[PAD : PAD + CHUNK])
            xm.append(pltpu.roll(centre, 1, 1))
            xp.append(pltpu.roll(centre, cols - 1, 1))
        zm = [below(f) for f in range(fields)]
        zp = [above(f) for f in range(fields)]
        sides = [xm, xp, ym, yp, zm, zp]
        factors = []
        for axis, speed in enumerate((advect_xaxis, advect_yaxis, advect_zaxis)):
            factors.append((viscosity + 0.5 * speed) + 0.5 * sides[2 * axis][axis])
            factors.append((viscosity - 0.5 * speed) - 0.5 * sides[2 * axis + 1][axis])
        shift = viscosity - diffusivity
        rates = []
        for f in range(fields):
            forcing = src[f, z, pl.ds(r0, CHUNK)]
            if f == 3:
                total = (
                    (xp[0] - xm[0]) + (yp[1] - ym[1]) + (zp[2] - zm[2])
                ) * (-0.5 * compress_rate)
            else:
                gain = viscosity if f < 3 else diffusivity
                total = (-6.0 * gain) * mid[f]
                for factor, side in zip(factors, sides):
                    total = total + (factor if f < 3 else factor - shift) * side[f]
                if f < 3:
                    total = total + 0.5 * (sides[2 * f][3] - sides[2 * f + 1][3])
            rates.append(total + forcing)
        share = time_step / 6.0 * (1.0, 2.0, 2.0, 1.0)[stage]
        for f in range(fields):
            at = f * depth + z
            here = pl.ds(r0, CHUNK)
            begin = y1[f, z, pl.ds(pl.multiple_of(r0 + PAD, 8), CHUNK)]
            done = begin if stage == 0 else fine[at, here]
            fine[at, here] = done + share * rates[f]
            if stage < 3:
                later = states[stage + 1]
                step = (0.5, 0.5, 1.0)[stage] * time_step
                value = begin + step * rates[f]
                later[f, z, pl.ds(pl.multiple_of(r0 + PAD, 8), CHUNK)] = value

                @pl.when(r0 == 0)
                def _():
                    later[f, z, pl.ds(PAD + rows, PAD)] = value[:PAD]

                @pl.when(r0 == rows - CHUNK)
                def _():
                    later[f, z, pl.ds(0, PAD)] = value[CHUNK - PAD :]

    for stage in range(4):
        state = states[stage]

        def inner(i, carry):
            z = 1 + i // chunks
            r0 = pl.multiple_of(lax.rem(i, chunks) * CHUNK, CHUNK)
            at = pl.ds(pl.multiple_of(r0 + PAD, 8), CHUNK)
            update(stage, z, r0, lambda f: state[f, z - 1, at], lambda f: state[f, z + 1, at])
            return carry

        def edge(c, carry):
            r0 = pl.multiple_of(c * CHUNK, CHUNK)
            at = pl.ds(pl.multiple_of(r0 + PAD, 8), CHUNK)
            for side in range(2):
                halo_copy(stage, side, c).wait_recv()
                here = lambda f: halo[stage, side, f, pl.ds(r0, CHUNK)]
                if side == 0:
                    update(stage, 0, r0, here, lambda f: state[f, 1, at])
                else:
                    update(stage, depth - 1, r0, lambda f: state[f, depth - 2, at], here)
                if stage < 3:
                    halo_copy(stage + 1, 1 - side, c).start()
            return carry

        lax.fori_loop(0, (depth - 2) * chunks, inner, 0)
        lax.fori_loop(0, chunks, edge, 0)
        for level in range(levels):
            if min(level, 2) == stage:
                heard(level)
                if level + 1 < levels:
                    relay(level + 1)

    spec = transform(lambda l: fine[l])

    def jump_copy(index, tile, target):
        return pltpu.make_async_remote_copy(
            src_ref=jumps.at[tile],
            dst_ref=gathered.at[index],
            send_sem=jump_send,
            recv_sem=jump_recv,
            device_id=target,
            device_id_type=MESH,
        )

    def others(act):
        def body(dt, carry):
            t = n + dt
            t = jnp.where(t >= times_n, t - times_n, t)
            for ds in reversed(range(spaces)):
                where = s + ds
                where = jnp.where(where >= spaces, where - spaces, where)
                run = functools.partial(act, t, where)
                if ds == 0:
                    pl.when(dt > 0)(run)
                else:
                    run()
            return carry

        if times_n <= 8:
            for dt in sorted(range(times_n), key=lambda d: -min(d, times_n - d)):
                body(dt, 0)
        else:
            lax.fori_loop(0, times_n, body, 0)

    sent = lambda t, where: jump_copy(
        n * spaces + s, lax.rem(t, pair) * spaces + where, (t, where)
    )

    @pl.when(n < times_n - 1)
    def _():
        ahead_copy.wait_recv()
        jumps[...] = spec - ahead[...]
        others(lambda t, where: sent(t, where).start())
        gathered[n * spaces + s] = jumps[me]

    def settle(ref, count, sem):
        held = ref if count is None else ref.at[pl.ds(0, count)]
        pltpu.make_async_copy(held, held, sem).wait()

    pl.when(n < times_n - 1)(
        lambda: settle(gathered, (times_n - 1) * spaces - 1, jump_recv)
    )
    pl.when(n == times_n - 1)(lambda: settle(gathered, (times_n - 1) * spaces, jump_recv))

    width = depth * spaces * keep_x
    half = depth * slot
    steps = times_n - 1
    part = lax.broadcasted_iota(jnp.int32, (1, LANES), 1) // half

    def turned(values, move):
        move = move % LANES
        return pltpu.roll(values, move, 1) if move else values

    def joined(blocks):
        total = None
        for i, block in enumerate(blocks):
            total = block if total is None else jnp.where(part == i, block, total)
        return total

    slabs = [
        jnp.concatenate([gathered[m * spaces + k] for m in range(steps)], axis=0)
        for k in range(spaces)
    ]
    lined = [
        jnp.concatenate(
            [
                joined([turned(slabs[at + i], (i - fp) * half) for i in range(per)])
                for at in range(0, spaces, per)
            ],
            axis=1,
        )
        for fp in range(per)
    ]
    fresh = times(jnp.concatenate(lined, axis=0), zf)
    gain_re, gain_im = sym[me, 0], sym[me, 1]
    weight = jnp.where(lax.rem(lane, keep_x) == 0, 1.0, 2.0)
    zero = jnp.zeros((height, width), jnp.float32)
    held = [(zero, zero)] * per
    sizes_of = [jnp.zeros((1, LANES), jnp.float32)]
    corrections[0] = jnp.zeros((per, height, 2 * width), jnp.float32)
    for m in range(steps):
        size = None
        for fp in range(per):
            at = (fp * steps + m) * height
            re = held[fp][0] + fresh[at : at + height, :width]
            im = held[fp][1] + fresh[at : at + height, width:]
            re, im = gain_re * re - gain_im * im, gain_re * im + gain_im * re
            held[fp] = (re, im)
            corrections[m + 1, fp, :, :width] = re
            corrections[m + 1, fp, :, width:] = im
            square = re * re + im * im
            size = square if size is None else size + square
        sizes_of.append(jnp.sum(size * weight, axis=0, keepdims=True))
    back = times(
        jnp.concatenate([corrections[base + j, fp] for j in range(pair) for fp in range(per)], axis=0), zi
    )
    column = jnp.sum(jnp.concatenate(sizes_of, axis=0), axis=1, keepdims=True)
    shape = (times_n, LANES)
    diagonal = lax.broadcasted_iota(jnp.int32, shape, 0) == lax.broadcasted_iota(jnp.int32, shape, 1)
    squares = jnp.sum(jnp.where(diagonal, column, 0.0), axis=0, keepdims=True) * (
        1.0 / (depth * spaces * rows * cols)
    )
    last = lax.broadcasted_iota(jnp.int32, (height, LANES), 0) == used
    for j in range(pair):
        for k in range(spaces):
            at = k * half
            tile, inside = at // LANES * LANES, at % LANES
            piece = joined(
                [
                    turned(
                        back[(j * per + fp) * height : (j * per + fp + 1) * height, tile : tile + LANES],
                        fp * half - inside,
                    )
                    for fp in range(per)
                ]
            )
            pieces[j * spaces + k] = jnp.where(last, squares, piece)

    def mode_copy(dj, dk):
        j, k = lax.rem(place + dj, pair), lax.rem(s + dk, spaces)
        return pltpu.make_async_remote_copy(
            src_ref=pieces.at[j * spaces + k],
            dst_ref=modes.at[me],
            send_sem=mode_send,
            recv_sem=mode_recv,
            device_id=(base + j, k),
            device_id_type=MESH,
        )

    sharers = [(dj, dk) for dj in reversed(range(pair)) for dk in reversed(range(spaces)) if dj + dk]
    for dj, dk in sharers:
        mode_copy(dj, dk).start()
    modes[me] = pieces[me]
    settle(modes, owners - 1, mode_recv)
    found = modes[...].reshape(owners * height, LANES)
    total = None
    for o in range(owners):
        row = found[o * height + used : o * height + used + 1]
        total = row if total is None else total + row
    cells = fields * depth * spaces * rows * cols

    def norm(values, count):
        value = jnp.sqrt(jnp.sum(values, axis=1, keepdims=True) * (1.0 / count) + epsilon)
        return jnp.broadcast_to(value, (1, LANES))

    norms[0] = norm(jnp.where(lane == n, total, 0.0), cells)
    norms[1] = norm(total, cells * times_n)

    planes = under(yi, jnp.concatenate([found, swapped(found)], axis=0))
    for g in range(groups):
        plane = planes[g * rows : (g + 1) * rows]
        count = min(slots, layers - g * slots) // 2
        shifted = [
            plane if p == 0 else pltpu.roll(plane, LANES - 2 * p * slot, 1) for p in range(count)
        ]
        fix = times(jnp.concatenate(shifted, axis=0), xi)
        for p in range(count):
            for i in range(2):
                l = g * slots + 2 * p + i
                ends[l] = fine[l] + fix[p * rows : (p + 1) * rows, i * cols : (i + 1) * cols]

    pl.when(n < times_n - 1)(lambda: settle(gathered, times_n * spaces - 1, jump_send))

    @pl.when(n > 0)
    def _():
        ahead_copy.wait_send()

    settle(halo, None, halo_send)
    settle(modes, owners - 1, mode_send)


def finish(ends, norms, out, slice_out, total_out, slice_held, total_held, sems):
    copies = [pltpu.make_async_copy(ends, out, sems.at[0])]
    copies[0].start()
    for i, (held, to) in enumerate(((slice_held, slice_out), (total_held, total_out))):
        held[0] = norms[i, 0, 0]
        copies.append(pltpu.make_async_copy(held, to, sems.at[1 + i]))
        copies[-1].start()
    for copy in copies:
        copy.wait()


def solution(mesh):
    times_n, spaces = mesh.shape["tm"], mesh.shape["space"]

    def step(starts, source):
        _, fields, depth, rows, cols = starts.shape
        matrices, symbol = tables(fields, depth, rows, cols, times_n, spaces)
        constants = [halves(t) for t in matrices] + [symbol]
        operands = [starts, source] + [jnp.asarray(c) for c in constants]
        _, pair, owners, _, _, height = layout(fields, depth, rows, cols, times_n, spaces)
        slot = cols // 16 * 2
        per = LANES // (slot * depth)
        chunks = rows // CHUNK
        devices = times_n * spaces
        state = pltpu.VMEM((fields, depth, rows + 2 * PAD, cols), jnp.float32)
        dma = pltpu.SemaphoreType.DMA
        layer_shape = (fields * depth, rows, cols)
        ends, norms = pl.pallas_call(
            functools.partial(kernel, (times_n, spaces, fields, depth, rows, cols)),
            out_shape=(
                pltpu.VMEM(layer_shape, jnp.float32),
                pltpu.VMEM((2, 1, LANES), jnp.float32),
            ),
            in_specs=[pl.BlockSpec(memory_space=pltpu.HBM)] * (2 + len(constants)),
            out_specs=(
                pl.BlockSpec(memory_space=pltpu.VMEM),
                pl.BlockSpec(memory_space=pltpu.VMEM),
            ),
            scratch_shapes=[
                state, state, state, state,
                pltpu.VMEM((fields, depth, rows, cols), jnp.float32),
                pltpu.VMEM(layer_shape, jnp.float32),
                pltpu.VMEM((4, 2, fields, rows, cols), jnp.float32),
                *[pltpu.VMEM(c.shape, c.dtype) for c in constants],
                *[pltpu.VMEM((owners, height, LANES), jnp.float32)] * 3,
                pltpu.VMEM((devices, height, LANES), jnp.float32),
                pltpu.VMEM((times_n, per, height, depth * spaces * slot), jnp.float32),
                *[pltpu.VMEM((owners, height, LANES), jnp.float32)] * 2,
                dma((6,)), dma((len(constants),)),
                dma, dma((2, 2, chunks)), dma((2,)), dma, dma, dma, dma,
                pltpu.SemaphoreType.REGULAR(((times_n - 1).bit_length(), 2)),
            ],
            compiler_params=pltpu.CompilerParams(
                collective_id=0, has_side_effects=True, vmem_limit_bytes=VMEM_BYTES
            ),
        )(*[pltpu.with_memory_space_constraint(a, pltpu.HBM) for a in operands])
        out, slice_norm, total_norm = pl.pallas_call(
            finish,
            out_shape=(
                jax.ShapeDtypeStruct(layer_shape, jnp.float32),
                jax.ShapeDtypeStruct((1,), jnp.float32),
                jax.ShapeDtypeStruct((1,), jnp.float32),
            ),
            in_specs=[pl.BlockSpec(memory_space=pltpu.VMEM)] * 2,
            out_specs=[pl.BlockSpec(memory_space=pltpu.HBM)] * 3,
            scratch_shapes=[
                pltpu.SMEM((1,), jnp.float32), pltpu.SMEM((1,), jnp.float32), dma((3,)),
            ],
            compiler_params=pltpu.CompilerParams(vmem_limit_bytes=VMEM_BYTES // 2),
        )(
            pltpu.with_memory_space_constraint(ends, pltpu.VMEM),
            pltpu.with_memory_space_constraint(norms, pltpu.VMEM),
        )
        return out.reshape(starts.shape), slice_norm, total_norm

    return jax.shard_map(
        step,
        mesh=mesh,
        in_specs=(P("tm", None, "space", None, None), P(None, "space", None, None)),
        out_specs=(P("tm", None, "space", None, None), P("tm"), P()),
        check_vma=False,
    )
```

```python
import functools
import math

import jax
import jax.numpy as jnp
import numpy as np
from jax import lax
from jax.experimental import pallas as pl
from jax.experimental.pallas import tpu as pltpu
from jax.sharding import PartitionSpec as P

viscosity = 0.08
diffusivity = 0.05
compress_rate = 0.25
time_step = 0.5
diffusion_number = 0.08
advect_xaxis = 0.2
advect_yaxis = 0.15
advect_zaxis = 0.1
epsilon = 1e-06
MESH = pl.DeviceIdType.MESH
PAD = 8
CHUNK = 16
LANES = 128
SUBLANES = 8
PAIR = 2
VMEM_BYTES = 32 * 1024 * 1024


def layout(fields, depth, rows, cols, times_n, spaces):
    keep_y, keep_x = rows // 8, cols // 16
    groups = -(-fields * depth // (LANES // (2 * keep_x)))
    pair = PAIR if times_n % PAIR == 0 else 1
    owners = spaces * pair
    share = 2 * keep_y // owners
    used = groups * share
    height = -(-max(used + 1, used + share) // SUBLANES) * SUBLANES
    return groups, pair, owners, share, used, height


def tables(fields, depth, rows, cols, times_n, spaces):
    groups, pair, owners, share, used, height = layout(fields, depth, rows, cols, times_n, spaces)
    keep_y, keep_x = rows // 8, cols // 16
    slot = 2 * keep_x
    full = depth * spaces
    k = np.arange(keep_x)
    x = np.arange(cols)
    ax = 2 * math.pi / cols * ((x[:, None] * k[None, :]) % cols)
    weight = np.where(k == 0, 1.0, 2.0) / (full * rows * cols)
    xf = np.zeros((2 * cols, LANES))
    xi = np.zeros((LANES, 2 * cols))
    for i in range(2):
        at = i * slot
        xf[i * cols : (i + 1) * cols, at : at + keep_x] = np.cos(ax)
        xf[i * cols : (i + 1) * cols, at + keep_x : at + slot] = -np.sin(ax)
        xi[at : at + keep_x, i * cols : (i + 1) * cols] = (np.cos(ax) * weight).T
        xi[at + keep_x : at + slot, i * cols : (i + 1) * cols] = (-np.sin(ax) * weight).T
    ky = np.arange(2 * keep_y)
    ky = np.where(ky < keep_y, ky, ky - 2 * keep_y)
    y = np.arange(rows)
    ay = 2 * math.pi / rows * ((ky[:, None] * y[None, :]) % rows)
    kz = np.arange(full)
    width = full * keep_x
    block = owners * height
    yf = np.zeros((block, (groups + 1) * 2 * rows))
    yi = np.zeros((groups * rows, 2 * block))
    for g in range(groups + 1):
        for at in range(2 * keep_y):
            row = at // share * height + g * share + at % share
            yf[row, g * 2 * rows : (g + 1) * 2 * rows] = np.concatenate([np.cos(ay[at]), np.sin(ay[at])])
    for g in range(groups):
        for at in range(2 * keep_y):
            row = at // share * height + g * share + at % share
            yi[g * rows : (g + 1) * rows, row] = np.cos(ay[at])
            yi[g * rows : (g + 1) * rows, block + row] = -np.sin(ay[at])
    zf = np.zeros((full * slot, 2 * width))
    for z in range(full):
        a = 2 * math.pi / full * ((kz * z) % full)
        for kk in range(keep_x):
            row = z * slot + kk
            re = kz * keep_x + kk
            im = re + width
            zf[row, re] = np.cos(a)
            zf[row, im] = -np.sin(a)
            zf[row + keep_x, re] = np.sin(a)
            zf[row + keep_x, im] = np.cos(a)
    zi = np.zeros((2 * width, full * slot))
    for z in range(full):
        a = 2 * math.pi / full * ((kz * z) % full)
        for kk in range(keep_x):
            re = kz * keep_x + kk
            im = re + width
            col = z * slot + kk
            zi[re, col] = np.cos(a)
            zi[im, col] = -np.sin(a)
            zi[re, col + keep_x] = np.sin(a)
            zi[im, col + keep_x] = np.cos(a)
    tz = 2 * math.pi / full * kz
    ty = 2 * math.pi / rows * ky
    tx = 2 * math.pi / cols * k
    live = (ky != -keep_y).astype(np.float64)[:, None, None]
    real = 1.0 + diffusion_number * (
        (2 * np.cos(ty) - 2)[:, None, None]
        + (2 * np.cos(tz) - 2)[None, :, None]
        + (2 * np.cos(tx) - 2)[None, None, :]
    )
    imag = -(
        advect_yaxis * np.sin(ty)[:, None, None]
        + advect_zaxis * np.sin(tz)[None, :, None]
        + advect_xaxis * np.sin(tx)[None, None, :]
    )
    symbol = (real + 1j * imag) * live
    symbol = symbol.reshape(owners, share, width)
    per = LANES // (slot * depth)
    gains = np.zeros((owners, per, 2, height, width), np.float32)
    for f in range(fields):
        at = f // per * share
        gains[:, f % per, 0, at : at + share] = symbol.real
        gains[:, f % per, 1, at : at + share] = symbol.imag
    return [xf, yf, zf, zi, yi, xi], gains


def halves(table):
    high = table.astype(jnp.bfloat16)
    low = (table - high.astype(np.float64)).astype(jnp.bfloat16)
    return np.stack([high, low])


def split(values):
    high = values.astype(jnp.bfloat16)
    return high, (values - high.astype(jnp.float32)).astype(jnp.bfloat16)


def dot(a, b):
    return jnp.dot(a, b, preferred_element_type=jnp.float32)


def times(values, table):
    high, low = split(values)
    return dot(high, table[0]) + dot(low, table[0]) + dot(high, table[1])


def under(table, values):
    high, low = split(values)
    return dot(table[0], high) + dot(table[0], low) + dot(table[1], high)


def kernel(
    sizes, starts, source, xf_h, yf_h, zf_h, zi_h, yi_h, xi_h, sym_h,
    ends, norms,
    y1, y2, y3, y4, src, fine, rims, halo, xf, yf, zf, zi, yi, xi, sym,
    own, jumps, ahead, gathered, corrections, pieces, modes,
    load_sem, table_sem, halo_send, halo_recv, ahead_sems, jump_send, jump_recv,
    mode_send, mode_recv, relays,
):
    times_n, spaces, fields, depth, rows, cols = sizes
    keep_y, keep_x = rows // 8, cols // 16
    slot = 2 * keep_x
    layers = fields * depth
    slots = LANES // slot
    per = LANES // (slot * depth)
    groups, pair, owners, share, used, height = layout(fields, depth, rows, cols, times_n, spaces)
    chunks = rows // CHUNK
    n = lax.axis_index("tm")
    s = lax.axis_index("space")
    place = lax.rem(n, pair)
    me = place * spaces + s
    base = n - place
    up = lax.rem(s + 1, spaces)
    down = lax.rem(s + spaces - 1, spaces)

    barrier = pltpu.get_barrier_semaphore()

    def near(distance, act):
        for side, target in enumerate((n - distance, n + distance)):
            pl.when((target >= 0) & (target < times_n))(functools.partial(act, side, target))

    def enter(target, where):
        pl.semaphore_signal(barrier, inc=1, device_id=(target, where), device_id_type=MESH)

    for offset in range(1, spaces):
        enter(n, lax.rem(s + offset, spaces))
    near(1, lambda side, target: enter(target, s))
    loads = [
        pltpu.make_async_copy(starts.at[0, :, 0], y1.at[:, 0, pl.ds(PAD, rows)], load_sem.at[0]),
        pltpu.make_async_copy(
            starts.at[0, :, depth - 1], y1.at[:, depth - 1, pl.ds(PAD, rows)], load_sem.at[4]
        ),
        pltpu.make_async_copy(
            starts.at[0, :, pl.ds(1, depth - 2)],
            y1.at[:, pl.ds(1, depth - 2), pl.ds(PAD, rows)],
            load_sem.at[5],
        ),
        pltpu.make_async_copy(
            starts.at[0, :, :, pl.ds(rows - PAD, PAD)], y1.at[:, :, pl.ds(0, PAD)], load_sem.at[1]
        ),
        pltpu.make_async_copy(
            starts.at[0, :, :, pl.ds(0, PAD)], y1.at[:, :, pl.ds(PAD + rows, PAD)], load_sem.at[2]
        ),
        pltpu.make_async_copy(source, src, load_sem.at[3]),
    ]
    for copy in loads:
        copy.start()
    fills = [
        pltpu.make_async_copy(a, b, table_sem.at[i])
        for i, (a, b) in enumerate(
            [(xf_h, xf), (yf_h, yf), (zf_h, zf), (zi_h, zi), (yi_h, yi), (xi_h, xi), (sym_h, sym)]
        )
    ]
    for copy in fills:
        copy.start()
    for copy in loads[:2]:
        copy.wait()
    beside = jnp.where(n > 0, 1, 0) + jnp.where(n < times_n - 1, 1, 0)
    pl.semaphore_wait(barrier, spaces - 1 + beside)

    def relay(level):
        near(
            2**level,
            lambda side, target: pl.semaphore_signal(
                relays.at[level, side], inc=1, device_id=(target, s), device_id_type=MESH
            ),
        )

    def heard(level):
        near(2**level, lambda side, target: pl.semaphore_wait(relays.at[level, 1 - side], 1))

    levels = (times_n - 1).bit_length()

    states = [y1, y2, y3, y4]

    def halo_copy(stage, side, chunk):
        r0 = pl.multiple_of(chunk * CHUNK, CHUNK)
        state = states[stage]
        layer = depth - 1 if side == 0 else 0
        return pltpu.make_async_remote_copy(
            src_ref=state.at[:, layer, pl.ds(pl.multiple_of(PAD + r0, 8), CHUNK)],
            dst_ref=halo.at[stage, side, :, pl.ds(r0, CHUNK)],
            send_sem=halo_send,
            recv_sem=halo_recv.at[stage % 2, side, chunk],
            device_id=(n, up if side == 0 else down),
            device_id_type=MESH,
        )

    def send_first(c, carry):
        for side in range(2):
            halo_copy(0, side, c).start()
        return carry

    lax.fori_loop(0, chunks, send_first, 0)
    relay(0)

    lane = lax.broadcasted_iota(jnp.int32, (1, LANES), 1)
    first = lax.rem(lane, slot) < keep_x

    def swapped(values):
        return jnp.where(
            first, pltpu.roll(values, LANES - keep_x, 1), -pltpu.roll(values, keep_x, 1)
        )

    def transform(pairs, count):
        stacked = jnp.concatenate(
            [jnp.concatenate([left, right], axis=1) for _, _, left, right in pairs], axis=0
        )
        packed = times(stacked, xf)
        result = [None] * count
        for i, (g, at, _, _) in enumerate(pairs):
            piece = packed[i * rows : (i + 1) * rows]
            if at > 0:
                piece = pltpu.roll(piece, at * slot, 1)
            result[g] = piece if result[g] is None else result[g] + piece
        both = jnp.concatenate([part for t in result for part in (t, swapped(t))], axis=0)
        table = [yf[i, :, : count * 2 * rows] for i in range(2)]
        return under(table, both).reshape(owners, height, LANES)

    def paired(layer_of):
        return [
            (l // slots, l % slots, layer_of(l), layer_of(l + 1)) for l in range(0, layers, 2)
        ]

    def rim_place(f):
        if f // per == groups - 1 and fields % per:
            return groups - 1, fields % per * depth
        return groups, f % per * depth + 2 * (f // per)

    for copy in loads[2:] + fills:
        copy.wait()

    own[...] = transform(
        paired(lambda l: y1[l // depth, l % depth, pl.ds(PAD, rows)]), groups
    )
    ahead_copy = pltpu.make_async_remote_copy(
        src_ref=own,
        dst_ref=ahead,
        send_sem=ahead_sems.at[0],
        recv_sem=ahead_sems.at[1],
        device_id=(jnp.maximum(n - 1, 0), s),
        device_id_type=MESH,
    )

    @pl.when(n > 0)
    def _():
        ahead_copy.start()

    shift = viscosity - diffusivity

    def reach(layer, sign):
        factor = (viscosity + sign * 0.5 * advect_zaxis) + (sign * 0.5) * layer[2]
        result = [factor * layer[f] for f in range(3)]
        result[2] = result[2] + (sign * 0.5) * layer[3]
        return result + [(sign * 0.5 * compress_rate) * layer[2], (factor - shift) * layer[4]]

    def weigh(stage):
        return time_step / 6.0 * (1.0, 2.0, 2.0, 1.0)[stage]

    def update(stage, z, r0, below, above, rim=None):
        state = states[stage]
        mid, xm, xp, ym, yp = [], [], [], [], []
        rolled = CHUNK + 2 * PAD
        for f in range(fields):
            wide = state[f, z, pl.ds(r0, rolled)]
            centre = wide[PAD : PAD + CHUNK]
            mid.append(centre)
            ym.append(pltpu.roll(wide, 1, 0)[PAD : PAD + CHUNK])
            yp.append(pltpu.roll(wide, rolled - 1, 0)[PAD : PAD + CHUNK])
            xm.append(pltpu.roll(centre, 1, 1))
            xp.append(pltpu.roll(centre, cols - 1, 1))
        sides = [(xm, 0, 1.0, advect_xaxis), (xp, 0, -1.0, advect_xaxis)]
        sides += [(ym, 1, 1.0, advect_yaxis), (yp, 1, -1.0, advect_yaxis)]
        for neighbour, sign in ((below, 1.0), (above, -1.0)):
            if neighbour is not None:
                held = [neighbour(f) for f in range(fields)]
                sides.append((held, 2, sign, advect_zaxis))
        factors = [
            (viscosity + sign * 0.5 * speed) + (sign * 0.5) * side[axis]
            for side, axis, sign, speed in sides
        ]
        rates = []
        for f in range(fields):
            forcing = src[f, z, pl.ds(r0, CHUNK)]
            if f == 3:
                total = None
                for side, axis, sign, _ in sides:
                    if total is None:
                        total = side[axis]
                    else:
                        total = total + side[axis] if sign > 0 else total - side[axis]
                total = total * (0.5 * compress_rate)
            else:
                gain = viscosity if f < 3 else diffusivity
                total = (-6.0 * gain) * mid[f]
                push = None
                for factor, (side, axis, sign, _) in zip(factors, sides):
                    total = total + (factor if f < 3 else factor - shift) * side[f]
                    if axis == f:
                        term = (sign * 0.5) * side[3]
                        push = term if push is None else push + term
                if push is not None:
                    total = total + push
            rates.append(total + forcing)
        share_of = weigh(stage)
        if rim is not None:
            for f, value in enumerate(reach(mid, 1.0 if rim else -1.0)):
                rims[rim, f, pl.ds(r0, CHUNK)] = share_of * value
        for f in range(fields):
            at = f * depth + z
            here = pl.ds(r0, CHUNK)
            begin = y1[f, z, pl.ds(pl.multiple_of(r0 + PAD, 8), CHUNK)]
            done = begin if stage == 0 else fine[at, here]
            fine[at, here] = done + share_of * rates[f]
            if stage < 3:
                later = states[stage + 1]
                step = (0.5, 0.5, 1.0)[stage] * time_step
                value = begin + step * rates[f]
                later[f, z, pl.ds(pl.multiple_of(r0 + PAD, 8), CHUNK)] = value

                @pl.when(r0 == 0)
                def _():
                    later[f, z, pl.ds(PAD + rows, PAD)] = value[:PAD]

                @pl.when(r0 == rows - CHUNK)
                def _():
                    later[f, z, pl.ds(0, PAD)] = value[CHUNK - PAD :]

    for stage in range(4):
        state = states[stage]

        def inner(i, carry):
            z = 1 + i // chunks
            r0 = pl.multiple_of(lax.rem(i, chunks) * CHUNK, CHUNK)
            at = pl.ds(pl.multiple_of(r0 + PAD, 8), CHUNK)
            update(stage, z, r0, lambda f: state[f, z - 1, at], lambda f: state[f, z + 1, at])
            return carry

        def edge(c, carry):
            r0 = pl.multiple_of(c * CHUNK, CHUNK)
            at = pl.ds(pl.multiple_of(r0 + PAD, 8), CHUNK)
            for side in range(2):
                if stage == 3:
                    if side == 0:
                        update(stage, 0, r0, None, lambda f: state[f, 1, at], side)
                    else:
                        update(stage, depth - 1, r0, lambda f: state[f, depth - 2, at], None, side)
                    continue
                halo_copy(stage, side, c).wait_recv()
                here = lambda f: halo[stage, side, f, pl.ds(r0, CHUNK)]
                if side == 0:
                    update(stage, 0, r0, here, lambda f: state[f, 1, at])
                else:
                    update(stage, depth - 1, r0, lambda f: state[f, depth - 2, at], here)
                if stage < 2:
                    halo_copy(stage + 1, 1 - side, c).start()
            return carry

        lax.fori_loop(0, (depth - 2) * chunks, inner, 0)
        lax.fori_loop(0, chunks, edge, 0)
        for level in range(levels):
            if min(level, 2) == stage:
                heard(level)
                if level + 1 < levels:
                    relay(level + 1)

    spec = transform(
        paired(lambda l: fine[l]) + [(*rim_place(f), rims[1, f], rims[0, f]) for f in range(fields)],
        groups + 1,
    )

    def jump_copy(index, tile, target):
        return pltpu.make_async_remote_copy(
            src_ref=jumps.at[tile],
            dst_ref=gathered.at[index],
            send_sem=jump_send,
            recv_sem=jump_recv,
            device_id=target,
            device_id_type=MESH,
        )

    def others(act):
        def body(dt, carry):
            t = n + dt
            t = jnp.where(t >= times_n, t - times_n, t)
            for ds in reversed(range(spaces)):
                where = s + ds
                where = jnp.where(where >= spaces, where - spaces, where)
                run = functools.partial(act, t, where)
                if ds == 0:
                    pl.when(dt > 0)(run)
                else:
                    run()
            return carry

        if times_n <= 8:
            for dt in sorted(range(times_n), key=lambda d: -min(d, times_n - d)):
                body(dt, 0)
        else:
            lax.fori_loop(0, times_n, body, 0)

    sent = lambda t, where: jump_copy(
        n * spaces + s, lax.rem(t, pair) * spaces + where, (t, where)
    )

    @pl.when(n < times_n - 1)
    def _():
        ahead_copy.wait_recv()
        jumps[...] = spec - ahead[...]
        others(lambda t, where: sent(t, where).start())
        gathered[n * spaces + s] = jumps[me]

    def send_last(c, carry):
        for side in range(2):
            halo_copy(3, side, c).start()
        return carry

    def finish_edge(c, carry):
        here = pl.ds(pl.multiple_of(c * CHUNK, CHUNK), CHUNK)
        for side in range(2):
            halo_copy(3, side, c).wait_recv()
            layer = [halo[3, side, f, here] for f in range(fields)]
            for f, value in enumerate(reach(layer, -1.0 if side else 1.0)):
                at = f * depth + side * (depth - 1)
                fine[at, here] = fine[at, here] + weigh(3) * value
        return carry

    lax.fori_loop(0, chunks, send_last, 0)

    def settle(ref, count, sem):
        held = ref if count is None else ref.at[pl.ds(0, count)]
        pltpu.make_async_copy(held, held, sem).wait()

    pl.when(n < times_n - 1)(
        lambda: settle(gathered, (times_n - 1) * spaces - 1, jump_recv)
    )
    pl.when(n == times_n - 1)(lambda: settle(gathered, (times_n - 1) * spaces, jump_recv))

    width = depth * spaces * keep_x
    half = depth * slot
    steps = times_n - 1
    part = lax.broadcasted_iota(jnp.int32, (1, LANES), 1) // half

    def turned(values, move):
        move = move % LANES
        return pltpu.roll(values, move, 1) if move else values

    def joined(blocks):
        total = None
        for i, block in enumerate(blocks):
            total = block if total is None else jnp.where(part == i, block, total)
        return total

    place_of = lax.rem(lax.broadcasted_iota(jnp.int32, (1, 1, LANES), 2), half) // slot
    line_of = lax.broadcasted_iota(jnp.int32, (1, height, 1), 1) // share
    raw = [
        jnp.stack([gathered[m * spaces + k] for m in range(steps)], axis=0) for k in range(spaces)
    ]

    def slid(values, move, axis):
        move = move % values.shape[axis]
        return pltpu.roll(values, move, axis) if move else values

    def rim_values(values):
        total = None
        for f in range(0, fields, per):
            g, at = rim_place(f)
            moved = slid(slid(values, -(at - f % per * depth) * slot, 2), (f // per - g) * share, 1)
            total = moved if total is None else jnp.where(line_of == f // per, moved, total)
        return total

    reached = [rim_values(values) for values in raw]
    slabs = []
    for k in range(spaces):
        from_below = jnp.where(place_of == 0, reached[(k - 1) % spaces], 0.0)
        from_above = slid(reached[(k + 1) % spaces], (depth - 2) * slot, 2)
        from_above = jnp.where(place_of == depth - 1, from_above, 0.0)
        slabs.append((raw[k] + (from_below + from_above)).reshape(steps * height, LANES))
    lined = [
        jnp.concatenate(
            [
                joined([turned(slabs[at + i], (i - fp) * half) for i in range(per)])
                for at in range(0, spaces, per)
            ],
            axis=1,
        )
        for fp in range(per)
    ]
    fresh = times(jnp.concatenate(lined, axis=0), zf)
    gains = [(sym[me, fp, 0], sym[me, fp, 1]) for fp in range(per)]
    weight = jnp.where(lax.rem(lane, keep_x) == 0, 1.0, 2.0)
    zero = jnp.zeros((height, width), jnp.float32)
    held = [(zero, zero)] * per
    sizes_of = [jnp.zeros((1, LANES), jnp.float32)]
    corrections[0] = jnp.zeros((per, height, 2 * width), jnp.float32)
    for m in range(steps):
        size = None
        for fp in range(per):
            at = (fp * steps + m) * height
            re = held[fp][0] + fresh[at : at + height, :width]
            im = held[fp][1] + fresh[at : at + height, width:]
            gain_re, gain_im = gains[fp]
            re, im = gain_re * re - gain_im * im, gain_re * im + gain_im * re
            held[fp] = (re, im)
            corrections[m + 1, fp, :, :width] = re
            corrections[m + 1, fp, :, width:] = im
            square = re * re + im * im
            size = square if size is None else size + square
        sizes_of.append(jnp.sum(size * weight, axis=0, keepdims=True))
    back = times(
        jnp.concatenate([corrections[base + j, fp] for j in range(pair) for fp in range(per)], axis=0), zi
    )
    column = jnp.sum(jnp.concatenate(sizes_of, axis=0), axis=1, keepdims=True)
    shape = (times_n, LANES)
    diagonal = lax.broadcasted_iota(jnp.int32, shape, 0) == lax.broadcasted_iota(jnp.int32, shape, 1)
    squares = jnp.sum(jnp.where(diagonal, column, 0.0), axis=0, keepdims=True) * (
        1.0 / (depth * spaces * rows * cols)
    )
    last = lax.broadcasted_iota(jnp.int32, (height, LANES), 0) == used
    for j in range(pair):
        for k in range(spaces):
            at = k * half
            tile, inside = at // LANES * LANES, at % LANES
            piece = joined(
                [
                    turned(
                        back[(j * per + fp) * height : (j * per + fp + 1) * height, tile : tile + LANES],
                        fp * half - inside,
                    )
                    for fp in range(per)
                ]
            )
            pieces[j * spaces + k] = jnp.where(last, squares, piece)

    def mode_copy(dj, dk):
        j, k = lax.rem(place + dj, pair), lax.rem(s + dk, spaces)
        return pltpu.make_async_remote_copy(
            src_ref=pieces.at[j * spaces + k],
            dst_ref=modes.at[me],
            send_sem=mode_send,
            recv_sem=mode_recv,
            device_id=(base + j, k),
            device_id_type=MESH,
        )

    sharers = [(dj, dk) for dj in reversed(range(pair)) for dk in reversed(range(spaces)) if dj + dk]
    for dj, dk in sharers:
        mode_copy(dj, dk).start()
    modes[me] = pieces[me]
    lax.fori_loop(0, chunks, finish_edge, 0)
    settle(modes, owners - 1, mode_recv)
    found = modes[...].reshape(owners * height, LANES)
    total = None
    for o in range(owners):
        row = found[o * height + used : o * height + used + 1]
        total = row if total is None else total + row
    cells = fields * depth * spaces * rows * cols

    def norm(values, count):
        value = jnp.sqrt(jnp.sum(values, axis=1, keepdims=True) * (1.0 / count) + epsilon)
        return jnp.broadcast_to(value, (1, LANES))

    norms[0] = norm(jnp.where(lane == n, total, 0.0), cells)
    norms[1] = norm(total, cells * times_n)

    planes = under(yi, jnp.concatenate([found, swapped(found)], axis=0))
    for g in range(groups):
        plane = planes[g * rows : (g + 1) * rows]
        count = min(slots, layers - g * slots) // 2
        shifted = [
            plane if p == 0 else pltpu.roll(plane, LANES - 2 * p * slot, 1) for p in range(count)
        ]
        fix = times(jnp.concatenate(shifted, axis=0), xi)
        for p in range(count):
            for i in range(2):
                l = g * slots + 2 * p + i
                ends[l] = fine[l] + fix[p * rows : (p + 1) * rows, i * cols : (i + 1) * cols]

    pl.when(n < times_n - 1)(lambda: settle(gathered, times_n * spaces - 1, jump_send))

    @pl.when(n > 0)
    def _():
        ahead_copy.wait_send()

    settle(halo, None, halo_send)
    settle(modes, owners - 1, mode_send)


def finish(ends, norms, out, slice_out, total_out, slice_held, total_held, sems):
    copies = [pltpu.make_async_copy(ends, out, sems.at[0])]
    copies[0].start()
    for i, (held, to) in enumerate(((slice_held, slice_out), (total_held, total_out))):
        held[0] = norms[i, 0, 0]
        copies.append(pltpu.make_async_copy(held, to, sems.at[1 + i]))
        copies[-1].start()
    for copy in copies:
        copy.wait()


def solution(mesh):
    times_n, spaces = mesh.shape["tm"], mesh.shape["space"]

    def step(starts, source):
        _, fields, depth, rows, cols = starts.shape
        matrices, symbol = tables(fields, depth, rows, cols, times_n, spaces)
        constants = [halves(t) for t in matrices] + [symbol]
        operands = [starts, source] + [jnp.asarray(c) for c in constants]
        _, pair, owners, _, _, height = layout(fields, depth, rows, cols, times_n, spaces)
        slot = cols // 16 * 2
        per = LANES // (slot * depth)
        chunks = rows // CHUNK
        devices = times_n * spaces
        state = pltpu.VMEM((fields, depth, rows + 2 * PAD, cols), jnp.float32)
        dma = pltpu.SemaphoreType.DMA
        layer_shape = (fields * depth, rows, cols)
        ends, norms = pl.pallas_call(
            functools.partial(kernel, (times_n, spaces, fields, depth, rows, cols)),
            out_shape=(
                pltpu.VMEM(layer_shape, jnp.float32),
                pltpu.VMEM((2, 1, LANES), jnp.float32),
            ),
            in_specs=[pl.BlockSpec(memory_space=pltpu.HBM)] * (2 + len(constants)),
            out_specs=(
                pl.BlockSpec(memory_space=pltpu.VMEM),
                pl.BlockSpec(memory_space=pltpu.VMEM),
            ),
            scratch_shapes=[
                state, state, state, state,
                pltpu.VMEM((fields, depth, rows, cols), jnp.float32),
                pltpu.VMEM(layer_shape, jnp.float32),
                pltpu.VMEM((2, fields, rows, cols), jnp.float32),
                pltpu.VMEM((4, 2, fields, rows, cols), jnp.float32),
                *[pltpu.VMEM(c.shape, c.dtype) for c in constants],
                *[pltpu.VMEM((owners, height, LANES), jnp.float32)] * 3,
                pltpu.VMEM((devices, height, LANES), jnp.float32),
                pltpu.VMEM((times_n, per, height, depth * spaces * slot), jnp.float32),
                *[pltpu.VMEM((owners, height, LANES), jnp.float32)] * 2,
                dma((6,)), dma((len(constants),)),
                dma, dma((2, 2, chunks)), dma((2,)), dma, dma, dma, dma,
                pltpu.SemaphoreType.REGULAR(((times_n - 1).bit_length(), 2)),
            ],
            compiler_params=pltpu.CompilerParams(
                collective_id=0, has_side_effects=True, vmem_limit_bytes=VMEM_BYTES
            ),
        )(*[pltpu.with_memory_space_constraint(a, pltpu.HBM) for a in operands])
        out, slice_norm, total_norm = pl.pallas_call(
            finish,
            out_shape=(
                jax.ShapeDtypeStruct(layer_shape, jnp.float32),
                jax.ShapeDtypeStruct((1,), jnp.float32),
                jax.ShapeDtypeStruct((1,), jnp.float32),
            ),
            in_specs=[pl.BlockSpec(memory_space=pltpu.VMEM)] * 2,
            out_specs=[pl.BlockSpec(memory_space=pltpu.HBM)] * 3,
            scratch_shapes=[
                pltpu.SMEM((1,), jnp.float32), pltpu.SMEM((1,), jnp.float32), dma((3,)),
            ],
            compiler_params=pltpu.CompilerParams(vmem_limit_bytes=VMEM_BYTES // 2),
        )(
            pltpu.with_memory_space_constraint(ends, pltpu.VMEM),
            pltpu.with_memory_space_constraint(norms, pltpu.VMEM),
        )
        return out.reshape(starts.shape), slice_norm, total_norm

    return jax.shard_map(
        step,
        mesh=mesh,
        in_specs=(P("tm", None, "space", None, None), P(None, "space", None, None)),
        out_specs=(P("tm", None, "space", None, None), P("tm"), P()),
        check_vma=False,
    )
```

```python
import functools
import math

import jax
import jax.numpy as jnp
import numpy as np
from jax import lax
from jax.experimental import pallas as pl
from jax.experimental.pallas import tpu as pltpu
from jax.sharding import PartitionSpec as P

viscosity = 0.08
diffusivity = 0.05
compress_rate = 0.25
time_step = 0.5
diffusion_number = 0.08
advect_xaxis = 0.2
advect_yaxis = 0.15
advect_zaxis = 0.1
epsilon = 1e-06
MESH = pl.DeviceIdType.MESH
PAD = 8
CHUNK = 16
LANES = 128
SUBLANES = 8
PAIR = 2
VMEM_BYTES = 32 * 1024 * 1024


def layout(fields, depth, rows, cols, times_n, spaces):
    keep_y, keep_x = rows // 8, cols // 16
    groups = -(-fields * depth // (LANES // (2 * keep_x)))
    pair = PAIR if times_n % PAIR == 0 else 1
    owners = spaces * pair
    share = 2 * keep_y // owners
    used = groups * share
    height = -(-max(used + 1, used + share) // SUBLANES) * SUBLANES
    return groups, pair, owners, share, used, height


def tables(fields, depth, rows, cols, times_n, spaces):
    groups, pair, owners, share, used, height = layout(fields, depth, rows, cols, times_n, spaces)
    keep_y, keep_x = rows // 8, cols // 16
    slot = 2 * keep_x
    full = depth * spaces
    k = np.arange(keep_x)
    x = np.arange(cols)
    ax = 2 * math.pi / cols * ((x[:, None] * k[None, :]) % cols)
    weight = np.where(k == 0, 1.0, 2.0) / (full * rows * cols)
    xf = np.zeros((2 * cols, LANES))
    xi = np.zeros((LANES, 2 * cols))
    for i in range(2):
        at = i * slot
        xf[i * cols : (i + 1) * cols, at : at + keep_x] = np.cos(ax)
        xf[i * cols : (i + 1) * cols, at + keep_x : at + slot] = -np.sin(ax)
        xi[at : at + keep_x, i * cols : (i + 1) * cols] = (np.cos(ax) * weight).T
        xi[at + keep_x : at + slot, i * cols : (i + 1) * cols] = (-np.sin(ax) * weight).T
    ky = np.arange(2 * keep_y)
    ky = np.where(ky < keep_y, ky, ky - 2 * keep_y)
    y = np.arange(rows)
    ay = 2 * math.pi / rows * ((ky[:, None] * y[None, :]) % rows)
    kz = np.arange(full)
    width = full * keep_x
    block = owners * height
    yf = np.zeros((block, (groups + 1) * 2 * rows))
    yi = np.zeros((groups * rows, 2 * block))
    for g in range(groups + 1):
        for at in range(2 * keep_y):
            row = at // share * height + g * share + at % share
            yf[row, g * 2 * rows : (g + 1) * 2 * rows] = np.concatenate([np.cos(ay[at]), np.sin(ay[at])])
    for g in range(groups):
        for at in range(2 * keep_y):
            row = at // share * height + g * share + at % share
            yi[g * rows : (g + 1) * rows, row] = np.cos(ay[at])
            yi[g * rows : (g + 1) * rows, block + row] = -np.sin(ay[at])
    zf = np.zeros((full * slot, 2 * width))
    for z in range(full):
        a = 2 * math.pi / full * ((kz * z) % full)
        for kk in range(keep_x):
            row = z * slot + kk
            re = kz * keep_x + kk
            im = re + width
            zf[row, re] = np.cos(a)
            zf[row, im] = -np.sin(a)
            zf[row + keep_x, re] = np.sin(a)
            zf[row + keep_x, im] = np.cos(a)
    zi = np.zeros((2 * width, full * slot))
    for z in range(full):
        a = 2 * math.pi / full * ((kz * z) % full)
        for kk in range(keep_x):
            re = kz * keep_x + kk
            im = re + width
            col = z * slot + kk
            zi[re, col] = np.cos(a)
            zi[im, col] = -np.sin(a)
            zi[re, col + keep_x] = np.sin(a)
            zi[im, col + keep_x] = np.cos(a)
    tz = 2 * math.pi / full * kz
    ty = 2 * math.pi / rows * ky
    tx = 2 * math.pi / cols * k
    live = (ky != -keep_y).astype(np.float64)[:, None, None]
    real = 1.0 + diffusion_number * (
        (2 * np.cos(ty) - 2)[:, None, None]
        + (2 * np.cos(tz) - 2)[None, :, None]
        + (2 * np.cos(tx) - 2)[None, None, :]
    )
    imag = -(
        advect_yaxis * np.sin(ty)[:, None, None]
        + advect_zaxis * np.sin(tz)[None, :, None]
        + advect_xaxis * np.sin(tx)[None, None, :]
    )
    symbol = (real + 1j * imag) * live
    symbol = symbol.reshape(owners, share, width)
    per = LANES // (slot * depth)
    gains = np.zeros((owners, per, 2, height, width), np.float32)
    for f in range(fields):
        at = f // per * share
        gains[:, f % per, 0, at : at + share] = symbol.real
        gains[:, f % per, 1, at : at + share] = symbol.imag
    held = {
        "xf": halves(xf, 1), "yf": halves(yf, 1), "zf": halves(zf, 1), "zi": halves(zi, 1),
        "yi": halves(yi, 1, True), "xi": halves(xi, 0, True),
    }
    places, at, blocks = {}, 0, []
    for name, table in held.items():
        height, wide = table.shape
        places[name] = (at, height, wide // LANES)
        blocks += [table[:, i : i + LANES] for i in range(0, wide, LANES)]
        at += height * (wide // LANES)
    return places, np.concatenate(blocks, axis=0), gains


def halves(table, axis, twice=False):
    high = table.astype(jnp.bfloat16)
    low = (table - high.astype(np.float64)).astype(jnp.bfloat16)
    return np.concatenate([high, high, low] if twice else [high, low], axis=axis)


def split(values):
    high = values.astype(jnp.bfloat16)
    return high, (values - high.astype(jnp.float32)).astype(jnp.bfloat16)


def dot(a, b):
    return jnp.dot(a, b, preferred_element_type=jnp.float32)


def times(values, table):
    high, low = split(values)
    wide = table.shape[1] // 2
    if wide > LANES:
        return dot(high, table[:, :wide]) + dot(low, table[:, :wide]) + dot(high, table[:, wide:])
    both = dot(high, table)
    return both[:, :wide] + dot(low, table[:, :wide]) + both[:, wide:]


def times_deep(values, table):
    high, low = split(values)
    deep = 2 * values.shape[1]
    return dot(jnp.concatenate([high, low], axis=1), table[:deep]) + dot(high, table[deep:])


def under(table, values):
    high, low = split(values)
    deep, wide = values.shape
    both = dot(table[:, :deep], jnp.concatenate([high, low], axis=1))
    return both[:, :wide] + both[:, wide:] + dot(table[:, deep:], high)


def under_deep(table, values):
    high, low = split(values)
    deep = 2 * values.shape[0]
    return dot(table[:, :deep], jnp.concatenate([high, low], axis=0)) + dot(table[:, deep:], high)


def kernel(
    sizes, places, starts, source, tables_h, sym_h,
    ends, norms,
    y1, y2, y3, y4, src, fine, rims, late, begun, table, sym,
    own, jumps, ahead, gathered, corrections, pieces, modes,
    load_sem, table_sem, halo_send, halo_recv, ahead_sems, jump_send, jump_recv,
    mode_send, mode_recv, relays,
):
    times_n, spaces, fields, depth, rows, cols = sizes
    keep_y, keep_x = rows // 8, cols // 16
    slot = 2 * keep_x
    layers = fields * depth
    slots = LANES // slot
    per = LANES // (slot * depth)
    groups, pair, owners, share, used, height = layout(fields, depth, rows, cols, times_n, spaces)
    chunks = rows // CHUNK
    n = lax.axis_index("tm")
    s = lax.axis_index("space")
    place = lax.rem(n, pair)
    me = place * spaces + s
    base = n - place
    up = lax.rem(s + 1, spaces)
    down = lax.rem(s + spaces - 1, spaces)

    barrier = pltpu.get_barrier_semaphore()

    def near(distance, act):
        for side, target in enumerate((n - distance, n + distance)):
            pl.when((target >= 0) & (target < times_n))(functools.partial(act, side, target))

    def enter(target, where):
        pl.semaphore_signal(barrier, inc=1, device_id=(target, where), device_id_type=MESH)

    for offset in range(1, spaces):
        enter(n, lax.rem(s + offset, spaces))
    near(1, lambda side, target: enter(target, s))
    edges = [
        pltpu.make_async_copy(
            starts.at[0, :, z], y1.at[:, z + 1, pl.ds(PAD, rows)], load_sem.at[min(z, 1)]
        )
        for z in (0, depth - 1)
    ]
    for copy in edges:
        copy.start()
    loads = [
        pltpu.make_async_copy(
            starts.at[0, :, pl.ds(1, depth - 2)],
            y1.at[:, pl.ds(2, depth - 2), pl.ds(PAD, rows)],
            load_sem.at[2],
        ),
        pltpu.make_async_copy(tables_h, table, table_sem.at[0]),
        pltpu.make_async_copy(source, src, load_sem.at[3]),
        pltpu.make_async_copy(sym_h, sym, table_sem.at[1]),
    ]
    for copy in edges:
        copy.wait()
    beside = jnp.where(n > 0, 1, 0) + jnp.where(n < times_n - 1, 1, 0)
    pl.semaphore_wait(barrier, spaces - 1 + beside)

    def relay(level):
        near(
            2**level,
            lambda side, target: pl.semaphore_signal(
                relays.at[level, side], inc=1, device_id=(target, s), device_id_type=MESH
            ),
        )

    def heard(level):
        near(2**level, lambda side, target: pl.semaphore_wait(relays.at[level, 1 - side], 1))

    levels = (times_n - 1).bit_length()

    states = [y1, y2, y3, y4]

    parity = lax.rem(s, 2)
    far_to, near_to = jnp.where(parity == 0, down, up), jnp.where(parity == 0, up, down)
    far_z = jnp.where(parity == 0, 1, depth)
    near_z = depth + 1 - far_z
    step = 1 - 2 * parity
    far_halo, near_halo = far_z - step, near_z + step

    def settle(held, sem):
        pltpu.make_async_copy(held, held, sem).wait()

    def span(chunk):
        return pl.ds(pl.multiple_of(PAD + chunk * CHUNK, PAD), CHUNK)

    def send(src_ref, dst_ref, stage, index, target):
        pltpu.make_async_remote_copy(
            src_ref=src_ref,
            dst_ref=dst_ref,
            send_sem=halo_send.at[stage],
            recv_sem=halo_recv.at[stage % 2, index],
            device_id=(n, target),
            device_id_type=MESH,
        ).start()

    def send_near(stage):
        here, state = pl.ds(PAD, rows), states[stage]
        send(state.at[:, near_z, here], state.at[:, depth + 1 - near_halo, here], stage, 0, near_to)

    def send_far(stage, chunk):
        here, state = span(chunk), states[stage]
        send(
            state.at[:, far_z, here], state.at[:, depth + 1 - far_halo, here], stage, 1 + chunk, far_to
        )

    def send_first(c, carry):
        send_far(0, c)
        return carry

    lax.fori_loop(0, chunks, send_first, 0)
    send_near(0)
    for copy in loads:
        copy.start()
    relay(0)

    lane = lax.broadcasted_iota(jnp.int32, (1, LANES), 1)
    first = lax.rem(lane, slot) < keep_x

    def swapped(values):
        return jnp.where(
            first, pltpu.roll(values, LANES - keep_x, 1), -pltpu.roll(values, keep_x, 1)
        )

    def entry(name):
        at, height_of, wide = places[name]
        return jnp.concatenate(
            [table[pl.ds(at + i * height_of, height_of)] for i in range(wide)], axis=1
        )

    def pack(pairs, result):
        stacked = jnp.concatenate(
            [jnp.concatenate([left, right], axis=1) for _, _, left, right in pairs], axis=0
        )
        packed = times(stacked, entry("xf"))
        result = list(result)
        for i, (g, at, _, _) in enumerate(pairs):
            piece = packed[i * rows : (i + 1) * rows]
            if not (isinstance(at, int) and at == 0):
                piece = pltpu.roll(piece, at * slot, 1)
            result[g] = piece if result[g] is None else result[g] + piece
        return result

    def transform(result):
        both = jnp.concatenate([part for t in result for part in (t, swapped(t))], axis=0)
        at, tall, wide = places["yf"]
        blocks = wide // 2
        held = len(result) * 2 * rows // LANES
        columns = [i * blocks + j for i in range(2) for j in range(held)]
        matrix = jnp.concatenate([table[pl.ds(at + i * tall, tall)] for i in columns], axis=1)
        return under(matrix, both).reshape(owners, height, LANES)

    def paired(layer_of, first_of, count):
        return [
            (f // per, f % per * depth + z, layer_of(f, z), layer_of(f, z + 1))
            for f in range(fields)
            for z in (first_of + i for i in range(0, count, 2))
        ]

    def rim_place(f):
        if f // per == groups - 1 and fields % per:
            return groups - 1, fields % per * depth
        return groups, f % per * depth + 2 * (f // per)

    loads[0].wait()
    loads[1].wait()
    for f in range(fields):
        for z in range(1, depth + 1):
            y1[f, z, pl.ds(0, PAD)] = y1[f, z, pl.ds(rows, PAD)]
            y1[f, z, pl.ds(PAD + rows, PAD)] = y1[f, z, pl.ds(PAD, PAD)]
        for z in (0, depth + 1):
            y4[f, z, pl.ds(PAD, rows)] = jnp.zeros((rows, cols), jnp.float32)

    own[...] = transform(
        pack(paired(lambda f, z: y1[f, z + 1, pl.ds(PAD, rows)], 0, depth), [None] * groups)
    )
    ahead_copy = pltpu.make_async_remote_copy(
        src_ref=own,
        dst_ref=ahead,
        send_sem=ahead_sems.at[0],
        recv_sem=ahead_sems.at[1],
        device_id=(jnp.maximum(n - 1, 0), s),
        device_id_type=MESH,
    )

    @pl.when(n > 0)
    def _():
        ahead_copy.start()

    shift = viscosity - diffusivity

    def reach(layer, sign):
        factor = (viscosity + sign * 0.5 * advect_zaxis) + (sign * 0.5) * layer[2]
        result = [factor * layer[f] for f in range(3)]
        result[2] = result[2] + (sign * 0.5) * layer[3]
        return result + [(sign * 0.5 * compress_rate) * layer[2], (factor - shift) * layer[4]]

    def weigh(stage):
        return time_step / 6.0 * (1.0, 2.0, 2.0, 1.0)[stage]

    loads[2].wait()
    loads[3].wait()

    def update(stage, z, r0):
        state = states[stage]
        mid, xm, xp, ym, yp = [], [], [], [], []
        rolled = CHUNK + 2 * PAD
        for f in range(fields):
            wide = state[f, z, pl.ds(r0, rolled)]
            centre = wide[PAD : PAD + CHUNK]
            mid.append(centre)
            ym.append(pltpu.roll(wide, 1, 0)[PAD : PAD + CHUNK])
            yp.append(pltpu.roll(wide, rolled - 1, 0)[PAD : PAD + CHUNK])
            xm.append(pltpu.roll(centre, 1, 1))
            xp.append(pltpu.roll(centre, cols - 1, 1))
        sides = [(xm, 0, 1.0, advect_xaxis), (xp, 0, -1.0, advect_xaxis)]
        sides += [(ym, 1, 1.0, advect_yaxis), (yp, 1, -1.0, advect_yaxis)]
        here = pl.ds(pl.multiple_of(r0 + PAD, PAD), CHUNK)
        for offset, sign in ((-1, 1.0), (1, -1.0)):
            held = [state[f, z + offset, here] for f in range(fields)]
            sides.append((held, 2, sign, advect_zaxis))
        factors = [
            (viscosity + sign * 0.5 * speed) + (sign * 0.5) * side[axis]
            for side, axis, sign, speed in sides
        ]
        rates = []
        for f in range(fields):
            forcing = src[f, z - 1, pl.ds(r0, CHUNK)]
            if f == 3:
                total = None
                for side, axis, sign, _ in sides:
                    if total is None:
                        total = side[axis]
                    else:
                        total = total + side[axis] if sign > 0 else total - side[axis]
                total = total * (0.5 * compress_rate)
            else:
                gain = viscosity if f < 3 else diffusivity
                total = (-6.0 * gain) * mid[f]
                push = None
                for factor, (side, axis, sign, _) in zip(factors, sides):
                    total = total + (factor if f < 3 else factor - shift) * side[f]
                    if axis == f:
                        term = (sign * 0.5) * side[3]
                        push = term if push is None else push + term
                if push is not None:
                    total = total + push
            rates.append(total + forcing)
        share_of = weigh(stage)
        for f in range(fields):
            at = f * depth + z - 1
            here = pl.ds(r0, CHUNK)
            begin = y1[f, z, pl.ds(pl.multiple_of(r0 + PAD, 8), CHUNK)]
            done = begin if stage == 0 else fine[at, here]
            fine[at, here] = done + share_of * rates[f]
            if stage < 3:
                later = states[stage + 1]
                step = (0.5, 0.5, 1.0)[stage] * time_step
                value = begin + step * rates[f]
                later[f, z, pl.ds(pl.multiple_of(r0 + PAD, 8), CHUNK)] = value

                @pl.when(r0 == 0)
                def _():
                    later[f, z, pl.ds(PAD + rows, PAD)] = value[:PAD]

                @pl.when(r0 == rows - CHUNK)
                def _():
                    later[f, z, pl.ds(0, PAD)] = value[CHUNK - PAD :]

    def sweep(act):
        def body(c, carry):
            act(c, pl.multiple_of(c * CHUNK, CHUNK))
            return carry

        lax.fori_loop(0, chunks, body, 0)

    def rim(z, r0):
        side = jnp.where(z == depth, 1, 0)
        sign = jnp.where(z == depth, 1.0, -1.0)
        layer = [y4[f, z, pl.ds(pl.multiple_of(r0 + PAD, PAD), CHUNK)] for f in range(fields)]
        for f, value in enumerate(reach(layer, sign)):
            rims[side, f, pl.ds(r0, CHUNK)] = weigh(3) * value

    early = [near_z - step * k for k in range(depth - 2)]
    late_layers = [far_z, far_z + step]
    early_first = jnp.where(parity == 0, 2, 0)
    late_first = jnp.where(parity == 0, 0, depth - 2)

    def settled(f, z):
        return fine[f * depth + z]

    for stage in range(3):
        state = states[stage]

        def inner(c, r0):
            for z in range(2, depth):
                update(stage, z, r0)

        def edge(c, r0):
            settle(state.at[:, far_halo, span(c)], halo_recv.at[stage % 2, 1 + c])
            update(stage, far_z, r0)
            if stage < 2:
                send_far(stage + 1, c)

        sweep(inner)
        settle(state.at[:, near_halo, pl.ds(PAD, rows)], halo_recv.at[stage % 2, 0])
        sweep(lambda c, r0: update(stage, near_z, r0))
        if stage < 2:
            send_near(stage + 1)
        else:

            def ready(c, r0):
                for z in early:
                    update(3, z, r0)
                rim(near_z, r0)

            sweep(ready)
            result = pack(paired(settled, early_first, depth - 2), [None] * groups)
            for g in range(groups):
                begun[g] = result[g]
        sweep(edge)
        for level in range(levels):
            if min(level, 2) == stage:
                heard(level)
                if level + 1 < levels:
                    relay(level + 1)

    def remaining(c, r0):
        for z in late_layers:
            update(3, z, r0)
        rim(far_z, r0)

    sweep(remaining)
    pairs = paired(settled, late_first, 2)
    pairs += [(*rim_place(f), rims[1, f], rims[0, f]) for f in range(fields)]
    spec = transform(pack(pairs, [begun[g] for g in range(groups)] + [None]))

    def jump_copy(index, tile, target):
        return pltpu.make_async_remote_copy(
            src_ref=jumps.at[tile],
            dst_ref=gathered.at[index],
            send_sem=jump_send,
            recv_sem=jump_recv,
            device_id=target,
            device_id_type=MESH,
        )

    def others(act):
        def body(dt, carry):
            t = n + dt
            t = jnp.where(t >= times_n, t - times_n, t)
            for ds in reversed(range(spaces)):
                where = s + ds
                where = jnp.where(where >= spaces, where - spaces, where)
                run = functools.partial(act, t, where)
                if ds == 0:
                    pl.when(dt > 0)(run)
                else:
                    run()
            return carry

        if times_n <= 8:
            for dt in sorted(range(times_n), key=lambda d: -min(d, times_n - d)):
                body(dt, 0)
        else:
            lax.fori_loop(0, times_n, body, 0)

    sent = lambda t, where: jump_copy(
        n * spaces + s, lax.rem(t, pair) * spaces + where, (t, where)
    )

    @pl.when(n < times_n - 1)
    def _():
        ahead_copy.wait_recv()
        jumps[...] = spec - ahead[...]
        others(lambda t, where: sent(t, where).start())
        gathered[n * spaces + s] = jumps[me]

    whole = pl.ds(PAD, rows)
    send(y4.at[:, far_z, whole], late.at[1 - parity], 3, 1, far_to)
    send(y4.at[:, near_z, whole], late.at[parity], 3, 0, near_to)

    def finish_edge(c, r0):
        here = pl.ds(r0, CHUNK)
        for side in range(2):
            layer = [late[side, f, here] for f in range(fields)]
            for f, value in enumerate(reach(layer, -1.0 if side else 1.0)):
                at = f * depth + side * (depth - 1)
                fine[at, here] = fine[at, here] + weigh(3) * value

    pl.when(n < times_n - 1)(
        lambda: settle(gathered.at[pl.ds(0, (times_n - 1) * spaces - 1)], jump_recv)
    )
    pl.when(n == times_n - 1)(lambda: settle(gathered.at[pl.ds(0, (times_n - 1) * spaces)], jump_recv))

    width = depth * spaces * keep_x
    half = depth * slot
    steps = times_n - 1
    part = lax.broadcasted_iota(jnp.int32, (1, LANES), 1) // half

    def turned(values, move):
        move = move % LANES
        return pltpu.roll(values, move, 1) if move else values

    def joined(blocks):
        total = None
        for i, block in enumerate(blocks):
            total = block if total is None else jnp.where(part == i, block, total)
        return total

    place_of = lax.rem(lax.broadcasted_iota(jnp.int32, (1, 1, LANES), 2), half) // slot
    line_of = lax.broadcasted_iota(jnp.int32, (1, height, 1), 1) // share
    raw = [
        jnp.stack([gathered[m * spaces + k] for m in range(steps)], axis=0) for k in range(spaces)
    ]

    def slid(values, move, axis):
        move = move % values.shape[axis]
        return pltpu.roll(values, move, axis) if move else values

    def rim_values(values):
        total = None
        for f in range(0, fields, per):
            g, at = rim_place(f)
            moved = slid(slid(values, -(at - f % per * depth) * slot, 2), (f // per - g) * share, 1)
            total = moved if total is None else jnp.where(line_of == f // per, moved, total)
        return total

    reached = [rim_values(values) for values in raw]
    slabs = []
    for k in range(spaces):
        from_below = jnp.where(place_of == 0, reached[(k - 1) % spaces], 0.0)
        from_above = slid(reached[(k + 1) % spaces], (depth - 2) * slot, 2)
        from_above = jnp.where(place_of == depth - 1, from_above, 0.0)
        slabs.append((raw[k] + (from_below + from_above)).reshape(steps * height, LANES))
    lined = [
        jnp.concatenate(
            [
                joined([turned(slabs[at + i], (i - fp) * half) for i in range(per)])
                for at in range(0, spaces, per)
            ],
            axis=1,
        )
        for fp in range(per)
    ]
    fresh = times(jnp.concatenate(lined, axis=0), entry("zf"))
    gains = [(sym[me, fp, 0], sym[me, fp, 1]) for fp in range(per)]
    weight = jnp.where(lax.rem(lane, keep_x) == 0, 1.0, 2.0)
    zero = jnp.zeros((height, width), jnp.float32)
    held = [(zero, zero)] * per
    sizes_of = [jnp.zeros((1, LANES), jnp.float32)]
    corrections[0] = jnp.zeros((per, height, 2 * width), jnp.float32)
    for m in range(steps):
        size = None
        for fp in range(per):
            at = (fp * steps + m) * height
            re = held[fp][0] + fresh[at : at + height, :width]
            im = held[fp][1] + fresh[at : at + height, width:]
            gain_re, gain_im = gains[fp]
            re, im = gain_re * re - gain_im * im, gain_re * im + gain_im * re
            held[fp] = (re, im)
            corrections[m + 1, fp, :, :width] = re
            corrections[m + 1, fp, :, width:] = im
            square = re * re + im * im
            size = square if size is None else size + square
        sizes_of.append(jnp.sum(size * weight, axis=0, keepdims=True))
    back = times(
        jnp.concatenate([corrections[base + j, fp] for j in range(pair) for fp in range(per)], axis=0),
        entry("zi"),
    )
    column = jnp.sum(jnp.concatenate(sizes_of, axis=0), axis=1, keepdims=True)
    shape = (times_n, LANES)
    diagonal = lax.broadcasted_iota(jnp.int32, shape, 0) == lax.broadcasted_iota(jnp.int32, shape, 1)
    squares = jnp.sum(jnp.where(diagonal, column, 0.0), axis=0, keepdims=True) * (
        1.0 / (depth * spaces * rows * cols)
    )
    last = lax.broadcasted_iota(jnp.int32, (height, LANES), 0) == used
    for j in range(pair):
        for k in range(spaces):
            at = k * half
            tile, inside = at // LANES * LANES, at % LANES
            piece = joined(
                [
                    turned(
                        back[(j * per + fp) * height : (j * per + fp + 1) * height, tile : tile + LANES],
                        fp * half - inside,
                    )
                    for fp in range(per)
                ]
            )
            pieces[j * spaces + k] = jnp.where(last, squares, piece)

    def mode_copy(dj, dk):
        j, k = lax.rem(place + dj, pair), lax.rem(s + dk, spaces)
        return pltpu.make_async_remote_copy(
            src_ref=pieces.at[j * spaces + k],
            dst_ref=modes.at[me],
            send_sem=mode_send,
            recv_sem=mode_recv,
            device_id=(base + j, k),
            device_id_type=MESH,
        )

    sharers = [(dj, dk) for dj in reversed(range(pair)) for dk in reversed(range(spaces)) if dj + dk]
    for dj, dk in sharers:
        mode_copy(dj, dk).start()
    modes[me] = pieces[me]
    settle(late.at[parity], halo_recv.at[1, 1])
    settle(late.at[1 - parity], halo_recv.at[1, 0])
    sweep(finish_edge)
    settle(modes.at[pl.ds(0, owners - 1)], mode_recv)
    found = modes[...].reshape(owners * height, LANES)
    total = None
    for o in range(owners):
        row = found[o * height + used : o * height + used + 1]
        total = row if total is None else total + row
    cells = fields * depth * spaces * rows * cols

    def norm(values, count):
        value = jnp.sqrt(jnp.sum(values, axis=1, keepdims=True) * (1.0 / count) + epsilon)
        return jnp.broadcast_to(value, (1, LANES))

    norms[0] = norm(jnp.where(lane == n, total, 0.0), cells)
    norms[1] = norm(total, cells * times_n)

    planes = under_deep(entry("yi"), jnp.concatenate([found, swapped(found)], axis=0))
    for g in range(groups):
        plane = planes[g * rows : (g + 1) * rows]
        count = min(slots, layers - g * slots) // 2
        shifted = [
            plane if p == 0 else pltpu.roll(plane, LANES - 2 * p * slot, 1) for p in range(count)
        ]
        fix = times_deep(jnp.concatenate(shifted, axis=0), entry("xi"))
        for p in range(count):
            for i in range(2):
                l = g * slots + 2 * p + i
                ends[l] = fine[l] + fix[p * rows : (p + 1) * rows, i * cols : (i + 1) * cols]

    pl.when(n < times_n - 1)(lambda: settle(gathered.at[pl.ds(0, times_n * spaces - 1)], jump_send))

    @pl.when(n > 0)
    def _():
        ahead_copy.wait_send()

    for stage in range(4):
        settle(states[stage].at[:, pl.ds(0, 2), pl.ds(PAD, rows)], halo_send.at[stage])
    settle(modes.at[pl.ds(0, owners - 1)], mode_send)


def finish(ends, norms, out, slice_out, total_out, slice_held, total_held, sems):
    copies = [pltpu.make_async_copy(ends, out, sems.at[0])]
    copies[0].start()
    for i, (held, to) in enumerate(((slice_held, slice_out), (total_held, total_out))):
        held[0] = norms[i, 0, 0]
        copies.append(pltpu.make_async_copy(held, to, sems.at[1 + i]))
        copies[-1].start()
    for copy in copies:
        copy.wait()


def solution(mesh):
    times_n, spaces = mesh.shape["tm"], mesh.shape["space"]

    def step(starts, source):
        _, fields, depth, rows, cols = starts.shape
        places, packed, gains = tables(fields, depth, rows, cols, times_n, spaces)
        constants = [packed, gains]
        operands = [starts, source] + [jnp.asarray(c) for c in constants]
        groups, _, owners, _, _, height = layout(fields, depth, rows, cols, times_n, spaces)
        slot = cols // 16 * 2
        per = LANES // (slot * depth)
        chunks = rows // CHUNK
        devices = times_n * spaces
        state = pltpu.VMEM((fields, depth + 2, rows + 2 * PAD, cols), jnp.float32)
        dma = pltpu.SemaphoreType.DMA
        layer_shape = (fields * depth, rows, cols)
        ends, norms = pl.pallas_call(
            functools.partial(kernel, (times_n, spaces, fields, depth, rows, cols), places),
            out_shape=(
                pltpu.VMEM(layer_shape, jnp.float32),
                pltpu.VMEM((2, 1, LANES), jnp.float32),
            ),
            in_specs=[pl.BlockSpec(memory_space=pltpu.HBM)] * (2 + len(constants)),
            out_specs=(
                pl.BlockSpec(memory_space=pltpu.VMEM),
                pl.BlockSpec(memory_space=pltpu.VMEM),
            ),
            scratch_shapes=[
                state, state, state, state,
                pltpu.VMEM((fields, depth, rows, cols), jnp.float32),
                pltpu.VMEM(layer_shape, jnp.float32),
                pltpu.VMEM((2, fields, rows, cols), jnp.float32),
                pltpu.VMEM((2, fields, rows, cols), jnp.float32),
                pltpu.VMEM((groups, rows, LANES), jnp.float32),
                *[pltpu.VMEM(c.shape, c.dtype) for c in constants],
                *[pltpu.VMEM((owners, height, LANES), jnp.float32)] * 3,
                pltpu.VMEM((devices, height, LANES), jnp.float32),
                pltpu.VMEM((times_n, per, height, depth * spaces * slot), jnp.float32),
                *[pltpu.VMEM((owners, height, LANES), jnp.float32)] * 2,
                dma((4,)), dma((2,)),
                dma((4,)), dma((2, 1 + chunks)), dma((2,)), dma, dma, dma, dma,
                pltpu.SemaphoreType.REGULAR(((times_n - 1).bit_length(), 2)),
            ],
            compiler_params=pltpu.CompilerParams(
                collective_id=0, has_side_effects=True, vmem_limit_bytes=VMEM_BYTES
            ),
        )(*[pltpu.with_memory_space_constraint(a, pltpu.HBM) for a in operands])
        out, slice_norm, total_norm = pl.pallas_call(
            finish,
            out_shape=(
                jax.ShapeDtypeStruct(layer_shape, jnp.float32),
                jax.ShapeDtypeStruct((1,), jnp.float32),
                jax.ShapeDtypeStruct((1,), jnp.float32),
            ),
            in_specs=[pl.BlockSpec(memory_space=pltpu.VMEM)] * 2,
            out_specs=[pl.BlockSpec(memory_space=pltpu.HBM)] * 3,
            scratch_shapes=[
                pltpu.SMEM((1,), jnp.float32), pltpu.SMEM((1,), jnp.float32), dma((3,)),
            ],
            compiler_params=pltpu.CompilerParams(vmem_limit_bytes=VMEM_BYTES // 2),
        )(
            pltpu.with_memory_space_constraint(ends, pltpu.VMEM),
            pltpu.with_memory_space_constraint(norms, pltpu.VMEM),
        )
        return out.reshape(starts.shape), slice_norm, total_norm

    return jax.shard_map(
        step,
        mesh=mesh,
        in_specs=(P("tm", None, "space", None, None), P(None, "space", None, None)),
        out_specs=(P("tm", None, "space", None, None), P("tm"), P()),
        check_vma=False,
    )
```

```python
import functools
import math

import jax
import jax.numpy as jnp
import numpy as np
from jax import lax
from jax.experimental import pallas as pl
from jax.experimental.pallas import tpu as pltpu
from jax.sharding import PartitionSpec as P

viscosity = 0.08
diffusivity = 0.05
compress_rate = 0.25
time_step = 0.5
diffusion_number = 0.08
advect_xaxis = 0.2
advect_yaxis = 0.15
advect_zaxis = 0.1
epsilon = 1e-06
MESH = pl.DeviceIdType.MESH
PAD = 8
CHUNK = 16
LANES = 128
SUBLANES = 8
PAIR = 2
VMEM_BYTES = 32 * 1024 * 1024


def layout(fields, depth, rows, cols, times_n, spaces):
    keep_y, keep_x = rows // 8, cols // 16
    groups = -(-fields * depth // (LANES // (2 * keep_x)))
    pair = PAIR if times_n % PAIR == 0 else 1
    owners = spaces * pair
    share = 2 * keep_y // owners
    used = groups * share
    height = -(-max(used + 1, used + share) // SUBLANES) * SUBLANES
    return groups, pair, owners, share, used, height


def tables(fields, depth, rows, cols, times_n, spaces):
    groups, pair, owners, share, used, height = layout(fields, depth, rows, cols, times_n, spaces)
    keep_y, keep_x = rows // 8, cols // 16
    slot = 2 * keep_x
    full = depth * spaces
    k = np.arange(keep_x)
    x = np.arange(cols)
    ax = 2 * math.pi / cols * ((x[:, None] * k[None, :]) % cols)
    weight = np.where(k == 0, 1.0, 2.0) / (full * rows * cols)
    xf = np.zeros((2 * cols, LANES))
    xi = np.zeros((LANES, 2 * cols))
    for i in range(2):
        at = i * slot
        xf[i * cols : (i + 1) * cols, at : at + keep_x] = np.cos(ax)
        xf[i * cols : (i + 1) * cols, at + keep_x : at + slot] = -np.sin(ax)
        xi[at : at + keep_x, i * cols : (i + 1) * cols] = (np.cos(ax) * weight).T
        xi[at + keep_x : at + slot, i * cols : (i + 1) * cols] = (-np.sin(ax) * weight).T
    ky = np.arange(2 * keep_y)
    ky = np.where(ky < keep_y, ky, ky - 2 * keep_y)
    y = np.arange(rows)
    ay = 2 * math.pi / rows * ((ky[:, None] * y[None, :]) % rows)
    kz = np.arange(full)
    width = full * keep_x
    block = owners * height
    yf = np.zeros((block, (groups + 1) * 2 * rows))
    yi = np.zeros((groups * rows, 2 * block))
    for g in range(groups + 1):
        for at in range(2 * keep_y):
            row = at // share * height + g * share + at % share
            yf[row, g * 2 * rows : (g + 1) * 2 * rows] = np.concatenate([np.cos(ay[at]), np.sin(ay[at])])
    for g in range(groups):
        for at in range(2 * keep_y):
            row = at // share * height + g * share + at % share
            yi[g * rows : (g + 1) * rows, row] = np.cos(ay[at])
            yi[g * rows : (g + 1) * rows, block + row] = -np.sin(ay[at])
    zf = np.zeros((full * slot, 2 * width))
    for z in range(full):
        a = 2 * math.pi / full * ((kz * z) % full)
        for kk in range(keep_x):
            row = z * slot + kk
            re = kz * keep_x + kk
            im = re + width
            zf[row, re] = np.cos(a)
            zf[row, im] = -np.sin(a)
            zf[row + keep_x, re] = np.sin(a)
            zf[row + keep_x, im] = np.cos(a)
    zi = np.zeros((2 * width, full * slot))
    for z in range(full):
        a = 2 * math.pi / full * ((kz * z) % full)
        for kk in range(keep_x):
            re = kz * keep_x + kk
            im = re + width
            col = z * slot + kk
            zi[re, col] = np.cos(a)
            zi[im, col] = -np.sin(a)
            zi[re, col + keep_x] = np.sin(a)
            zi[im, col + keep_x] = np.cos(a)
    tz = 2 * math.pi / full * kz
    ty = 2 * math.pi / rows * ky
    tx = 2 * math.pi / cols * k
    live = (ky != -keep_y).astype(np.float64)[:, None, None]
    real = 1.0 + diffusion_number * (
        (2 * np.cos(ty) - 2)[:, None, None]
        + (2 * np.cos(tz) - 2)[None, :, None]
        + (2 * np.cos(tx) - 2)[None, None, :]
    )
    imag = -(
        advect_yaxis * np.sin(ty)[:, None, None]
        + advect_zaxis * np.sin(tz)[None, :, None]
        + advect_xaxis * np.sin(tx)[None, None, :]
    )
    symbol = (real + 1j * imag) * live
    symbol = symbol.reshape(owners, share, width)
    per = LANES // (slot * depth)
    gains = np.zeros((owners, per, 2, height, width), np.float32)
    for f in range(fields):
        at = f // per * share
        gains[:, f % per, 0, at : at + share] = symbol.real
        gains[:, f % per, 1, at : at + share] = symbol.imag
    held = {
        "xf": halves(xf, 1), "yf": halves(yf, 1), "zf": halves(zf, 1), "zi": halves(zi, 1),
        "yi": halves(yi, 1, True), "xi": halves(xi, 0, True),
    }
    places, at, blocks = {}, 0, []
    for name, table in held.items():
        height, wide = table.shape
        places[name] = (at, height, wide // LANES)
        blocks += [table[:, i : i + LANES] for i in range(0, wide, LANES)]
        at += height * (wide // LANES)
    return places, np.concatenate(blocks, axis=0), gains


def halves(table, axis, twice=False):
    high = table.astype(jnp.bfloat16)
    low = (table - high.astype(np.float64)).astype(jnp.bfloat16)
    return np.concatenate([high, high, low] if twice else [high, low], axis=axis)


def split(values):
    high = values.astype(jnp.bfloat16)
    return high, (values - high.astype(jnp.float32)).astype(jnp.bfloat16)


def dot(a, b):
    return jnp.dot(a, b, preferred_element_type=jnp.float32)


def times(values, table):
    high, low = split(values)
    wide = table.shape[1] // 2
    if wide > LANES:
        return dot(high, table[:, :wide]) + dot(low, table[:, :wide]) + dot(high, table[:, wide:])
    both = dot(high, table)
    return both[:, :wide] + dot(low, table[:, :wide]) + both[:, wide:]


def times_deep(values, table):
    high, low = split(values)
    deep = 2 * values.shape[1]
    return dot(jnp.concatenate([high, low], axis=1), table[:deep]) + dot(high, table[deep:])


def under(table, values):
    high, low = split(values)
    deep, wide = values.shape
    both = dot(table[:, :deep], jnp.concatenate([high, low], axis=1))
    return both[:, :wide] + both[:, wide:] + dot(table[:, deep:], high)


def under_deep(table, values):
    high, low = split(values)
    deep = 2 * values.shape[0]
    return dot(table[:, :deep], jnp.concatenate([high, low], axis=0)) + dot(table[:, deep:], high)


def entry_of(table, places, name):
    at, height, wide = places[name]
    return jnp.concatenate([table[pl.ds(at + i * height, height)] for i in range(wide)], axis=1)


def swap(values, keep_x):
    lane = lax.broadcasted_iota(jnp.int32, (1, LANES), 1)
    first = lax.rem(lane, 2 * keep_x) < keep_x
    return jnp.where(first, pltpu.roll(values, LANES - keep_x, 1), -pltpu.roll(values, keep_x, 1))


def kernel(
    sizes, places, starts, source, tables_h, sym_h,
    fine, table, spectrum,
    y1, y2, y3, y4, src, rims, late, begun, sym,
    own, jumps, ahead, gathered, corrections, pieces, modes,
    load_sem, table_sem, halo_send, halo_recv, ahead_sems, jump_send, jump_recv,
    mode_send, mode_recv, relays,
):
    times_n, spaces, fields, depth, rows, cols = sizes
    keep_y, keep_x = rows // 8, cols // 16
    slot = 2 * keep_x
    layers = fields * depth
    slots = LANES // slot
    per = LANES // (slot * depth)
    groups, pair, owners, share, used, height = layout(fields, depth, rows, cols, times_n, spaces)
    chunks = rows // CHUNK
    n = lax.axis_index("tm")
    s = lax.axis_index("space")
    place = lax.rem(n, pair)
    me = place * spaces + s
    base = n - place
    up = lax.rem(s + 1, spaces)
    down = lax.rem(s + spaces - 1, spaces)

    barrier = pltpu.get_barrier_semaphore()

    def near(distance, act):
        for side, target in enumerate((n - distance, n + distance)):
            pl.when((target >= 0) & (target < times_n))(functools.partial(act, side, target))

    def enter(target, where):
        pl.semaphore_signal(barrier, inc=1, device_id=(target, where), device_id_type=MESH)

    for offset in range(1, spaces):
        enter(n, lax.rem(s + offset, spaces))
    near(1, lambda side, target: enter(target, s))
    edges = [
        pltpu.make_async_copy(
            starts.at[0, :, z], y1.at[:, z + 1, pl.ds(PAD, rows)], load_sem.at[min(z, 1)]
        )
        for z in (0, depth - 1)
    ]
    for copy in edges:
        copy.start()
    loads = [
        pltpu.make_async_copy(
            starts.at[0, :, pl.ds(1, depth - 2)],
            y1.at[:, pl.ds(2, depth - 2), pl.ds(PAD, rows)],
            load_sem.at[2],
        ),
        pltpu.make_async_copy(tables_h, table, table_sem.at[0]),
        pltpu.make_async_copy(source, src, load_sem.at[3]),
        pltpu.make_async_copy(sym_h, sym, table_sem.at[1]),
    ]
    for copy in loads:
        copy.start()
    for copy in edges:
        copy.wait()
    beside = jnp.where(n > 0, 1, 0) + jnp.where(n < times_n - 1, 1, 0)
    pl.semaphore_wait(barrier, spaces - 1 + beside)

    def relay(level):
        near(
            2**level,
            lambda side, target: pl.semaphore_signal(
                relays.at[level, side], inc=1, device_id=(target, s), device_id_type=MESH
            ),
        )

    def heard(level):
        near(2**level, lambda side, target: pl.semaphore_wait(relays.at[level, 1 - side], 1))

    levels = (times_n - 1).bit_length()

    states = [y1, y2, y3, y4]

    parity = lax.rem(s, 2)
    far_to, near_to = jnp.where(parity == 0, down, up), jnp.where(parity == 0, up, down)
    far_z = jnp.where(parity == 0, 1, depth)
    near_z = depth + 1 - far_z
    step = 1 - 2 * parity
    far_halo, near_halo = far_z - step, near_z + step

    def settle(held, sem):
        pltpu.make_async_copy(held, held, sem).wait()

    def span(chunk):
        return pl.ds(pl.multiple_of(PAD + chunk * CHUNK, PAD), CHUNK)

    def send(src_ref, dst_ref, stage, index, target):
        pltpu.make_async_remote_copy(
            src_ref=src_ref,
            dst_ref=dst_ref,
            send_sem=halo_send.at[stage],
            recv_sem=halo_recv.at[stage % 2, index],
            device_id=(n, target),
            device_id_type=MESH,
        ).start()

    def send_near(stage):
        here, state = pl.ds(PAD, rows), states[stage]
        send(state.at[:, near_z, here], state.at[:, depth + 1 - near_halo, here], stage, 0, near_to)

    def send_far(stage, chunk):
        here, state = span(chunk), states[stage]
        send(
            state.at[:, far_z, here], state.at[:, depth + 1 - far_halo, here], stage, 1 + chunk, far_to
        )

    def send_first(c, carry):
        send_far(0, c)
        return carry

    lax.fori_loop(0, chunks, send_first, 0)
    send_near(0)
    relay(0)

    lane = lax.broadcasted_iota(jnp.int32, (1, LANES), 1)
    swapped = functools.partial(swap, keep_x=keep_x)

    entry = functools.partial(entry_of, table, places)

    def pack(pairs, result):
        stacked = jnp.concatenate(
            [jnp.concatenate([left, right], axis=1) for _, _, left, right in pairs], axis=0
        )
        packed = times(stacked, entry("xf"))
        result = list(result)
        for i, (g, at, _, _) in enumerate(pairs):
            piece = packed[i * rows : (i + 1) * rows]
            if not (isinstance(at, int) and at == 0):
                piece = pltpu.roll(piece, at * slot, 1)
            result[g] = piece if result[g] is None else result[g] + piece
        return result

    def transform(result):
        both = jnp.concatenate([part for t in result for part in (t, swapped(t))], axis=0)
        at, tall, wide = places["yf"]
        blocks = wide // 2
        held = len(result) * 2 * rows // LANES
        columns = [i * blocks + j for i in range(2) for j in range(held)]
        matrix = jnp.concatenate([table[pl.ds(at + i * tall, tall)] for i in columns], axis=1)
        return under(matrix, both).reshape(owners, height, LANES)

    def paired(layer_of, first_of, count):
        return [
            (f // per, f % per * depth + z, layer_of(f, z), layer_of(f, z + 1))
            for f in range(fields)
            for z in (first_of + i for i in range(0, count, 2))
        ]

    def rim_place(f):
        if f // per == groups - 1 and fields % per:
            return groups - 1, fields % per * depth
        return groups, f % per * depth + 2 * (f // per)

    loads[0].wait()
    loads[1].wait()
    for f in range(fields):
        for z in range(1, depth + 1):
            y1[f, z, pl.ds(0, PAD)] = y1[f, z, pl.ds(rows, PAD)]
            y1[f, z, pl.ds(PAD + rows, PAD)] = y1[f, z, pl.ds(PAD, PAD)]
        for z in (0, depth + 1):
            y4[f, z, pl.ds(PAD, rows)] = jnp.zeros((rows, cols), jnp.float32)

    own[...] = transform(
        pack(paired(lambda f, z: y1[f, z + 1, pl.ds(PAD, rows)], 0, depth), [None] * groups)
    )
    ahead_copy = pltpu.make_async_remote_copy(
        src_ref=own,
        dst_ref=ahead,
        send_sem=ahead_sems.at[0],
        recv_sem=ahead_sems.at[1],
        device_id=(jnp.maximum(n - 1, 0), s),
        device_id_type=MESH,
    )

    @pl.when(n > 0)
    def _():
        ahead_copy.start()

    shift = viscosity - diffusivity

    def reach(layer, sign):
        factor = (viscosity + sign * 0.5 * advect_zaxis) + (sign * 0.5) * layer[2]
        result = [factor * layer[f] for f in range(3)]
        result[2] = result[2] + (sign * 0.5) * layer[3]
        return result + [(sign * 0.5 * compress_rate) * layer[2], (factor - shift) * layer[4]]

    def weigh(stage):
        return time_step / 6.0 * (1.0, 2.0, 2.0, 1.0)[stage]

    loads[2].wait()
    loads[3].wait()

    def update(stage, z, r0):
        state = states[stage]
        mid, xm, xp, ym, yp = [], [], [], [], []
        rolled = CHUNK + 2 * PAD
        for f in range(fields):
            wide = state[f, z, pl.ds(r0, rolled)]
            centre = wide[PAD : PAD + CHUNK]
            mid.append(centre)
            ym.append(pltpu.roll(wide, 1, 0)[PAD : PAD + CHUNK])
            yp.append(pltpu.roll(wide, rolled - 1, 0)[PAD : PAD + CHUNK])
            xm.append(pltpu.roll(centre, 1, 1))
            xp.append(pltpu.roll(centre, cols - 1, 1))
        sides = [(xm, 0, 1.0, advect_xaxis), (xp, 0, -1.0, advect_xaxis)]
        sides += [(ym, 1, 1.0, advect_yaxis), (yp, 1, -1.0, advect_yaxis)]
        here = pl.ds(pl.multiple_of(r0 + PAD, PAD), CHUNK)
        for offset, sign in ((-1, 1.0), (1, -1.0)):
            held = [state[f, z + offset, here] for f in range(fields)]
            sides.append((held, 2, sign, advect_zaxis))
        factors = [
            (viscosity + sign * 0.5 * speed) + (sign * 0.5) * side[axis]
            for side, axis, sign, speed in sides
        ]
        rates = []
        for f in range(fields):
            forcing = src[f, z - 1, pl.ds(r0, CHUNK)]
            if f == 3:
                total = None
                for side, axis, sign, _ in sides:
                    if total is None:
                        total = side[axis]
                    else:
                        total = total + side[axis] if sign > 0 else total - side[axis]
                total = total * (0.5 * compress_rate)
            else:
                gain = viscosity if f < 3 else diffusivity
                total = (-6.0 * gain) * mid[f]
                push = None
                for factor, (side, axis, sign, _) in zip(factors, sides):
                    total = total + (factor if f < 3 else factor - shift) * side[f]
                    if axis == f:
                        term = (sign * 0.5) * side[3]
                        push = term if push is None else push + term
                if push is not None:
                    total = total + push
            rates.append(total + forcing)
        share_of = weigh(stage)
        for f in range(fields):
            at = f * depth + z - 1
            here = pl.ds(r0, CHUNK)
            begin = y1[f, z, pl.ds(pl.multiple_of(r0 + PAD, 8), CHUNK)]
            done = begin if stage == 0 else fine[at, here]
            fine[at, here] = done + share_of * rates[f]
            if stage < 3:
                later = states[stage + 1]
                step = (0.5, 0.5, 1.0)[stage] * time_step
                value = begin + step * rates[f]
                later[f, z, pl.ds(pl.multiple_of(r0 + PAD, 8), CHUNK)] = value

                @pl.when(r0 == 0)
                def _():
                    later[f, z, pl.ds(PAD + rows, PAD)] = value[:PAD]

                @pl.when(r0 == rows - CHUNK)
                def _():
                    later[f, z, pl.ds(0, PAD)] = value[CHUNK - PAD :]

    def sweep(act):
        def body(c, carry):
            act(c, pl.multiple_of(c * CHUNK, CHUNK))
            return carry

        lax.fori_loop(0, chunks, body, 0)

    def rim(z, r0):
        side = jnp.where(z == depth, 1, 0)
        sign = jnp.where(z == depth, 1.0, -1.0)
        layer = [y4[f, z, pl.ds(pl.multiple_of(r0 + PAD, PAD), CHUNK)] for f in range(fields)]
        for f, value in enumerate(reach(layer, sign)):
            rims[side, f, pl.ds(r0, CHUNK)] = weigh(3) * value

    early = [near_z - step * k for k in range(depth - 2)]
    late_layers = [far_z, far_z + step]
    early_first = jnp.where(parity == 0, 2, 0)
    late_first = jnp.where(parity == 0, 0, depth - 2)

    def settled(f, z):
        return fine[f * depth + z]

    def remaining(c):
        r0 = pl.multiple_of(c * CHUNK, CHUNK)
        for z in late_layers:
            update(3, z, r0)
        rim(far_z, r0)

    for stage in range(3):
        state = states[stage]

        def inner(c, r0):
            for z in range(2, depth):
                update(stage, z, r0)

        def edge(c, r0):
            settle(state.at[:, far_halo, span(c)], halo_recv.at[stage % 2, 1 + c])
            update(stage, far_z, r0)
            if stage < 2:
                send_far(stage + 1, c)
            else:
                pl.when(c >= 2)(lambda: remaining(c - 1))

        sweep(inner)
        settle(state.at[:, near_halo, pl.ds(PAD, rows)], halo_recv.at[stage % 2, 0])
        sweep(lambda c, r0: update(stage, near_z, r0))
        if stage < 2:
            send_near(stage + 1)
        else:

            def ready(c, r0):
                for z in early:
                    update(3, z, r0)
                rim(near_z, r0)

            sweep(ready)
            result = pack(paired(settled, early_first, depth - 2), [None] * groups)
            for g in range(groups):
                begun[g] = result[g]
        sweep(edge)
        for level in range(levels):
            if min(level, 2) == stage:
                heard(level)
                if level + 1 < levels:
                    relay(level + 1)

    remaining(chunks - 1)
    remaining(0)
    pairs = paired(settled, late_first, 2)
    pairs += [(*rim_place(f), rims[1, f], rims[0, f]) for f in range(fields)]
    spec = transform(pack(pairs, [begun[g] for g in range(groups)] + [None]))

    def jump_copy(index, tile, target):
        return pltpu.make_async_remote_copy(
            src_ref=jumps.at[tile],
            dst_ref=gathered.at[index],
            send_sem=jump_send,
            recv_sem=jump_recv,
            device_id=target,
            device_id_type=MESH,
        )

    def others(act):
        def body(dt, carry):
            t = n + dt
            t = jnp.where(t >= times_n, t - times_n, t)
            for ds in reversed(range(spaces)):
                where = s + ds
                where = jnp.where(where >= spaces, where - spaces, where)
                run = functools.partial(act, t, where)
                if ds == 0:
                    pl.when(dt > 0)(run)
                else:
                    run()
            return carry

        if times_n <= 8:
            for dt in sorted(range(times_n), key=lambda d: -min(d, times_n - d)):
                body(dt, 0)
        else:
            lax.fori_loop(0, times_n, body, 0)

    sent = lambda t, where: jump_copy(
        n * spaces + s, lax.rem(t, pair) * spaces + where, (t, where)
    )

    @pl.when(n < times_n - 1)
    def _():
        ahead_copy.wait_recv()
        jumps[...] = spec - ahead[...]
        others(lambda t, where: sent(t, where).start())
        gathered[n * spaces + s] = jumps[me]

    whole = pl.ds(PAD, rows)
    send(y4.at[:, far_z, whole], late.at[1 - parity], 3, 1, far_to)
    send(y4.at[:, near_z, whole], late.at[parity], 3, 0, near_to)

    def finish_edge(c, r0):
        here = pl.ds(r0, CHUNK)
        for side in range(2):
            layer = [late[side, f, here] for f in range(fields)]
            for f, value in enumerate(reach(layer, -1.0 if side else 1.0)):
                at = f * depth + side * (depth - 1)
                fine[at, here] = fine[at, here] + weigh(3) * value

    pl.when(n < times_n - 1)(
        lambda: settle(gathered.at[pl.ds(0, (times_n - 1) * spaces - 1)], jump_recv)
    )
    pl.when(n == times_n - 1)(lambda: settle(gathered.at[pl.ds(0, (times_n - 1) * spaces)], jump_recv))

    width = depth * spaces * keep_x
    half = depth * slot
    steps = times_n - 1
    part = lax.broadcasted_iota(jnp.int32, (1, LANES), 1) // half

    def turned(values, move):
        move = move % LANES
        return pltpu.roll(values, move, 1) if move else values

    def joined(blocks):
        total = None
        for i, block in enumerate(blocks):
            total = block if total is None else jnp.where(part == i, block, total)
        return total

    place_of = lax.rem(lax.broadcasted_iota(jnp.int32, (1, 1, LANES), 2), half) // slot
    line_of = lax.broadcasted_iota(jnp.int32, (1, height, 1), 1) // share
    raw = [
        jnp.stack([gathered[m * spaces + k] for m in range(steps)], axis=0) for k in range(spaces)
    ]

    def slid(values, move, axis):
        move = move % values.shape[axis]
        return pltpu.roll(values, move, axis) if move else values

    def rim_values(values):
        total = None
        for f in range(0, fields, per):
            g, at = rim_place(f)
            moved = slid(slid(values, -(at - f % per * depth) * slot, 2), (f // per - g) * share, 1)
            total = moved if total is None else jnp.where(line_of == f // per, moved, total)
        return total

    reached = [rim_values(values) for values in raw]
    slabs = []
    for k in range(spaces):
        from_below = jnp.where(place_of == 0, reached[(k - 1) % spaces], 0.0)
        from_above = slid(reached[(k + 1) % spaces], (depth - 2) * slot, 2)
        from_above = jnp.where(place_of == depth - 1, from_above, 0.0)
        slabs.append((raw[k] + (from_below + from_above)).reshape(steps * height, LANES))
    lined = [
        jnp.concatenate(
            [
                joined([turned(slabs[at + i], (i - fp) * half) for i in range(per)])
                for at in range(0, spaces, per)
            ],
            axis=1,
        )
        for fp in range(per)
    ]
    fresh = times(jnp.concatenate(lined, axis=0), entry("zf"))
    gains = [(sym[me, fp, 0], sym[me, fp, 1]) for fp in range(per)]
    weight = jnp.where(lax.rem(lane, keep_x) == 0, 1.0, 2.0)
    zero = jnp.zeros((height, width), jnp.float32)
    held = [(zero, zero)] * per
    sizes_of = [jnp.zeros((1, LANES), jnp.float32)]
    corrections[0] = jnp.zeros((per, height, 2 * width), jnp.float32)
    for m in range(steps):
        size = None
        for fp in range(per):
            at = (fp * steps + m) * height
            re = held[fp][0] + fresh[at : at + height, :width]
            im = held[fp][1] + fresh[at : at + height, width:]
            gain_re, gain_im = gains[fp]
            re, im = gain_re * re - gain_im * im, gain_re * im + gain_im * re
            held[fp] = (re, im)
            corrections[m + 1, fp, :, :width] = re
            corrections[m + 1, fp, :, width:] = im
            square = re * re + im * im
            size = square if size is None else size + square
        sizes_of.append(jnp.sum(size * weight, axis=0, keepdims=True))
    back = times(
        jnp.concatenate([corrections[base + j, fp] for j in range(pair) for fp in range(per)], axis=0),
        entry("zi"),
    )
    column = jnp.sum(jnp.concatenate(sizes_of, axis=0), axis=1, keepdims=True)
    shape = (times_n, LANES)
    diagonal = lax.broadcasted_iota(jnp.int32, shape, 0) == lax.broadcasted_iota(jnp.int32, shape, 1)
    squares = jnp.sum(jnp.where(diagonal, column, 0.0), axis=0, keepdims=True) * (
        1.0 / (depth * spaces * rows * cols)
    )
    last = lax.broadcasted_iota(jnp.int32, (height, LANES), 0) == used
    for j in range(pair):
        for k in range(spaces):
            at = k * half
            tile, inside = at // LANES * LANES, at % LANES
            piece = joined(
                [
                    turned(
                        back[(j * per + fp) * height : (j * per + fp + 1) * height, tile : tile + LANES],
                        fp * half - inside,
                    )
                    for fp in range(per)
                ]
            )
            pieces[j * spaces + k] = jnp.where(last, squares, piece)

    def mode_copy(dj, dk):
        j, k = lax.rem(place + dj, pair), lax.rem(s + dk, spaces)
        return pltpu.make_async_remote_copy(
            src_ref=pieces.at[j * spaces + k],
            dst_ref=modes.at[me],
            send_sem=mode_send,
            recv_sem=mode_recv,
            device_id=(base + j, k),
            device_id_type=MESH,
        )

    sharers = [(dj, dk) for dj in reversed(range(pair)) for dk in reversed(range(spaces)) if dj + dk]
    for dj, dk in sharers:
        mode_copy(dj, dk).start()
    modes[me] = pieces[me]
    settle(late.at[parity], halo_recv.at[1, 1])
    settle(late.at[1 - parity], halo_recv.at[1, 0])
    sweep(finish_edge)
    settle(modes.at[pl.ds(0, owners - 1)], mode_recv)
    spectrum[...] = modes[...].reshape(owners * height, LANES)

    pl.when(n < times_n - 1)(lambda: settle(gathered.at[pl.ds(0, times_n * spaces - 1)], jump_send))

    @pl.when(n > 0)
    def _():
        ahead_copy.wait_send()

    for stage in range(4):
        settle(states[stage].at[:, pl.ds(0, 2), pl.ds(PAD, rows)], halo_send.at[stage])
    settle(modes.at[pl.ds(0, owners - 1)], mode_send)


def finish(
    sizes, places, fine, table, spectrum, out, slice_out, total_out, ends, slice_held, total_held, sems
):
    times_n, spaces, fields, depth, rows, cols = sizes
    keep_x = cols // 16
    slot = 2 * keep_x
    layers = fields * depth
    slots = LANES // slot
    groups, _, owners, _, used, height = layout(fields, depth, rows, cols, times_n, spaces)
    n = lax.axis_index("tm")
    lane = lax.broadcasted_iota(jnp.int32, (1, LANES), 1)
    found = spectrum[...]
    total = None
    for o in range(owners):
        row = found[o * height + used : o * height + used + 1]
        total = row if total is None else total + row
    cells = fields * depth * spaces * rows * cols

    def norm(values, count):
        return jnp.sqrt(jnp.sum(values, axis=1, keepdims=True) * (1.0 / count) + epsilon)

    slice_held[0] = norm(jnp.where(lane == n, total, 0.0), cells)[0, 0]
    total_held[0] = norm(total, cells * times_n)[0, 0]
    copies = [
        pltpu.make_async_copy(slice_held, slice_out, sems.at[0]),
        pltpu.make_async_copy(total_held, total_out, sems.at[1]),
    ]
    for copy in copies:
        copy.start()
    planes = under_deep(
        entry_of(table, places, "yi"), jnp.concatenate([found, swap(found, keep_x)], axis=0)
    )
    for g in range(groups):
        plane = planes[g * rows : (g + 1) * rows]
        count = min(slots, layers - g * slots) // 2
        shifted = [
            plane if p == 0 else pltpu.roll(plane, LANES - 2 * p * slot, 1) for p in range(count)
        ]
        fix = times_deep(jnp.concatenate(shifted, axis=0), entry_of(table, places, "xi"))
        for p in range(count):
            for i in range(2):
                l = g * slots + 2 * p + i
                ends[l] = fine[l] + fix[p * rows : (p + 1) * rows, i * cols : (i + 1) * cols]
        held = pl.ds(g * slots, 2 * count)
        copies.append(pltpu.make_async_copy(ends.at[held], out.at[held], sems.at[2 + g]))
        copies[-1].start()
    for copy in copies:
        copy.wait()


def solution(mesh):
    times_n, spaces = mesh.shape["tm"], mesh.shape["space"]

    def step(starts, source):
        _, fields, depth, rows, cols = starts.shape
        places, packed, gains = tables(fields, depth, rows, cols, times_n, spaces)
        constants = [packed, gains]
        operands = [starts, source] + [jnp.asarray(c) for c in constants]
        groups, _, owners, _, _, height = layout(fields, depth, rows, cols, times_n, spaces)
        slot = cols // 16 * 2
        per = LANES // (slot * depth)
        chunks = rows // CHUNK
        devices = times_n * spaces
        state = pltpu.VMEM((fields, depth + 2, rows + 2 * PAD, cols), jnp.float32)
        dma = pltpu.SemaphoreType.DMA
        layer_shape = (fields * depth, rows, cols)
        held = pl.pallas_call(
            functools.partial(kernel, (times_n, spaces, fields, depth, rows, cols), places),
            out_shape=(
                pltpu.VMEM(layer_shape, jnp.float32),
                pltpu.VMEM(packed.shape, jnp.bfloat16),
                pltpu.VMEM((owners * height, LANES), jnp.float32),
            ),
            in_specs=[pl.BlockSpec(memory_space=pltpu.HBM)] * (2 + len(constants)),
            out_specs=(pl.BlockSpec(memory_space=pltpu.VMEM),) * 3,
            scratch_shapes=[
                state, state, state, state,
                pltpu.VMEM((fields, depth, rows, cols), jnp.float32),
                pltpu.VMEM((2, fields, rows, cols), jnp.float32),
                pltpu.VMEM((2, fields, rows, cols), jnp.float32),
                pltpu.VMEM((groups, rows, LANES), jnp.float32),
                pltpu.VMEM(gains.shape, jnp.float32),
                *[pltpu.VMEM((owners, height, LANES), jnp.float32)] * 3,
                pltpu.VMEM((devices, height, LANES), jnp.float32),
                pltpu.VMEM((times_n, per, height, depth * spaces * slot), jnp.float32),
                *[pltpu.VMEM((owners, height, LANES), jnp.float32)] * 2,
                dma((4,)), dma((2,)),
                dma((4,)), dma((2, 1 + chunks)), dma((2,)), dma, dma, dma, dma,
                pltpu.SemaphoreType.REGULAR(((times_n - 1).bit_length(), 2)),
            ],
            compiler_params=pltpu.CompilerParams(
                collective_id=0, has_side_effects=True, vmem_limit_bytes=VMEM_BYTES
            ),
        )(*[pltpu.with_memory_space_constraint(a, pltpu.HBM) for a in operands])
        out, slice_norm, total_norm = pl.pallas_call(
            functools.partial(finish, (times_n, spaces, fields, depth, rows, cols), places),
            out_shape=(
                jax.ShapeDtypeStruct(layer_shape, jnp.float32),
                jax.ShapeDtypeStruct((1,), jnp.float32),
                jax.ShapeDtypeStruct((1,), jnp.float32),
            ),
            in_specs=[pl.BlockSpec(memory_space=pltpu.VMEM)] * 3,
            out_specs=[pl.BlockSpec(memory_space=pltpu.HBM)] * 3,
            scratch_shapes=[
                pltpu.VMEM(layer_shape, jnp.float32),
                pltpu.SMEM((1,), jnp.float32), pltpu.SMEM((1,), jnp.float32), dma((2 + groups,)),
            ],
            compiler_params=pltpu.CompilerParams(vmem_limit_bytes=VMEM_BYTES // 2),
        )(*[pltpu.with_memory_space_constraint(a, pltpu.VMEM) for a in held])
        return out.reshape(starts.shape), slice_norm, total_norm

    return jax.shard_map(
        step,
        mesh=mesh,
        in_specs=(P("tm", None, "space", None, None), P(None, "space", None, None)),
        out_specs=(P("tm", None, "space", None, None), P("tm"), P()),
        check_vma=False,
    )
```

```python
import functools
import math

import jax
import jax.numpy as jnp
import numpy as np
from jax import lax
from jax.experimental import pallas as pl
from jax.experimental.pallas import tpu as pltpu
from jax.sharding import PartitionSpec as P

viscosity = 0.08
diffusivity = 0.05
compress_rate = 0.25
time_step = 0.5
diffusion_number = 0.08
advect_xaxis = 0.2
advect_yaxis = 0.15
advect_zaxis = 0.1
epsilon = 1e-06
MESH = pl.DeviceIdType.MESH
PAD = 8
CHUNK = 16
LANES = 128
SUBLANES = 8
PAIR = 2
VMEM_BYTES = 32 * 1024 * 1024


def layout(fields, depth, rows, cols, times_n, spaces):
    keep_y, keep_x = rows // 8, cols // 16
    groups = -(-fields * depth // (LANES // (2 * keep_x)))
    pair = PAIR if times_n % PAIR == 0 else 1
    owners = spaces * pair
    share = 2 * keep_y // owners
    used = groups * share
    height = -(-max(used + 1, used + share) // SUBLANES) * SUBLANES
    return groups, pair, owners, share, used, height


def tables(fields, depth, rows, cols, times_n, spaces):
    groups, pair, owners, share, used, height = layout(fields, depth, rows, cols, times_n, spaces)
    keep_y, keep_x = rows // 8, cols // 16
    slot = 2 * keep_x
    full = depth * spaces
    k = np.arange(keep_x)
    x = np.arange(cols)
    ax = 2 * math.pi / cols * ((x[:, None] * k[None, :]) % cols)
    weight = np.where(k == 0, 1.0, 2.0) / (full * rows * cols)
    xf = np.zeros((2 * cols, LANES))
    xi = np.zeros((LANES, 2 * cols))
    for i in range(2):
        at = i * slot
        xf[i * cols : (i + 1) * cols, at : at + keep_x] = np.cos(ax)
        xf[i * cols : (i + 1) * cols, at + keep_x : at + slot] = -np.sin(ax)
        xi[at : at + keep_x, i * cols : (i + 1) * cols] = (np.cos(ax) * weight).T
        xi[at + keep_x : at + slot, i * cols : (i + 1) * cols] = (-np.sin(ax) * weight).T
    ky = np.arange(2 * keep_y)
    ky = np.where(ky < keep_y, ky, ky - 2 * keep_y)
    y = np.arange(rows)
    ay = 2 * math.pi / rows * ((ky[:, None] * y[None, :]) % rows)
    kz = np.arange(full)
    width = full * keep_x
    block = owners * height
    yf = np.zeros((block, (groups + 1) * 2 * rows))
    yi = np.zeros((groups * rows, 2 * block))
    for g in range(groups + 1):
        for at in range(2 * keep_y):
            row = at // share * height + g * share + at % share
            yf[row, g * 2 * rows : (g + 1) * 2 * rows] = np.concatenate([np.cos(ay[at]), np.sin(ay[at])])
    for g in range(groups):
        for at in range(2 * keep_y):
            row = at // share * height + g * share + at % share
            yi[g * rows : (g + 1) * rows, row] = np.cos(ay[at])
            yi[g * rows : (g + 1) * rows, block + row] = -np.sin(ay[at])
    zf = np.zeros((full * slot, 2 * width))
    for z in range(full):
        a = 2 * math.pi / full * ((kz * z) % full)
        for kk in range(keep_x):
            row = z * slot + kk
            re = kz * keep_x + kk
            im = re + width
            zf[row, re] = np.cos(a)
            zf[row, im] = -np.sin(a)
            zf[row + keep_x, re] = np.sin(a)
            zf[row + keep_x, im] = np.cos(a)
    zi = np.zeros((2 * width, full * slot))
    for z in range(full):
        a = 2 * math.pi / full * ((kz * z) % full)
        for kk in range(keep_x):
            re = kz * keep_x + kk
            im = re + width
            col = z * slot + kk
            zi[re, col] = np.cos(a)
            zi[im, col] = -np.sin(a)
            zi[re, col + keep_x] = np.sin(a)
            zi[im, col + keep_x] = np.cos(a)
    tz = 2 * math.pi / full * kz
    ty = 2 * math.pi / rows * ky
    tx = 2 * math.pi / cols * k
    live = (ky != -keep_y).astype(np.float64)[:, None, None]
    real = 1.0 + diffusion_number * (
        (2 * np.cos(ty) - 2)[:, None, None]
        + (2 * np.cos(tz) - 2)[None, :, None]
        + (2 * np.cos(tx) - 2)[None, None, :]
    )
    imag = -(
        advect_yaxis * np.sin(ty)[:, None, None]
        + advect_zaxis * np.sin(tz)[None, :, None]
        + advect_xaxis * np.sin(tx)[None, None, :]
    )
    symbol = (real + 1j * imag) * live
    symbol = symbol.reshape(owners, share, width)
    per = LANES // (slot * depth)
    gains = np.zeros((owners, per, 2, height, width), np.float32)
    for f in range(fields):
        at = f // per * share
        gains[:, f % per, 0, at : at + share] = symbol.real
        gains[:, f % per, 1, at : at + share] = symbol.imag
    held = {
        "xf": halves(xf, 1), "yf": halves(yf, 1), "zf": halves(zf, 1), "zi": halves(zi, 1),
        "yi": halves(yi, 1, True), "xi": halves(xi, 0, True),
    }
    places, at, blocks = {}, 0, []
    for name, table in held.items():
        height, wide = table.shape
        places[name] = (at, height, wide // LANES)
        blocks += [table[:, i : i + LANES] for i in range(0, wide, LANES)]
        at += height * (wide // LANES)
    return places, np.concatenate(blocks, axis=0), gains


def halves(table, axis, twice=False):
    high = table.astype(jnp.bfloat16)
    low = (table - high.astype(np.float64)).astype(jnp.bfloat16)
    return np.concatenate([high, high, low] if twice else [high, low], axis=axis)


def split(values):
    high = values.astype(jnp.bfloat16)
    return high, (values - high.astype(jnp.float32)).astype(jnp.bfloat16)


def dot(a, b):
    return jnp.dot(a, b, preferred_element_type=jnp.float32)


def times(values, table):
    high, low = split(values)
    wide = table.shape[1] // 2
    if wide > LANES:
        return dot(high, table[:, :wide]) + dot(low, table[:, :wide]) + dot(high, table[:, wide:])
    both = dot(high, table)
    return both[:, :wide] + dot(low, table[:, :wide]) + both[:, wide:]


def times_deep(values, table):
    high, low = split(values)
    deep = 2 * values.shape[1]
    return dot(jnp.concatenate([high, low], axis=1), table[:deep]) + dot(high, table[deep:])


def under(table, values):
    high, low = split(values)
    deep, wide = values.shape
    both = dot(table[:, :deep], jnp.concatenate([high, low], axis=1))
    return both[:, :wide] + both[:, wide:] + dot(table[:, deep:], high)


def under_deep(table, values):
    high, low = split(values)
    deep = 2 * values.shape[0]
    return dot(table[:, :deep], jnp.concatenate([high, low], axis=0)) + dot(table[:, deep:], high)


def entry_of(table, places, name):
    at, height, wide = places[name]
    return jnp.concatenate([table[pl.ds(at + i * height, height)] for i in range(wide)], axis=1)


def swap(values, keep_x):
    lane = lax.broadcasted_iota(jnp.int32, (1, LANES), 1)
    first = lax.rem(lane, 2 * keep_x) < keep_x
    return jnp.where(first, pltpu.roll(values, LANES - keep_x, 1), -pltpu.roll(values, keep_x, 1))


def kernel(
    sizes, places, starts, source, tables_h, sym_h,
    fine, table, spectrum,
    y1, y2, y3, y4, src, rims, late, begun, sym,
    own, jumps, ahead, gathered, corrections, pieces, modes,
    load_sem, table_sem, halo_send, halo_recv, ahead_sems, jump_send, jump_recv,
    mode_send, mode_recv, relays,
):
    times_n, spaces, fields, depth, rows, cols = sizes
    keep_y, keep_x = rows // 8, cols // 16
    slot = 2 * keep_x
    layers = fields * depth
    slots = LANES // slot
    per = LANES // (slot * depth)
    groups, pair, owners, share, used, height = layout(fields, depth, rows, cols, times_n, spaces)
    chunks = rows // CHUNK
    n = lax.axis_index("tm")
    s = lax.axis_index("space")
    place = lax.rem(n, pair)
    me = place * spaces + s
    base = n - place
    up = lax.rem(s + 1, spaces)
    down = lax.rem(s + spaces - 1, spaces)

    barrier = pltpu.get_barrier_semaphore()

    def near(distance, act):
        for side, target in enumerate((n - distance, n + distance)):
            pl.when((target >= 0) & (target < times_n))(functools.partial(act, side, target))

    def enter(target, where):
        pl.semaphore_signal(barrier, inc=1, device_id=(target, where), device_id_type=MESH)

    for offset in range(1, spaces):
        enter(n, lax.rem(s + offset, spaces))
    near(1, lambda side, target: enter(target, s))
    edges = [
        pltpu.make_async_copy(
            starts.at[0, :, z], y1.at[:, z + 1, pl.ds(PAD, rows)], load_sem.at[min(z, 1)]
        )
        for z in (0, depth - 1)
    ]
    for copy in edges:
        copy.start()
    loads = [
        pltpu.make_async_copy(
            starts.at[0, :, pl.ds(1, depth - 2)],
            y1.at[:, pl.ds(2, depth - 2), pl.ds(PAD, rows)],
            load_sem.at[2],
        ),
        pltpu.make_async_copy(tables_h, table, table_sem.at[0]),
        pltpu.make_async_copy(source, src, load_sem.at[3]),
        pltpu.make_async_copy(sym_h, sym, table_sem.at[1]),
    ]
    for copy in loads:
        copy.start()
    for copy in edges:
        copy.wait()
    beside = jnp.where(n > 0, 1, 0) + jnp.where(n < times_n - 1, 1, 0)
    pl.semaphore_wait(barrier, spaces - 1 + beside)

    def relay(level):
        near(
            2**level,
            lambda side, target: pl.semaphore_signal(
                relays.at[level, side], inc=1, device_id=(target, s), device_id_type=MESH
            ),
        )

    def heard(level):
        near(2**level, lambda side, target: pl.semaphore_wait(relays.at[level, 1 - side], 1))

    levels = (times_n - 1).bit_length()

    states = [y1, y2, y3, y4]

    parity = lax.rem(s, 2)
    far_to, near_to = jnp.where(parity == 0, down, up), jnp.where(parity == 0, up, down)
    far_z = jnp.where(parity == 0, 1, depth)
    near_z = depth + 1 - far_z
    step = 1 - 2 * parity
    far_halo, near_halo = far_z - step, near_z + step

    def settle(held, sem):
        pltpu.make_async_copy(held, held, sem).wait()

    def span(chunk):
        return pl.ds(pl.multiple_of(PAD + chunk * CHUNK, PAD), CHUNK)

    def send(src_ref, dst_ref, stage, index, target):
        pltpu.make_async_remote_copy(
            src_ref=src_ref,
            dst_ref=dst_ref,
            send_sem=halo_send.at[stage],
            recv_sem=halo_recv.at[stage % 2, index],
            device_id=(n, target),
            device_id_type=MESH,
        ).start()

    def send_near(stage):
        here, state = pl.ds(PAD, rows), states[stage]
        send(state.at[:, near_z, here], state.at[:, depth + 1 - near_halo, here], stage, 0, near_to)

    def send_far(stage, chunk):
        here, state = span(chunk), states[stage]
        send(
            state.at[:, far_z, here], state.at[:, depth + 1 - far_halo, here], stage, 1 + chunk, far_to
        )

    def send_first(c, carry):
        send_far(0, c)
        return carry

    lax.fori_loop(0, chunks, send_first, 0)
    send_near(0)
    relay(0)

    lane = lax.broadcasted_iota(jnp.int32, (1, LANES), 1)
    swapped = functools.partial(swap, keep_x=keep_x)

    entry = functools.partial(entry_of, table, places)

    def pack(pairs, result):
        stacked = jnp.concatenate(
            [jnp.concatenate([left, right], axis=1) for _, _, left, right in pairs], axis=0
        )
        packed = times(stacked, entry("xf"))
        result = list(result)
        for i, (g, at, _, _) in enumerate(pairs):
            tall = packed.shape[0] // len(pairs)
            piece = packed[i * tall : (i + 1) * tall]
            if not (isinstance(at, int) and at == 0):
                piece = pltpu.roll(piece, at * slot, 1)
            result[g] = piece if result[g] is None else result[g] + piece
        return result

    def transform(result):
        both = jnp.concatenate([part for t in result for part in (t, swapped(t))], axis=0)
        at, tall, wide = places["yf"]
        blocks = wide // 2
        held = len(result) * 2 * rows // LANES
        columns = [i * blocks + j for i in range(2) for j in range(held)]
        matrix = jnp.concatenate([table[pl.ds(at + i * tall, tall)] for i in columns], axis=1)
        return under(matrix, both).reshape(owners, height, LANES)

    def paired(layer_of, first_of, count):
        return [
            (f // per, f % per * depth + z, layer_of(f, z), layer_of(f, z + 1))
            for f in range(fields)
            for z in (first_of + i for i in range(0, count, 2))
        ]

    def rim_place(f):
        if f // per == groups - 1 and fields % per:
            return groups - 1, fields % per * depth
        return groups, f % per * depth + 2 * (f // per)

    loads[0].wait()
    loads[1].wait()
    def wrap(state, z):
        for f in range(fields):
            state[f, z, pl.ds(0, PAD)] = state[f, z, pl.ds(rows, PAD)]
            state[f, z, pl.ds(PAD + rows, PAD)] = state[f, z, pl.ds(PAD, PAD)]

    for z in range(1, depth + 1):
        wrap(y1, z)
    for f in range(fields):
        for z in (0, depth + 1):
            y4[f, z, pl.ds(PAD, rows)] = jnp.zeros((rows, cols), jnp.float32)

    own[...] = transform(
        pack(paired(lambda f, z: y1[f, z + 1, pl.ds(PAD, rows)], 0, depth), [None] * groups)
    )
    ahead_copy = pltpu.make_async_remote_copy(
        src_ref=own,
        dst_ref=ahead,
        send_sem=ahead_sems.at[0],
        recv_sem=ahead_sems.at[1],
        device_id=(jnp.maximum(n - 1, 0), s),
        device_id_type=MESH,
    )

    @pl.when(n > 0)
    def _():
        ahead_copy.start()

    shift = viscosity - diffusivity

    def reach(layer, sign):
        factor = (viscosity + sign * 0.5 * advect_zaxis) + (sign * 0.5) * layer[2]
        result = [factor * layer[f] for f in range(3)]
        result[2] = result[2] + (sign * 0.5) * layer[3]
        return result + [(sign * 0.5 * compress_rate) * layer[2], (factor - shift) * layer[4]]

    def weigh(stage):
        return time_step / 6.0 * (1.0, 2.0, 2.0, 1.0)[stage]

    loads[2].wait()
    loads[3].wait()

    def update(stage, z, r0, size=CHUNK):
        state = states[stage]
        mid, xm, xp, ym, yp = [], [], [], [], []
        rolled = size + 2 * PAD
        for f in range(fields):
            wide = state[f, z, pl.ds(r0, rolled)]
            centre = wide[PAD : PAD + size]
            mid.append(centre)
            ym.append(pltpu.roll(wide, 1, 0)[PAD : PAD + size])
            yp.append(pltpu.roll(wide, rolled - 1, 0)[PAD : PAD + size])
            xm.append(pltpu.roll(centre, 1, 1))
            xp.append(pltpu.roll(centre, cols - 1, 1))
        sides = [(xm, 0, 1.0, advect_xaxis), (xp, 0, -1.0, advect_xaxis)]
        sides += [(ym, 1, 1.0, advect_yaxis), (yp, 1, -1.0, advect_yaxis)]
        here = pl.ds(pl.multiple_of(r0 + PAD, PAD), size)
        for offset, sign in ((-1, 1.0), (1, -1.0)):
            held = [state[f, z + offset, here] for f in range(fields)]
            sides.append((held, 2, sign, advect_zaxis))
        factors = [
            (viscosity + sign * 0.5 * speed) + (sign * 0.5) * side[axis]
            for side, axis, sign, speed in sides
        ]
        rates = []
        for f in range(fields):
            forcing = src[f, z - 1, pl.ds(r0, size)]
            if f == 3:
                total = None
                for side, axis, sign, _ in sides:
                    if total is None:
                        total = side[axis]
                    else:
                        total = total + side[axis] if sign > 0 else total - side[axis]
                total = total * (0.5 * compress_rate)
            else:
                gain = viscosity if f < 3 else diffusivity
                total = (-6.0 * gain) * mid[f]
                push = None
                for factor, (side, axis, sign, _) in zip(factors, sides):
                    total = total + (factor if f < 3 else factor - shift) * side[f]
                    if axis == f:
                        term = (sign * 0.5) * side[3]
                        push = term if push is None else push + term
                if push is not None:
                    total = total + push
            rates.append(total + forcing)
        share_of = weigh(stage)
        for f in range(fields):
            at = f * depth + z - 1
            here = pl.ds(r0, size)
            begin = y1[f, z, pl.ds(pl.multiple_of(r0 + PAD, 8), size)]
            done = begin if stage == 0 else fine[at, here]
            fine[at, here] = done + share_of * rates[f]
            if stage < 3:
                later = states[stage + 1]
                step = (0.5, 0.5, 1.0)[stage] * time_step
                value = begin + step * rates[f]
                later[f, z, pl.ds(pl.multiple_of(r0 + PAD, 8), size)] = value

    def sweep(act, count=chunks):
        def body(c, carry):
            act(c, pl.multiple_of(c * CHUNK, CHUNK))
            return carry

        lax.fori_loop(0, count, body, 0)

    def rim(z, r0, size=CHUNK):
        side = jnp.where(z == depth, 1, 0)
        sign = jnp.where(z == depth, 1.0, -1.0)
        layer = [y4[f, z, pl.ds(pl.multiple_of(r0 + PAD, PAD), size)] for f in range(fields)]
        for f, value in enumerate(reach(layer, sign)):
            rims[side, f, pl.ds(r0, size)] = weigh(3) * value

    early = [near_z - step * k for k in range(depth - 2)]
    late_layers = [far_z, far_z + step]
    early_first = jnp.where(parity == 0, 2, 0)
    late_first = jnp.where(parity == 0, 0, depth - 2)

    def settled(f, z):
        return fine[f * depth + z]

    def remaining(r0, size):
        for z in late_layers:
            update(3, z, r0, size)
        rim(far_z, r0, size)

    def finish_rows(spans):
        def of(ref, *index):
            return jnp.concatenate([ref[*index, pl.ds(r0, size)] for r0, size in spans], axis=0)

        pairs = paired(lambda f, z: of(fine, f * depth + z), late_first, 2)
        pairs += [(*rim_place(f), of(rims, 1, f), of(rims, 0, f)) for f in range(fields)]
        result = pack(pairs, [of(begun, g) for g in range(groups)] + [None])
        for g in range(groups + 1):
            at = 0
            for r0, size in spans:
                begun[g, pl.ds(r0, size)] = result[g][at : at + size]
                at += size

    for stage in range(3):
        state = states[stage]

        def inner(c, r0):
            for z in range(2, depth):
                update(stage, z, r0)

        def edge(c, r0):
            settle(state.at[:, far_halo, span(c)], halo_recv.at[stage % 2, 1 + c])
            update(stage, far_z, r0)
            if stage < 2:
                send_far(stage + 1, c)
            else:
                pl.when(c >= 1)(lambda: remaining(pl.multiple_of(r0 - PAD, PAD), CHUNK))

        sweep(inner)
        for z in range(2, depth):
            wrap(states[stage + 1], z)
        settle(state.at[:, near_halo, pl.ds(PAD, rows)], halo_recv.at[stage % 2, 0])
        sweep(lambda c, r0: update(stage, near_z, r0))
        wrap(states[stage + 1], near_z)
        if stage < 2:
            send_near(stage + 1)
        else:

            def ready(c, r0):
                for z in early:
                    update(3, z, r0)
                rim(near_z, r0)

            sweep(ready)
            result = pack(paired(settled, early_first, depth - 2), [None] * groups)
            for g in range(groups):
                begun[g] = result[g]
        sweep(edge, chunks if stage < 2 else chunks - 1)
        if stage == 2:
            finish_rows([(PAD, rows - CHUNK - 2 * PAD)])
            edge(chunks - 1, rows - CHUNK)
        wrap(states[stage + 1], far_z)
        for level in range(levels):
            if min(level, 2) == stage:
                heard(level)
                if level + 1 < levels:
                    relay(level + 1)

    remaining(rows - PAD, PAD)
    remaining(0, PAD)
    finish_rows([(rows - CHUNK - PAD, CHUNK + PAD), (0, PAD)])
    spec = transform([begun[g] for g in range(groups + 1)])

    def jump_copy(index, tile, target):
        return pltpu.make_async_remote_copy(
            src_ref=jumps.at[tile],
            dst_ref=gathered.at[index],
            send_sem=jump_send,
            recv_sem=jump_recv,
            device_id=target,
            device_id_type=MESH,
        )

    def others(act):
        def body(dt, carry):
            t = n + dt
            t = jnp.where(t >= times_n, t - times_n, t)
            for ds in reversed(range(spaces)):
                where = s + ds
                where = jnp.where(where >= spaces, where - spaces, where)
                run = functools.partial(act, t, where)
                if ds == 0:
                    pl.when(dt > 0)(run)
                else:
                    run()
            return carry

        if times_n <= 8:
            for dt in sorted(range(times_n), key=lambda d: -min(d, times_n - d)):
                body(dt, 0)
        else:
            lax.fori_loop(0, times_n, body, 0)

    sent = lambda t, where: jump_copy(
        n * spaces + s, lax.rem(t, pair) * spaces + where, (t, where)
    )

    @pl.when(n < times_n - 1)
    def _():
        ahead_copy.wait_recv()
        jumps[...] = spec - ahead[...]
        others(lambda t, where: sent(t, where).start())
        gathered[n * spaces + s] = jumps[me]

    whole = pl.ds(PAD, rows)
    send(y4.at[:, far_z, whole], late.at[1 - parity], 3, 1, far_to)
    send(y4.at[:, near_z, whole], late.at[parity], 3, 0, near_to)

    def finish_edge(c, r0):
        here = pl.ds(r0, CHUNK)
        for side in range(2):
            layer = [late[side, f, here] for f in range(fields)]
            for f, value in enumerate(reach(layer, -1.0 if side else 1.0)):
                at = f * depth + side * (depth - 1)
                fine[at, here] = fine[at, here] + weigh(3) * value

    pl.when(n < times_n - 1)(
        lambda: settle(gathered.at[pl.ds(0, (times_n - 1) * spaces - 1)], jump_recv)
    )
    pl.when(n == times_n - 1)(lambda: settle(gathered.at[pl.ds(0, (times_n - 1) * spaces)], jump_recv))

    width = depth * spaces * keep_x
    half = depth * slot
    steps = times_n - 1
    part = lax.broadcasted_iota(jnp.int32, (1, LANES), 1) // half

    def turned(values, move):
        move = move % LANES
        return pltpu.roll(values, move, 1) if move else values

    def joined(blocks):
        total = None
        for i, block in enumerate(blocks):
            total = block if total is None else jnp.where(part == i, block, total)
        return total

    place_of = lax.rem(lax.broadcasted_iota(jnp.int32, (1, 1, LANES), 2), half) // slot
    line_of = lax.broadcasted_iota(jnp.int32, (1, height, 1), 1) // share
    raw = [
        jnp.stack([gathered[m * spaces + k] for m in range(steps)], axis=0) for k in range(spaces)
    ]

    def slid(values, move, axis):
        move = move % values.shape[axis]
        return pltpu.roll(values, move, axis) if move else values

    def rim_values(values):
        total = None
        for f in range(0, fields, per):
            g, at = rim_place(f)
            moved = slid(slid(values, -(at - f % per * depth) * slot, 2), (f // per - g) * share, 1)
            total = moved if total is None else jnp.where(line_of == f // per, moved, total)
        return total

    reached = [rim_values(values) for values in raw]
    slabs = []
    for k in range(spaces):
        from_below = jnp.where(place_of == 0, reached[(k - 1) % spaces], 0.0)
        from_above = slid(reached[(k + 1) % spaces], (depth - 2) * slot, 2)
        from_above = jnp.where(place_of == depth - 1, from_above, 0.0)
        slabs.append((raw[k] + (from_below + from_above)).reshape(steps * height, LANES))
    lined = [
        jnp.concatenate(
            [
                joined([turned(slabs[at + i], (i - fp) * half) for i in range(per)])
                for at in range(0, spaces, per)
            ],
            axis=1,
        )
        for fp in range(per)
    ]
    fresh = times(jnp.concatenate(lined, axis=0), entry("zf"))
    gains = [(sym[me, fp, 0], sym[me, fp, 1]) for fp in range(per)]
    weight = jnp.where(lax.rem(lane, keep_x) == 0, 1.0, 2.0)
    zero = jnp.zeros((height, width), jnp.float32)
    held = [(zero, zero)] * per
    sizes_of = [jnp.zeros((1, LANES), jnp.float32)]
    corrections[0] = jnp.zeros((per, height, 2 * width), jnp.float32)
    for m in range(steps):
        size = None
        for fp in range(per):
            at = (fp * steps + m) * height
            re = held[fp][0] + fresh[at : at + height, :width]
            im = held[fp][1] + fresh[at : at + height, width:]
            gain_re, gain_im = gains[fp]
            re, im = gain_re * re - gain_im * im, gain_re * im + gain_im * re
            held[fp] = (re, im)
            corrections[m + 1, fp, :, :width] = re
            corrections[m + 1, fp, :, width:] = im
            square = re * re + im * im
            size = square if size is None else size + square
        sizes_of.append(jnp.sum(size * weight, axis=0, keepdims=True))
    back = times(
        jnp.concatenate([corrections[base + j, fp] for j in range(pair) for fp in range(per)], axis=0),
        entry("zi"),
    )
    column = jnp.sum(jnp.concatenate(sizes_of, axis=0), axis=1, keepdims=True)
    shape = (times_n, LANES)
    diagonal = lax.broadcasted_iota(jnp.int32, shape, 0) == lax.broadcasted_iota(jnp.int32, shape, 1)
    squares = jnp.sum(jnp.where(diagonal, column, 0.0), axis=0, keepdims=True) * (
        1.0 / (depth * spaces * rows * cols)
    )
    last = lax.broadcasted_iota(jnp.int32, (height, LANES), 0) == used
    for j in range(pair):
        for k in range(spaces):
            at = k * half
            tile, inside = at // LANES * LANES, at % LANES
            piece = joined(
                [
                    turned(
                        back[(j * per + fp) * height : (j * per + fp + 1) * height, tile : tile + LANES],
                        fp * half - inside,
                    )
                    for fp in range(per)
                ]
            )
            pieces[j * spaces + k] = jnp.where(last, squares, piece)

    def mode_copy(dj, dk):
        j, k = lax.rem(place + dj, pair), lax.rem(s + dk, spaces)
        return pltpu.make_async_remote_copy(
            src_ref=pieces.at[j * spaces + k],
            dst_ref=modes.at[me],
            send_sem=mode_send,
            recv_sem=mode_recv,
            device_id=(base + j, k),
            device_id_type=MESH,
        )

    sharers = [(dj, dk) for dj in reversed(range(pair)) for dk in reversed(range(spaces)) if dj + dk]
    for dj, dk in sharers:
        mode_copy(dj, dk).start()
    modes[me] = pieces[me]
    settle(late.at[parity], halo_recv.at[1, 1])
    settle(late.at[1 - parity], halo_recv.at[1, 0])
    sweep(finish_edge)
    settle(modes.at[pl.ds(0, owners - 1)], mode_recv)
    spectrum[...] = modes[...].reshape(owners * height, LANES)

    pl.when(n < times_n - 1)(lambda: settle(gathered.at[pl.ds(0, times_n * spaces - 1)], jump_send))

    @pl.when(n > 0)
    def _():
        ahead_copy.wait_send()

    for stage in range(4):
        settle(states[stage].at[:, pl.ds(0, 2), pl.ds(PAD, rows)], halo_send.at[stage])
    settle(modes.at[pl.ds(0, owners - 1)], mode_send)


def finish(
    sizes, places, fine, table, spectrum, out, slice_out, total_out, ends, slice_held, total_held, sems
):
    times_n, spaces, fields, depth, rows, cols = sizes
    keep_x = cols // 16
    slot = 2 * keep_x
    layers = fields * depth
    slots = LANES // slot
    groups, _, owners, _, used, height = layout(fields, depth, rows, cols, times_n, spaces)
    n = lax.axis_index("tm")
    lane = lax.broadcasted_iota(jnp.int32, (1, LANES), 1)
    found = spectrum[...]
    total = None
    for o in range(owners):
        row = found[o * height + used : o * height + used + 1]
        total = row if total is None else total + row
    cells = fields * depth * spaces * rows * cols

    def norm(values, count):
        return jnp.sqrt(jnp.sum(values, axis=1, keepdims=True) * (1.0 / count) + epsilon)

    slice_held[0] = norm(jnp.where(lane == n, total, 0.0), cells)[0, 0]
    total_held[0] = norm(total, cells * times_n)[0, 0]
    copies = [
        pltpu.make_async_copy(slice_held, slice_out, sems.at[0]),
        pltpu.make_async_copy(total_held, total_out, sems.at[1]),
    ]
    for copy in copies:
        copy.start()
    planes = under_deep(
        entry_of(table, places, "yi"), jnp.concatenate([found, swap(found, keep_x)], axis=0)
    )
    for g in range(groups):
        plane = planes[g * rows : (g + 1) * rows]
        count = min(slots, layers - g * slots) // 2
        shifted = [
            plane if p == 0 else pltpu.roll(plane, LANES - 2 * p * slot, 1) for p in range(count)
        ]
        fix = times_deep(jnp.concatenate(shifted, axis=0), entry_of(table, places, "xi"))
        for p in range(count):
            for i in range(2):
                l = g * slots + 2 * p + i
                ends[l] = fine[l] + fix[p * rows : (p + 1) * rows, i * cols : (i + 1) * cols]
        held = pl.ds(g * slots, 2 * count)
        copies.append(pltpu.make_async_copy(ends.at[held], out.at[held], sems.at[2 + g]))
        copies[-1].start()
    for copy in copies:
        copy.wait()


def solution(mesh):
    times_n, spaces = mesh.shape["tm"], mesh.shape["space"]

    def step(starts, source):
        _, fields, depth, rows, cols = starts.shape
        places, packed, gains = tables(fields, depth, rows, cols, times_n, spaces)
        constants = [packed, gains]
        operands = [starts, source] + [jnp.asarray(c) for c in constants]
        groups, _, owners, _, _, height = layout(fields, depth, rows, cols, times_n, spaces)
        slot = cols // 16 * 2
        per = LANES // (slot * depth)
        chunks = rows // CHUNK
        devices = times_n * spaces
        state = pltpu.VMEM((fields, depth + 2, rows + 2 * PAD, cols), jnp.float32)
        dma = pltpu.SemaphoreType.DMA
        layer_shape = (fields * depth, rows, cols)
        held = pl.pallas_call(
            functools.partial(kernel, (times_n, spaces, fields, depth, rows, cols), places),
            out_shape=(
                pltpu.VMEM(layer_shape, jnp.float32),
                pltpu.VMEM(packed.shape, jnp.bfloat16),
                pltpu.VMEM((owners * height, LANES), jnp.float32),
            ),
            in_specs=[pl.BlockSpec(memory_space=pltpu.HBM)] * (2 + len(constants)),
            out_specs=(pl.BlockSpec(memory_space=pltpu.VMEM),) * 3,
            scratch_shapes=[
                state, state, state, state,
                pltpu.VMEM((fields, depth, rows, cols), jnp.float32),
                pltpu.VMEM((2, fields, rows, cols), jnp.float32),
                pltpu.VMEM((2, fields, rows, cols), jnp.float32),
                pltpu.VMEM((groups + 1, rows, LANES), jnp.float32),
                pltpu.VMEM(gains.shape, jnp.float32),
                *[pltpu.VMEM((owners, height, LANES), jnp.float32)] * 3,
                pltpu.VMEM((devices, height, LANES), jnp.float32),
                pltpu.VMEM((times_n, per, height, depth * spaces * slot), jnp.float32),
                *[pltpu.VMEM((owners, height, LANES), jnp.float32)] * 2,
                dma((4,)), dma((2,)),
                dma((4,)), dma((2, 1 + chunks)), dma((2,)), dma, dma, dma, dma,
                pltpu.SemaphoreType.REGULAR(((times_n - 1).bit_length(), 2)),
            ],
            compiler_params=pltpu.CompilerParams(
                collective_id=0, has_side_effects=True, vmem_limit_bytes=VMEM_BYTES
            ),
        )(*[pltpu.with_memory_space_constraint(a, pltpu.HBM) for a in operands])
        out, slice_norm, total_norm = pl.pallas_call(
            functools.partial(finish, (times_n, spaces, fields, depth, rows, cols), places),
            out_shape=(
                jax.ShapeDtypeStruct(layer_shape, jnp.float32),
                jax.ShapeDtypeStruct((1,), jnp.float32),
                jax.ShapeDtypeStruct((1,), jnp.float32),
            ),
            in_specs=[pl.BlockSpec(memory_space=pltpu.VMEM)] * 3,
            out_specs=[pl.BlockSpec(memory_space=pltpu.HBM)] * 3,
            scratch_shapes=[
                pltpu.VMEM(layer_shape, jnp.float32),
                pltpu.SMEM((1,), jnp.float32), pltpu.SMEM((1,), jnp.float32), dma((2 + groups,)),
            ],
            compiler_params=pltpu.CompilerParams(vmem_limit_bytes=VMEM_BYTES // 2),
        )(*[pltpu.with_memory_space_constraint(a, pltpu.VMEM) for a in held])
        return out.reshape(starts.shape), slice_norm, total_norm

    return jax.shard_map(
        step,
        mesh=mesh,
        in_specs=(P("tm", None, "space", None, None), P(None, "space", None, None)),
        out_specs=(P("tm", None, "space", None, None), P("tm"), P()),
        check_vma=False,
    )
```

```python
import functools
import math

import jax
import jax.numpy as jnp
import numpy as np
from jax import lax
from jax.experimental import pallas as pl
from jax.experimental.pallas import tpu as pltpu
from jax.sharding import PartitionSpec as P

viscosity = 0.08
diffusivity = 0.05
compress_rate = 0.25
time_step = 0.5
diffusion_number = 0.08
advect_xaxis = 0.2
advect_yaxis = 0.15
advect_zaxis = 0.1
epsilon = 1e-06
MESH = pl.DeviceIdType.MESH
PAD = 8
CHUNK = 16
LANES = 128
SUBLANES = 8
PAIR = 2
VMEM_BYTES = 32 * 1024 * 1024


def layout(fields, depth, rows, cols, times_n, spaces):
    keep_y, keep_x = rows // 8, cols // 16
    groups = -(-fields * depth // (LANES // (2 * keep_x)))
    pair = PAIR if times_n % PAIR == 0 else 1
    owners = spaces * pair
    share = 2 * keep_y // owners
    used = groups * share
    height = -(-max(used + 1, used + share) // SUBLANES) * SUBLANES
    return groups, pair, owners, share, used, height


def tables(fields, depth, rows, cols, times_n, spaces):
    groups, pair, owners, share, used, height = layout(fields, depth, rows, cols, times_n, spaces)
    keep_y, keep_x = rows // 8, cols // 16
    slot = 2 * keep_x
    full = depth * spaces
    k = np.arange(keep_x)
    x = np.arange(cols)
    ax = 2 * math.pi / cols * ((x[:, None] * k[None, :]) % cols)
    weight = np.where(k == 0, 1.0, 2.0) / (full * rows * cols)
    xf = np.zeros((2 * cols, LANES))
    xi = np.zeros((LANES, 2 * cols))
    for i in range(2):
        at = i * slot
        xf[i * cols : (i + 1) * cols, at : at + keep_x] = np.cos(ax)
        xf[i * cols : (i + 1) * cols, at + keep_x : at + slot] = -np.sin(ax)
        xi[at : at + keep_x, i * cols : (i + 1) * cols] = (np.cos(ax) * weight).T
        xi[at + keep_x : at + slot, i * cols : (i + 1) * cols] = (-np.sin(ax) * weight).T
    ky = np.arange(2 * keep_y)
    ky = np.where(ky < keep_y, ky, ky - 2 * keep_y)
    y = np.arange(rows)
    ay = 2 * math.pi / rows * ((ky[:, None] * y[None, :]) % rows)
    kz = np.arange(full)
    width = full * keep_x
    block = owners * height
    yf = np.zeros((block, (groups + 1) * 2 * rows))
    yi = np.zeros((groups * rows, 2 * block))
    for g in range(groups + 1):
        for at in range(2 * keep_y):
            row = at // share * height + g * share + at % share
            yf[row, g * 2 * rows : (g + 1) * 2 * rows] = np.concatenate([np.cos(ay[at]), np.sin(ay[at])])
    for g in range(groups):
        for at in range(2 * keep_y):
            row = at // share * height + g * share + at % share
            yi[g * rows : (g + 1) * rows, row] = np.cos(ay[at])
            yi[g * rows : (g + 1) * rows, block + row] = -np.sin(ay[at])
    zf = np.zeros((full * slot, 2 * width))
    for z in range(full):
        a = 2 * math.pi / full * ((kz * z) % full)
        for kk in range(keep_x):
            row = z * slot + kk
            re = kz * keep_x + kk
            im = re + width
            zf[row, re] = np.cos(a)
            zf[row, im] = -np.sin(a)
            zf[row + keep_x, re] = np.sin(a)
            zf[row + keep_x, im] = np.cos(a)
    zi = np.zeros((2 * width, full * slot))
    for z in range(full):
        a = 2 * math.pi / full * ((kz * z) % full)
        for kk in range(keep_x):
            re = kz * keep_x + kk
            im = re + width
            col = z * slot + kk
            zi[re, col] = np.cos(a)
            zi[im, col] = -np.sin(a)
            zi[re, col + keep_x] = np.sin(a)
            zi[im, col + keep_x] = np.cos(a)
    tz = 2 * math.pi / full * kz
    ty = 2 * math.pi / rows * ky
    tx = 2 * math.pi / cols * k
    live = (ky != -keep_y).astype(np.float64)[:, None, None]
    real = 1.0 + diffusion_number * (
        (2 * np.cos(ty) - 2)[:, None, None]
        + (2 * np.cos(tz) - 2)[None, :, None]
        + (2 * np.cos(tx) - 2)[None, None, :]
    )
    imag = -(
        advect_yaxis * np.sin(ty)[:, None, None]
        + advect_zaxis * np.sin(tz)[None, :, None]
        + advect_xaxis * np.sin(tx)[None, None, :]
    )
    symbol = (real + 1j * imag) * live
    symbol = symbol.reshape(owners, share, width)
    per = LANES // (slot * depth)
    gains = np.zeros((owners, per, 2, height, width), np.float32)
    for f in range(fields):
        at = f // per * share
        gains[:, f % per, 0, at : at + share] = symbol.real
        gains[:, f % per, 1, at : at + share] = symbol.imag
    held = {
        "xf": halves(xf, 1), "yf": halves(yf, 1), "zf": halves(zf, 1), "zi": halves(zi, 1),
        "yi": halves(yi, 1, True), "xi": halves(xi, 0, True),
    }
    places, at, blocks = {}, 0, []
    for name, table in held.items():
        height, wide = table.shape
        places[name] = (at, height, wide // LANES)
        blocks += [table[:, i : i + LANES] for i in range(0, wide, LANES)]
        at += height * (wide // LANES)
    return places, np.concatenate(blocks, axis=0), gains


def halves(table, axis, twice=False):
    high = table.astype(jnp.bfloat16)
    low = (table - high.astype(np.float64)).astype(jnp.bfloat16)
    return np.concatenate([high, high, low] if twice else [high, low], axis=axis)


def split(values):
    high = values.astype(jnp.bfloat16)
    return high, (values - high.astype(jnp.float32)).astype(jnp.bfloat16)


def dot(a, b):
    return jnp.dot(a, b, preferred_element_type=jnp.float32)


def times(values, table):
    high, low = split(values)
    wide = table.shape[1] // 2
    if wide > LANES:
        stacked = dot(jnp.concatenate([high, low], axis=0), table[:, :wide])
        tall = values.shape[0]
        return stacked[:tall] + stacked[tall:] + dot(high, table[:, wide:])
    both = dot(high, table)
    return both[:, :wide] + dot(low, table[:, :wide]) + both[:, wide:]


def times_deep(values, table):
    high, low = split(values)
    deep = 2 * values.shape[1]
    return dot(jnp.concatenate([high, low], axis=1), table[:deep]) + dot(high, table[deep:])


def under(table, values):
    high, low = split(values)
    deep, wide = values.shape
    both = dot(table[:, :deep], jnp.concatenate([high, low], axis=1))
    return both[:, :wide] + both[:, wide:] + dot(table[:, deep:], high)


def under_deep(table, values):
    high, low = split(values)
    deep = 2 * values.shape[0]
    return dot(table[:, :deep], jnp.concatenate([high, low], axis=0)) + dot(table[:, deep:], high)


def entry_of(table, places, name):
    at, height, wide = places[name]
    return jnp.concatenate([table[pl.ds(at + i * height, height)] for i in range(wide)], axis=1)


def swap(values, keep_x):
    lane = lax.broadcasted_iota(jnp.int32, (1, LANES), 1)
    first = lax.rem(lane, 2 * keep_x) < keep_x
    return jnp.where(first, pltpu.roll(values, LANES - keep_x, 1), -pltpu.roll(values, keep_x, 1))


def kernel(
    sizes, places, starts, source, tables_h, sym_h,
    fine, table, spectrum,
    y1, y2, y3, y4, src, rims, late, begun, sym,
    own, jumps, ahead, gathered, corrections, pieces, modes,
    load_sem, table_sem, halo_send, halo_recv, ahead_sems, jump_send, jump_recv,
    mode_send, mode_recv, relays,
):
    times_n, spaces, fields, depth, rows, cols = sizes
    keep_y, keep_x = rows // 8, cols // 16
    slot = 2 * keep_x
    layers = fields * depth
    slots = LANES // slot
    per = LANES // (slot * depth)
    groups, pair, owners, share, used, height = layout(fields, depth, rows, cols, times_n, spaces)
    chunks = rows // CHUNK
    n = lax.axis_index("tm")
    s = lax.axis_index("space")
    place = lax.rem(n, pair)
    me = place * spaces + s
    base = n - place
    up = lax.rem(s + 1, spaces)
    down = lax.rem(s + spaces - 1, spaces)

    barrier = pltpu.get_barrier_semaphore()

    def near(distance, act):
        for side, target in enumerate((n - distance, n + distance)):
            pl.when((target >= 0) & (target < times_n))(functools.partial(act, side, target))

    def enter(target, where):
        pl.semaphore_signal(barrier, inc=1, device_id=(target, where), device_id_type=MESH)

    for offset in range(1, spaces):
        enter(n, lax.rem(s + offset, spaces))
    near(1, lambda side, target: enter(target, s))
    edges = [
        pltpu.make_async_copy(
            starts.at[0, :, z], y1.at[:, z + 1, pl.ds(PAD, rows)], load_sem.at[min(z, 1)]
        )
        for z in (0, depth - 1)
    ]
    for copy in edges:
        copy.start()
    loads = [
        pltpu.make_async_copy(
            starts.at[0, :, pl.ds(1, depth - 2)],
            y1.at[:, pl.ds(2, depth - 2), pl.ds(PAD, rows)],
            load_sem.at[2],
        ),
        pltpu.make_async_copy(tables_h, table, table_sem.at[0]),
        pltpu.make_async_copy(source, src, load_sem.at[3]),
        pltpu.make_async_copy(sym_h, sym, table_sem.at[1]),
    ]
    for copy in loads:
        copy.start()
    for copy in edges:
        copy.wait()
    beside = jnp.where(n > 0, 1, 0) + jnp.where(n < times_n - 1, 1, 0)
    pl.semaphore_wait(barrier, spaces - 1 + beside)

    def relay(level):
        near(
            2**level,
            lambda side, target: pl.semaphore_signal(
                relays.at[level, side], inc=1, device_id=(target, s), device_id_type=MESH
            ),
        )

    def heard(level):
        near(2**level, lambda side, target: pl.semaphore_wait(relays.at[level, 1 - side], 1))

    levels = (times_n - 1).bit_length()

    states = [y1, y2, y3, y4]

    parity = lax.rem(s, 2)
    far_to, near_to = jnp.where(parity == 0, down, up), jnp.where(parity == 0, up, down)
    far_z = jnp.where(parity == 0, 1, depth)
    near_z = depth + 1 - far_z
    step = 1 - 2 * parity
    far_halo, near_halo = far_z - step, near_z + step

    def settle(held, sem):
        pltpu.make_async_copy(held, held, sem).wait()

    def span(chunk):
        return pl.ds(pl.multiple_of(PAD + chunk * CHUNK, PAD), CHUNK)

    def send(src_ref, dst_ref, stage, index, target):
        pltpu.make_async_remote_copy(
            src_ref=src_ref,
            dst_ref=dst_ref,
            send_sem=halo_send.at[stage],
            recv_sem=halo_recv.at[stage % 2, index],
            device_id=(n, target),
            device_id_type=MESH,
        ).start()

    def send_near(stage):
        here, state = pl.ds(PAD, rows), states[stage]
        send(state.at[:, near_z, here], state.at[:, depth + 1 - near_halo, here], stage, 0, near_to)

    def send_far(stage, chunk):
        here, state = span(chunk), states[stage]
        send(
            state.at[:, far_z, here], state.at[:, depth + 1 - far_halo, here], stage, 1 + chunk, far_to
        )

    def send_first(c, carry):
        send_far(0, c)
        return carry

    lax.fori_loop(0, chunks, send_first, 0)
    send_near(0)
    relay(0)

    lane = lax.broadcasted_iota(jnp.int32, (1, LANES), 1)
    swapped = functools.partial(swap, keep_x=keep_x)

    entry = functools.partial(entry_of, table, places)

    def pack(pairs, result):
        stacked = jnp.concatenate(
            [jnp.concatenate([left, right], axis=1) for _, _, left, right in pairs], axis=0
        )
        packed = times(stacked, entry("xf"))
        result = list(result)
        for i, (g, at, _, _) in enumerate(pairs):
            tall = packed.shape[0] // len(pairs)
            piece = packed[i * tall : (i + 1) * tall]
            if not (isinstance(at, int) and at == 0):
                piece = pltpu.roll(piece, at * slot, 1)
            result[g] = piece if result[g] is None else result[g] + piece
        return result

    def transform(result):
        both = jnp.concatenate([part for t in result for part in (t, swapped(t))], axis=0)
        at, tall, wide = places["yf"]
        blocks = wide // 2
        held = len(result) * 2 * rows // LANES
        columns = [i * blocks + j for i in range(2) for j in range(held)]
        matrix = jnp.concatenate([table[pl.ds(at + i * tall, tall)] for i in columns], axis=1)
        return under(matrix, both).reshape(owners, height, LANES)

    def paired(layer_of, first_of, count):
        return [
            (f // per, f % per * depth + z, layer_of(f, z), layer_of(f, z + 1))
            for f in range(fields)
            for z in (first_of + i for i in range(0, count, 2))
        ]

    def rim_place(f):
        if f // per == groups - 1 and fields % per:
            return groups - 1, fields % per * depth
        return groups, f % per * depth + 2 * (f // per)

    loads[0].wait()
    loads[1].wait()
    def wrap(state, z):
        for f in range(fields):
            state[f, z, pl.ds(0, PAD)] = state[f, z, pl.ds(rows, PAD)]
            state[f, z, pl.ds(PAD + rows, PAD)] = state[f, z, pl.ds(PAD, PAD)]

    for z in range(1, depth + 1):
        wrap(y1, z)
    for f in range(fields):
        for z in (0, depth + 1):
            y4[f, z, pl.ds(PAD, rows)] = jnp.zeros((rows, cols), jnp.float32)

    own[...] = transform(
        pack(paired(lambda f, z: y1[f, z + 1, pl.ds(PAD, rows)], 0, depth), [None] * groups)
    )
    ahead_copy = pltpu.make_async_remote_copy(
        src_ref=own,
        dst_ref=ahead,
        send_sem=ahead_sems.at[0],
        recv_sem=ahead_sems.at[1],
        device_id=(jnp.maximum(n - 1, 0), s),
        device_id_type=MESH,
    )

    @pl.when(n > 0)
    def _():
        ahead_copy.start()

    shift = viscosity - diffusivity

    def reach(layer, sign):
        factor = (viscosity + sign * 0.5 * advect_zaxis) + (sign * 0.5) * layer[2]
        result = [factor * layer[f] for f in range(3)]
        result[2] = result[2] + (sign * 0.5) * layer[3]
        return result + [(sign * 0.5 * compress_rate) * layer[2], (factor - shift) * layer[4]]

    def weigh(stage):
        return time_step / 6.0 * (1.0, 2.0, 2.0, 1.0)[stage]

    loads[2].wait()
    loads[3].wait()

    def update(stage, z, r0, size=CHUNK):
        state = states[stage]
        mid, xm, xp, ym, yp = [], [], [], [], []
        rolled = size + 2 * PAD
        for f in range(fields):
            wide = state[f, z, pl.ds(r0, rolled)]
            centre = wide[PAD : PAD + size]
            mid.append(centre)
            ym.append(pltpu.roll(wide, 1, 0)[PAD : PAD + size])
            yp.append(pltpu.roll(wide, rolled - 1, 0)[PAD : PAD + size])
            xm.append(pltpu.roll(centre, 1, 1))
            xp.append(pltpu.roll(centre, cols - 1, 1))
        sides = [(xm, 0, 1.0, advect_xaxis), (xp, 0, -1.0, advect_xaxis)]
        sides += [(ym, 1, 1.0, advect_yaxis), (yp, 1, -1.0, advect_yaxis)]
        here = pl.ds(pl.multiple_of(r0 + PAD, PAD), size)
        for offset, sign in ((-1, 1.0), (1, -1.0)):
            held = [state[f, z + offset, here] for f in range(fields)]
            sides.append((held, 2, sign, advect_zaxis))
        factors = [
            (viscosity + sign * 0.5 * speed) + (sign * 0.5) * side[axis]
            for side, axis, sign, speed in sides
        ]
        rates = []
        for f in range(fields):
            forcing = src[f, z - 1, pl.ds(r0, size)]
            if f == 3:
                total = None
                for side, axis, sign, _ in sides:
                    if total is None:
                        total = side[axis]
                    else:
                        total = total + side[axis] if sign > 0 else total - side[axis]
                total = total * (0.5 * compress_rate)
            else:
                gain = viscosity if f < 3 else diffusivity
                total = (-6.0 * gain) * mid[f]
                push = None
                for factor, (side, axis, sign, _) in zip(factors, sides):
                    total = total + (factor if f < 3 else factor - shift) * side[f]
                    if axis == f:
                        term = (sign * 0.5) * side[3]
                        push = term if push is None else push + term
                if push is not None:
                    total = total + push
            rates.append(total + forcing)
        share_of = weigh(stage)
        for f in range(fields):
            at = f * depth + z - 1
            here = pl.ds(r0, size)
            begin = y1[f, z, pl.ds(pl.multiple_of(r0 + PAD, 8), size)]
            done = begin if stage == 0 else fine[at, here]
            fine[at, here] = done + share_of * rates[f]
            if stage < 3:
                later = states[stage + 1]
                step = (0.5, 0.5, 1.0)[stage] * time_step
                value = begin + step * rates[f]
                later[f, z, pl.ds(pl.multiple_of(r0 + PAD, 8), size)] = value

    def sweep(act, count=chunks):
        def body(c, carry):
            act(c, pl.multiple_of(c * CHUNK, CHUNK))
            return carry

        lax.fori_loop(0, count, body, 0)

    def rim(z, r0, size=CHUNK):
        side = jnp.where(z == depth, 1, 0)
        sign = jnp.where(z == depth, 1.0, -1.0)
        layer = [y4[f, z, pl.ds(pl.multiple_of(r0 + PAD, PAD), size)] for f in range(fields)]
        for f, value in enumerate(reach(layer, sign)):
            rims[side, f, pl.ds(r0, size)] = weigh(3) * value

    early = [near_z - step * k for k in range(depth - 2)]
    late_layers = [far_z, far_z + step]
    early_first = jnp.where(parity == 0, 2, 0)
    late_first = jnp.where(parity == 0, 0, depth - 2)

    def settled(f, z):
        return fine[f * depth + z]

    def remaining(r0, size):
        for z in late_layers:
            update(3, z, r0, size)
        rim(far_z, r0, size)

    def finish_rows(spans):
        def of(ref, *index):
            return jnp.concatenate([ref[*index, pl.ds(r0, size)] for r0, size in spans], axis=0)

        pairs = paired(lambda f, z: of(fine, f * depth + z), late_first, 2)
        pairs += [(*rim_place(f), of(rims, 1, f), of(rims, 0, f)) for f in range(fields)]
        result = pack(pairs, [of(begun, g) for g in range(groups)] + [None])
        for g in range(groups + 1):
            at = 0
            for r0, size in spans:
                begun[g, pl.ds(r0, size)] = result[g][at : at + size]
                at += size

    for stage in range(3):
        state = states[stage]

        def inner(c, r0):
            for z in range(2, depth):
                update(stage, z, r0)

        def edge(c, r0):
            settle(state.at[:, far_halo, span(c)], halo_recv.at[stage % 2, 1 + c])
            update(stage, far_z, r0)
            if stage < 2:
                send_far(stage + 1, c)
            else:
                pl.when(c >= 1)(lambda: remaining(pl.multiple_of(r0 - PAD, PAD), CHUNK))

        sweep(inner)
        for z in range(2, depth):
            wrap(states[stage + 1], z)
        settle(state.at[:, near_halo, pl.ds(PAD, rows)], halo_recv.at[stage % 2, 0])
        sweep(lambda c, r0: update(stage, near_z, r0))
        wrap(states[stage + 1], near_z)
        if stage < 2:
            send_near(stage + 1)
        else:

            def ready(c, r0):
                for z in early:
                    update(3, z, r0)
                rim(near_z, r0)

            sweep(ready)
            result = pack(paired(settled, early_first, depth - 2), [None] * groups)
            for g in range(groups):
                begun[g] = result[g]
        sweep(edge, chunks if stage < 2 else chunks - 1)
        if stage == 2:
            finish_rows([(PAD, rows - CHUNK - 2 * PAD)])
            edge(chunks - 1, rows - CHUNK)
        wrap(states[stage + 1], far_z)
        for level in range(levels):
            if min(level, 2) == stage:
                heard(level)
                if level + 1 < levels:
                    relay(level + 1)

    remaining(rows - PAD, PAD)
    remaining(0, PAD)
    finish_rows([(rows - CHUNK - PAD, CHUNK + PAD), (0, PAD)])
    spec = transform([begun[g] for g in range(groups + 1)])

    def jump_copy(index, tile, target):
        return pltpu.make_async_remote_copy(
            src_ref=jumps.at[tile],
            dst_ref=gathered.at[index],
            send_sem=jump_send,
            recv_sem=jump_recv,
            device_id=target,
            device_id_type=MESH,
        )

    def others(act):
        def body(dt, carry):
            t = n + dt
            t = jnp.where(t >= times_n, t - times_n, t)
            for ds in reversed(range(spaces)):
                where = s + ds
                where = jnp.where(where >= spaces, where - spaces, where)
                run = functools.partial(act, t, where)
                if ds == 0:
                    pl.when(dt > 0)(run)
                else:
                    run()
            return carry

        if times_n <= 8:
            for dt in sorted(range(times_n), key=lambda d: -min(d, times_n - d)):
                body(dt, 0)
        else:
            lax.fori_loop(0, times_n, body, 0)

    sent = lambda t, where: jump_copy(
        n * spaces + s, lax.rem(t, pair) * spaces + where, (t, where)
    )

    @pl.when(n < times_n - 1)
    def _():
        ahead_copy.wait_recv()
        jumps[...] = spec - ahead[...]
        others(lambda t, where: sent(t, where).start())
        gathered[n * spaces + s] = jumps[me]

    whole = pl.ds(PAD, rows)
    send(y4.at[:, far_z, whole], late.at[1 - parity], 3, 1, far_to)
    send(y4.at[:, near_z, whole], late.at[parity], 3, 0, near_to)

    def finish_edge(c, r0):
        here = pl.ds(r0, CHUNK)
        for side in range(2):
            layer = [late[side, f, here] for f in range(fields)]
            for f, value in enumerate(reach(layer, -1.0 if side else 1.0)):
                at = f * depth + side * (depth - 1)
                fine[at, here] = fine[at, here] + weigh(3) * value

    pl.when(n < times_n - 1)(
        lambda: settle(gathered.at[pl.ds(0, (times_n - 1) * spaces - 1)], jump_recv)
    )
    pl.when(n == times_n - 1)(lambda: settle(gathered.at[pl.ds(0, (times_n - 1) * spaces)], jump_recv))

    width = depth * spaces * keep_x
    half = depth * slot
    steps = times_n - 1
    part = lax.broadcasted_iota(jnp.int32, (1, LANES), 1) // half

    def turned(values, move):
        move = move % LANES
        return pltpu.roll(values, move, 1) if move else values

    def joined(blocks):
        total = None
        for i, block in enumerate(blocks):
            total = block if total is None else jnp.where(part == i, block, total)
        return total

    place_of = lax.rem(lax.broadcasted_iota(jnp.int32, (1, 1, LANES), 2), half) // slot
    line_of = lax.broadcasted_iota(jnp.int32, (1, height, 1), 1) // share
    raw = [
        jnp.stack([gathered[m * spaces + k] for m in range(steps)], axis=0) for k in range(spaces)
    ]

    def slid(values, move, axis):
        move = move % values.shape[axis]
        return pltpu.roll(values, move, axis) if move else values

    def rim_values(values):
        total = None
        for f in range(0, fields, per):
            g, at = rim_place(f)
            moved = slid(slid(values, -(at - f % per * depth) * slot, 2), (f // per - g) * share, 1)
            total = moved if total is None else jnp.where(line_of == f // per, moved, total)
        return total

    reached = [rim_values(values) for values in raw]
    slabs = []
    for k in range(spaces):
        from_below = jnp.where(place_of == 0, reached[(k - 1) % spaces], 0.0)
        from_above = slid(reached[(k + 1) % spaces], (depth - 2) * slot, 2)
        from_above = jnp.where(place_of == depth - 1, from_above, 0.0)
        slabs.append((raw[k] + (from_below + from_above)).reshape(steps * height, LANES))
    lined = [
        jnp.concatenate(
            [
                joined([turned(slabs[at + i], (i - fp) * half) for i in range(per)])
                for at in range(0, spaces, per)
            ],
            axis=1,
        )
        for fp in range(per)
    ]
    fresh = times(jnp.concatenate(lined, axis=0), entry("zf"))
    gains = [(sym[me, fp, 0], sym[me, fp, 1]) for fp in range(per)]
    weight = jnp.where(lax.rem(lane, keep_x) == 0, 1.0, 2.0)
    zero = jnp.zeros((height, width), jnp.float32)
    held = [(zero, zero)] * per
    sizes_of = [jnp.zeros((1, LANES), jnp.float32)]
    corrections[0] = jnp.zeros((per, height, 2 * width), jnp.float32)
    for m in range(steps):
        size = None
        for fp in range(per):
            at = (fp * steps + m) * height
            re = held[fp][0] + fresh[at : at + height, :width]
            im = held[fp][1] + fresh[at : at + height, width:]
            gain_re, gain_im = gains[fp]
            re, im = gain_re * re - gain_im * im, gain_re * im + gain_im * re
            held[fp] = (re, im)
            corrections[m + 1, fp, :, :width] = re
            corrections[m + 1, fp, :, width:] = im
            square = re * re + im * im
            size = square if size is None else size + square
        sizes_of.append(jnp.sum(size * weight, axis=0, keepdims=True))
    back = times(
        jnp.concatenate([corrections[base + j, fp] for j in range(pair) for fp in range(per)], axis=0),
        entry("zi"),
    )
    column = jnp.sum(jnp.concatenate(sizes_of, axis=0), axis=1, keepdims=True)
    shape = (times_n, LANES)
    diagonal = lax.broadcasted_iota(jnp.int32, shape, 0) == lax.broadcasted_iota(jnp.int32, shape, 1)
    squares = jnp.sum(jnp.where(diagonal, column, 0.0), axis=0, keepdims=True) * (
        1.0 / (depth * spaces * rows * cols)
    )
    last = lax.broadcasted_iota(jnp.int32, (height, LANES), 0) == used
    for j in range(pair):
        for k in range(spaces):
            at = k * half
            tile, inside = at // LANES * LANES, at % LANES
            piece = joined(
                [
                    turned(
                        back[(j * per + fp) * height : (j * per + fp + 1) * height, tile : tile + LANES],
                        fp * half - inside,
                    )
                    for fp in range(per)
                ]
            )
            pieces[j * spaces + k] = jnp.where(last, squares, piece)

    def mode_copy(dj, dk):
        j, k = lax.rem(place + dj, pair), lax.rem(s + dk, spaces)
        return pltpu.make_async_remote_copy(
            src_ref=pieces.at[j * spaces + k],
            dst_ref=modes.at[me],
            send_sem=mode_send,
            recv_sem=mode_recv,
            device_id=(base + j, k),
            device_id_type=MESH,
        )

    sharers = [(dj, dk) for dj in reversed(range(pair)) for dk in reversed(range(spaces)) if dj + dk]
    for dj, dk in sharers:
        mode_copy(dj, dk).start()
    modes[me] = pieces[me]
    settle(late.at[parity], halo_recv.at[1, 1])
    settle(late.at[1 - parity], halo_recv.at[1, 0])
    sweep(finish_edge)
    settle(modes.at[pl.ds(0, owners - 1)], mode_recv)
    spectrum[...] = modes[...].reshape(owners * height, LANES)

    pl.when(n < times_n - 1)(lambda: settle(gathered.at[pl.ds(0, times_n * spaces - 1)], jump_send))

    @pl.when(n > 0)
    def _():
        ahead_copy.wait_send()

    for stage in range(4):
        settle(states[stage].at[:, pl.ds(0, 2), pl.ds(PAD, rows)], halo_send.at[stage])
    settle(modes.at[pl.ds(0, owners - 1)], mode_send)


def finish(
    sizes, places, fine, table, spectrum, out, slice_out, total_out, ends, slice_held, total_held, sems
):
    times_n, spaces, fields, depth, rows, cols = sizes
    keep_x = cols // 16
    slot = 2 * keep_x
    layers = fields * depth
    slots = LANES // slot
    groups, _, owners, _, used, height = layout(fields, depth, rows, cols, times_n, spaces)
    n = lax.axis_index("tm")
    lane = lax.broadcasted_iota(jnp.int32, (1, LANES), 1)
    found = spectrum[...]
    total = None
    for o in range(owners):
        row = found[o * height + used : o * height + used + 1]
        total = row if total is None else total + row
    cells = fields * depth * spaces * rows * cols

    def norm(values, count):
        return jnp.sqrt(jnp.sum(values, axis=1, keepdims=True) * (1.0 / count) + epsilon)

    copies = []
    planes = under_deep(
        entry_of(table, places, "yi"), jnp.concatenate([found, swap(found, keep_x)], axis=0)
    )
    for g in range(groups):
        plane = planes[g * rows : (g + 1) * rows]
        count = min(slots, layers - g * slots) // 2
        shifted = [
            plane if p == 0 else pltpu.roll(plane, LANES - 2 * p * slot, 1) for p in range(count)
        ]
        fix = times_deep(jnp.concatenate(shifted, axis=0), entry_of(table, places, "xi"))
        for p in range(count):
            for i in range(2):
                l = g * slots + 2 * p + i
                ends[l] = fine[l] + fix[p * rows : (p + 1) * rows, i * cols : (i + 1) * cols]
        held = pl.ds(g * slots, 2 * count)
        copies.append(pltpu.make_async_copy(ends.at[held], out.at[held], sems.at[2 + g]))
        copies[-1].start()
        if g == 0:
            slice_held[0] = norm(jnp.where(lane == n, total, 0.0), cells)[0, 0]
            total_held[0] = norm(total, cells * times_n)[0, 0]
            small = [
                pltpu.make_async_copy(slice_held, slice_out, sems.at[0]),
                pltpu.make_async_copy(total_held, total_out, sems.at[1]),
            ]
            for copy in small:
                copy.start()
            copies += small
    for copy in copies:
        copy.wait()


def solution(mesh):
    times_n, spaces = mesh.shape["tm"], mesh.shape["space"]

    def step(starts, source):
        _, fields, depth, rows, cols = starts.shape
        places, packed, gains = tables(fields, depth, rows, cols, times_n, spaces)
        constants = [packed, gains]
        operands = [starts, source] + [jnp.asarray(c) for c in constants]
        groups, _, owners, _, _, height = layout(fields, depth, rows, cols, times_n, spaces)
        slot = cols // 16 * 2
        per = LANES // (slot * depth)
        chunks = rows // CHUNK
        devices = times_n * spaces
        state = pltpu.VMEM((fields, depth + 2, rows + 2 * PAD, cols), jnp.float32)
        dma = pltpu.SemaphoreType.DMA
        layer_shape = (fields * depth, rows, cols)
        held = pl.pallas_call(
            functools.partial(kernel, (times_n, spaces, fields, depth, rows, cols), places),
            out_shape=(
                pltpu.VMEM(layer_shape, jnp.float32),
                pltpu.VMEM(packed.shape, jnp.bfloat16),
                pltpu.VMEM((owners * height, LANES), jnp.float32),
            ),
            in_specs=[pl.BlockSpec(memory_space=pltpu.HBM)] * (2 + len(constants)),
            out_specs=(pl.BlockSpec(memory_space=pltpu.VMEM),) * 3,
            scratch_shapes=[
                state, state, state, state,
                pltpu.VMEM((fields, depth, rows, cols), jnp.float32),
                pltpu.VMEM((2, fields, rows, cols), jnp.float32),
                pltpu.VMEM((2, fields, rows, cols), jnp.float32),
                pltpu.VMEM((groups + 1, rows, LANES), jnp.float32),
                pltpu.VMEM(gains.shape, jnp.float32),
                *[pltpu.VMEM((owners, height, LANES), jnp.float32)] * 3,
                pltpu.VMEM((devices, height, LANES), jnp.float32),
                pltpu.VMEM((times_n, per, height, depth * spaces * slot), jnp.float32),
                *[pltpu.VMEM((owners, height, LANES), jnp.float32)] * 2,
                dma((4,)), dma((2,)),
                dma((4,)), dma((2, 1 + chunks)), dma((2,)), dma, dma, dma, dma,
                pltpu.SemaphoreType.REGULAR(((times_n - 1).bit_length(), 2)),
            ],
            compiler_params=pltpu.CompilerParams(
                collective_id=0, has_side_effects=True, vmem_limit_bytes=VMEM_BYTES
            ),
        )(*[pltpu.with_memory_space_constraint(a, pltpu.HBM) for a in operands])
        out, slice_norm, total_norm = pl.pallas_call(
            functools.partial(finish, (times_n, spaces, fields, depth, rows, cols), places),
            out_shape=(
                jax.ShapeDtypeStruct(layer_shape, jnp.float32),
                jax.ShapeDtypeStruct((1,), jnp.float32),
                jax.ShapeDtypeStruct((1,), jnp.float32),
            ),
            in_specs=[pl.BlockSpec(memory_space=pltpu.VMEM)] * 3,
            out_specs=[pl.BlockSpec(memory_space=pltpu.HBM)] * 3,
            scratch_shapes=[
                pltpu.VMEM(layer_shape, jnp.float32),
                pltpu.SMEM((1,), jnp.float32), pltpu.SMEM((1,), jnp.float32), dma((2 + groups,)),
            ],
            compiler_params=pltpu.CompilerParams(vmem_limit_bytes=VMEM_BYTES // 2),
        )(*[pltpu.with_memory_space_constraint(a, pltpu.VMEM) for a in held])
        return out.reshape(starts.shape), slice_norm, total_norm

    return jax.shard_map(
        step,
        mesh=mesh,
        in_specs=(P("tm", None, "space", None, None), P(None, "space", None, None)),
        out_specs=(P("tm", None, "space", None, None), P("tm"), P()),
        check_vma=False,
    )
```

```python
import functools
import math

import jax
import jax.numpy as jnp
import numpy as np
from jax import lax
from jax.experimental import pallas as pl
from jax.experimental.pallas import tpu as pltpu
from jax.sharding import PartitionSpec as P

viscosity = 0.08
diffusivity = 0.05
compress_rate = 0.25
time_step = 0.5
diffusion_number = 0.08
advect_xaxis = 0.2
advect_yaxis = 0.15
advect_zaxis = 0.1
epsilon = 1e-06
MESH = pl.DeviceIdType.MESH
PAD = 8
CHUNK = 16
LANES = 128
SUBLANES = 8
PAIR = 2
VMEM_BYTES = 32 * 1024 * 1024


def layout(fields, depth, rows, cols, times_n, spaces):
    keep_y, keep_x = rows // 8, cols // 16
    groups = -(-fields * depth // (LANES // (2 * keep_x)))
    pair = PAIR if times_n % PAIR == 0 else 1
    owners = spaces * pair
    share = 2 * keep_y // owners
    used = groups * share
    height = -(-max(used + 1, used + share) // SUBLANES) * SUBLANES
    return groups, pair, owners, share, used, height


def tables(fields, depth, rows, cols, times_n, spaces):
    groups, pair, owners, share, used, height = layout(fields, depth, rows, cols, times_n, spaces)
    keep_y, keep_x = rows // 8, cols // 16
    slot = 2 * keep_x
    full = depth * spaces
    k = np.arange(keep_x)
    x = np.arange(cols)
    ax = 2 * math.pi / cols * ((x[:, None] * k[None, :]) % cols)
    weight = np.where(k == 0, 1.0, 2.0) / (full * rows * cols)
    xf = np.zeros((2 * cols, LANES))
    xi = np.zeros((LANES, 2 * cols))
    for i in range(2):
        at = i * slot
        xf[i * cols : (i + 1) * cols, at : at + keep_x] = np.cos(ax)
        xf[i * cols : (i + 1) * cols, at + keep_x : at + slot] = -np.sin(ax)
        xi[at : at + keep_x, i * cols : (i + 1) * cols] = (np.cos(ax) * weight).T
        xi[at + keep_x : at + slot, i * cols : (i + 1) * cols] = (-np.sin(ax) * weight).T
    ky = np.arange(2 * keep_y)
    ky = np.where(ky < keep_y, ky, ky - 2 * keep_y)
    y = np.arange(rows)
    ay = 2 * math.pi / rows * ((ky[:, None] * y[None, :]) % rows)
    kz = np.arange(full)
    width = full * keep_x
    block = owners * height
    yf = np.zeros((block, (groups + 1) * 2 * rows))
    yi = np.zeros((groups * rows, 2 * block))
    for g in range(groups + 1):
        for at in range(2 * keep_y):
            row = at // share * height + g * share + at % share
            yf[row, g * 2 * rows : (g + 1) * 2 * rows] = np.concatenate([np.cos(ay[at]), np.sin(ay[at])])
    for g in range(groups):
        for at in range(2 * keep_y):
            row = at // share * height + g * share + at % share
            yi[g * rows : (g + 1) * rows, row] = np.cos(ay[at])
            yi[g * rows : (g + 1) * rows, block + row] = -np.sin(ay[at])
    zf = np.zeros((full * slot, 2 * width))
    for z in range(full):
        a = 2 * math.pi / full * ((kz * z) % full)
        for kk in range(keep_x):
            row = z * slot + kk
            re = kz * keep_x + kk
            im = re + width
            zf[row, re] = np.cos(a)
            zf[row, im] = -np.sin(a)
            zf[row + keep_x, re] = np.sin(a)
            zf[row + keep_x, im] = np.cos(a)
    zi = np.zeros((2 * width, full * slot))
    for z in range(full):
        a = 2 * math.pi / full * ((kz * z) % full)
        for kk in range(keep_x):
            re = kz * keep_x + kk
            im = re + width
            col = z * slot + kk
            zi[re, col] = np.cos(a)
            zi[im, col] = -np.sin(a)
            zi[re, col + keep_x] = np.sin(a)
            zi[im, col + keep_x] = np.cos(a)
    tz = 2 * math.pi / full * kz
    ty = 2 * math.pi / rows * ky
    tx = 2 * math.pi / cols * k
    live = (ky != -keep_y).astype(np.float64)[:, None, None]
    real = 1.0 + diffusion_number * (
        (2 * np.cos(ty) - 2)[:, None, None]
        + (2 * np.cos(tz) - 2)[None, :, None]
        + (2 * np.cos(tx) - 2)[None, None, :]
    )
    imag = -(
        advect_yaxis * np.sin(ty)[:, None, None]
        + advect_zaxis * np.sin(tz)[None, :, None]
        + advect_xaxis * np.sin(tx)[None, None, :]
    )
    symbol = (real + 1j * imag) * live
    symbol = symbol.reshape(owners, share, width)
    per = LANES // (slot * depth)
    gains = np.zeros((owners, per, 2, height, width), np.float32)
    for f in range(fields):
        at = f // per * share
        gains[:, f % per, 0, at : at + share] = symbol.real
        gains[:, f % per, 1, at : at + share] = symbol.imag
    held = {
        "xf": halves(xf, 1), "yf": halves(yf, 1), "zf": halves(zf, 1), "zi": halves(zi, 1),
        "yi": halves(yi, 1, True), "xi": halves(xi, 0, True),
    }
    places, at, blocks = {}, 0, []
    for name, table in held.items():
        height, wide = table.shape
        places[name] = (at, height, wide // LANES)
        blocks += [table[:, i : i + LANES] for i in range(0, wide, LANES)]
        at += height * (wide // LANES)
    return places, np.concatenate(blocks, axis=0), gains


def halves(table, axis, twice=False):
    high = table.astype(jnp.bfloat16)
    low = (table - high.astype(np.float64)).astype(jnp.bfloat16)
    return np.concatenate([high, high, low] if twice else [high, low], axis=axis)


def split(values):
    high = values.astype(jnp.bfloat16)
    return high, (values - high.astype(jnp.float32)).astype(jnp.bfloat16)


def dot(a, b):
    return jnp.dot(a, b, preferred_element_type=jnp.float32)


def times(values, table):
    high, low = split(values)
    wide = table.shape[1] // 2
    if wide > LANES:
        stacked = dot(jnp.concatenate([high, low], axis=0), table[:, :wide])
        tall = values.shape[0]
        return stacked[:tall] + stacked[tall:] + dot(high, table[:, wide:])
    both = dot(high, table)
    return both[:, :wide] + dot(low, table[:, :wide]) + both[:, wide:]


def times_deep(values, table):
    high, low = split(values)
    deep = 2 * values.shape[1]
    return dot(jnp.concatenate([high, low], axis=1), table[:deep]) + dot(high, table[deep:])


def under(table, values):
    high, low = split(values)
    deep, wide = values.shape
    both = dot(table[:, :deep], jnp.concatenate([high, low], axis=1))
    return both[:, :wide] + both[:, wide:] + dot(table[:, deep:], high)


def under_deep(table, values):
    high, low = split(values)
    deep = 2 * values.shape[0]
    return dot(table[:, :deep], jnp.concatenate([high, low], axis=0)) + dot(table[:, deep:], high)


def entry_of(table, places, name):
    at, height, wide = places[name]
    return jnp.concatenate([table[pl.ds(at + i * height, height)] for i in range(wide)], axis=1)


def swap(values, keep_x):
    lane = lax.broadcasted_iota(jnp.int32, (1, LANES), 1)
    first = lax.rem(lane, 2 * keep_x) < keep_x
    return jnp.where(first, pltpu.roll(values, LANES - keep_x, 1), -pltpu.roll(values, keep_x, 1))


def kernel(
    sizes, places, starts, source, tables_h, sym_h,
    fine, table, spectrum,
    y1, y2, y3, y4, src, rims, late, begun, sym,
    own, jumps, ahead, gathered, corrections, pieces, modes,
    load_sem, table_sem, halo_send, halo_recv, ahead_sems, jump_send, jump_recv,
    mode_send, mode_recv, relays,
):
    times_n, spaces, fields, depth, rows, cols = sizes
    keep_y, keep_x = rows // 8, cols // 16
    slot = 2 * keep_x
    layers = fields * depth
    slots = LANES // slot
    per = LANES // (slot * depth)
    groups, pair, owners, share, used, height = layout(fields, depth, rows, cols, times_n, spaces)
    chunks = rows // CHUNK
    n = lax.axis_index("tm")
    s = lax.axis_index("space")
    place = lax.rem(n, pair)
    me = place * spaces + s
    base = n - place
    up = lax.rem(s + 1, spaces)
    down = lax.rem(s + spaces - 1, spaces)

    barrier = pltpu.get_barrier_semaphore()

    def near(distance, act):
        for side, target in enumerate((n - distance, n + distance)):
            pl.when((target >= 0) & (target < times_n))(functools.partial(act, side, target))

    def enter(target, where):
        pl.semaphore_signal(barrier, inc=1, device_id=(target, where), device_id_type=MESH)

    for offset in range(1, spaces):
        enter(n, lax.rem(s + offset, spaces))
    enter(n + 1 - 2 * lax.rem(n, 2), s)
    near(2, lambda side, target: enter(target, s))
    edges = [
        pltpu.make_async_copy(
            starts.at[0, :, z], y1.at[:, z + 1, pl.ds(PAD, rows)], load_sem.at[min(z, 1)]
        )
        for z in (0, depth - 1)
    ]
    for copy in edges:
        copy.start()
    loads = [
        pltpu.make_async_copy(
            starts.at[0, :, pl.ds(1, depth - 2)],
            y1.at[:, pl.ds(2, depth - 2), pl.ds(PAD, rows)],
            load_sem.at[2],
        ),
        pltpu.make_async_copy(tables_h, table, table_sem.at[0]),
        pltpu.make_async_copy(source, src, load_sem.at[3]),
        pltpu.make_async_copy(sym_h, sym, table_sem.at[1]),
    ]
    for copy in loads:
        copy.start()
    for copy in edges:
        copy.wait()
    beside = jnp.where(n > 1, 1, 0) + jnp.where(n < times_n - 2, 1, 0)
    pl.semaphore_wait(barrier, spaces + beside)

    def relay(level):
        near(
            2**level,
            lambda side, target: pl.semaphore_signal(
                relays.at[level, side], inc=1, device_id=(target, s), device_id_type=MESH
            ),
        )

    def greet():
        pl.semaphore_signal(
            relays.at[0, 0], inc=1, device_id=(n + 1 - 2 * lax.rem(n, 2), s), device_id_type=MESH
        )

    def heard(level):
        near(2**level, lambda side, target: pl.semaphore_wait(relays.at[level, 1 - side], 1))

    levels = (times_n - 1).bit_length()

    states = [y1, y2, y3, y4]

    parity = lax.rem(s, 2)
    far_to, near_to = jnp.where(parity == 0, down, up), jnp.where(parity == 0, up, down)
    far_z = jnp.where(parity == 0, 1, depth)
    near_z = depth + 1 - far_z
    step = 1 - 2 * parity
    far_halo, near_halo = far_z - step, near_z + step

    def settle(held, sem):
        pltpu.make_async_copy(held, held, sem).wait()

    def span(chunk):
        return pl.ds(pl.multiple_of(PAD + chunk * CHUNK, PAD), CHUNK)

    def send(src_ref, dst_ref, stage, index, target):
        pltpu.make_async_remote_copy(
            src_ref=src_ref,
            dst_ref=dst_ref,
            send_sem=halo_send.at[stage],
            recv_sem=halo_recv.at[stage % 2, index],
            device_id=(n, target),
            device_id_type=MESH,
        ).start()

    def send_near(stage):
        here, state = pl.ds(PAD, rows), states[stage]
        send(state.at[:, near_z, here], state.at[:, depth + 1 - near_halo, here], stage, 0, near_to)

    def send_far(stage, chunk):
        here, state = span(chunk), states[stage]
        send(
            state.at[:, far_z, here], state.at[:, depth + 1 - far_halo, here], stage, 1 + chunk, far_to
        )

    def send_first(c, carry):
        send_far(0, c)
        return carry

    lax.fori_loop(0, chunks, send_first, 0)
    send_near(0)
    greet()

    lane = lax.broadcasted_iota(jnp.int32, (1, LANES), 1)
    swapped = functools.partial(swap, keep_x=keep_x)

    entry = functools.partial(entry_of, table, places)

    def pack(pairs, result):
        stacked = jnp.concatenate(
            [jnp.concatenate([left, right], axis=1) for _, _, left, right in pairs], axis=0
        )
        packed = times(stacked, entry("xf"))
        result = list(result)
        for i, (g, at, _, _) in enumerate(pairs):
            tall = packed.shape[0] // len(pairs)
            piece = packed[i * tall : (i + 1) * tall]
            if not (isinstance(at, int) and at == 0):
                piece = pltpu.roll(piece, at * slot, 1)
            result[g] = piece if result[g] is None else result[g] + piece
        return result

    def transform(result):
        both = jnp.concatenate([part for t in result for part in (t, swapped(t))], axis=0)
        at, tall, wide = places["yf"]
        blocks = wide // 2
        held = len(result) * 2 * rows // LANES
        columns = [i * blocks + j for i in range(2) for j in range(held)]
        matrix = jnp.concatenate([table[pl.ds(at + i * tall, tall)] for i in columns], axis=1)
        return under(matrix, both).reshape(owners, height, LANES)

    def paired(layer_of, first_of, count):
        return [
            (f // per, f % per * depth + z, layer_of(f, z), layer_of(f, z + 1))
            for f in range(fields)
            for z in (first_of + i for i in range(0, count, 2))
        ]

    def rim_place(f):
        if f // per == groups - 1 and fields % per:
            return groups - 1, fields % per * depth
        return groups, f % per * depth + 2 * (f // per)

    loads[0].wait()
    loads[1].wait()
    def wrap(state, z):
        for f in range(fields):
            state[f, z, pl.ds(0, PAD)] = state[f, z, pl.ds(rows, PAD)]
            state[f, z, pl.ds(PAD + rows, PAD)] = state[f, z, pl.ds(PAD, PAD)]

    for z in range(1, depth + 1):
        wrap(y1, z)
    for f in range(fields):
        for z in (0, depth + 1):
            y4[f, z, pl.ds(PAD, rows)] = jnp.zeros((rows, cols), jnp.float32)

    own[...] = transform(
        pack(paired(lambda f, z: y1[f, z + 1, pl.ds(PAD, rows)], 0, depth), [None] * groups)
    )
    ahead_copy = pltpu.make_async_remote_copy(
        src_ref=own,
        dst_ref=ahead,
        send_sem=ahead_sems.at[0],
        recv_sem=ahead_sems.at[1],
        device_id=(jnp.maximum(n - 1, 0), s),
        device_id_type=MESH,
    )


    shift = viscosity - diffusivity

    def reach(layer, sign):
        factor = (viscosity + sign * 0.5 * advect_zaxis) + (sign * 0.5) * layer[2]
        result = [factor * layer[f] for f in range(3)]
        result[2] = result[2] + (sign * 0.5) * layer[3]
        return result + [(sign * 0.5 * compress_rate) * layer[2], (factor - shift) * layer[4]]

    def weigh(stage):
        return time_step / 6.0 * (1.0, 2.0, 2.0, 1.0)[stage]

    loads[2].wait()
    loads[3].wait()

    def update(stage, z, r0, size=CHUNK):
        state = states[stage]
        mid, xm, xp, ym, yp = [], [], [], [], []
        rolled = size + 2 * PAD
        for f in range(fields):
            wide = state[f, z, pl.ds(r0, rolled)]
            centre = wide[PAD : PAD + size]
            mid.append(centre)
            ym.append(pltpu.roll(wide, 1, 0)[PAD : PAD + size])
            yp.append(pltpu.roll(wide, rolled - 1, 0)[PAD : PAD + size])
            xm.append(pltpu.roll(centre, 1, 1))
            xp.append(pltpu.roll(centre, cols - 1, 1))
        sides = [(xm, 0, 1.0, advect_xaxis), (xp, 0, -1.0, advect_xaxis)]
        sides += [(ym, 1, 1.0, advect_yaxis), (yp, 1, -1.0, advect_yaxis)]
        here = pl.ds(pl.multiple_of(r0 + PAD, PAD), size)
        for offset, sign in ((-1, 1.0), (1, -1.0)):
            held = [state[f, z + offset, here] for f in range(fields)]
            sides.append((held, 2, sign, advect_zaxis))
        factors = [
            (viscosity + sign * 0.5 * speed) + (sign * 0.5) * side[axis]
            for side, axis, sign, speed in sides
        ]
        rates = []
        for f in range(fields):
            forcing = src[f, z - 1, pl.ds(r0, size)]
            if f == 3:
                total = None
                for side, axis, sign, _ in sides:
                    if total is None:
                        total = side[axis]
                    else:
                        total = total + side[axis] if sign > 0 else total - side[axis]
                total = total * (0.5 * compress_rate)
            else:
                gain = viscosity if f < 3 else diffusivity
                total = (-6.0 * gain) * mid[f]
                push = None
                for factor, (side, axis, sign, _) in zip(factors, sides):
                    total = total + (factor if f < 3 else factor - shift) * side[f]
                    if axis == f:
                        term = (sign * 0.5) * side[3]
                        push = term if push is None else push + term
                if push is not None:
                    total = total + push
            rates.append(total + forcing)
        share_of = weigh(stage)
        for f in range(fields):
            at = f * depth + z - 1
            here = pl.ds(r0, size)
            begin = y1[f, z, pl.ds(pl.multiple_of(r0 + PAD, 8), size)]
            done = begin if stage == 0 else fine[at, here]
            fine[at, here] = done + share_of * rates[f]
            if stage < 3:
                later = states[stage + 1]
                step = (0.5, 0.5, 1.0)[stage] * time_step
                value = begin + step * rates[f]
                later[f, z, pl.ds(pl.multiple_of(r0 + PAD, 8), size)] = value

    def sweep(act, count=chunks):
        def body(c, carry):
            act(c, pl.multiple_of(c * CHUNK, CHUNK))
            return carry

        lax.fori_loop(0, count, body, 0)

    def rim(z, r0, size=CHUNK):
        side = jnp.where(z == depth, 1, 0)
        sign = jnp.where(z == depth, 1.0, -1.0)
        layer = [y4[f, z, pl.ds(pl.multiple_of(r0 + PAD, PAD), size)] for f in range(fields)]
        for f, value in enumerate(reach(layer, sign)):
            rims[side, f, pl.ds(r0, size)] = weigh(3) * value

    early = [near_z - step * k for k in range(depth - 2)]
    late_layers = [far_z, far_z + step]
    early_first = jnp.where(parity == 0, 2, 0)
    late_first = jnp.where(parity == 0, 0, depth - 2)

    def settled(f, z):
        return fine[f * depth + z]

    def remaining(r0, size):
        for z in late_layers:
            update(3, z, r0, size)
        rim(far_z, r0, size)

    def finish_rows(spans):
        def of(ref, *index):
            return jnp.concatenate([ref[*index, pl.ds(r0, size)] for r0, size in spans], axis=0)

        pairs = paired(lambda f, z: of(fine, f * depth + z), late_first, 2)
        pairs += [(*rim_place(f), of(rims, 1, f), of(rims, 0, f)) for f in range(fields)]
        result = pack(pairs, [of(begun, g) for g in range(groups)] + [None])
        for g in range(groups + 1):
            at = 0
            for r0, size in spans:
                begun[g, pl.ds(r0, size)] = result[g][at : at + size]
                at += size

    for stage in range(3):
        state = states[stage]

        def inner(c, r0):
            for z in range(2, depth):
                update(stage, z, r0)

        def edge(c, r0):
            settle(state.at[:, far_halo, span(c)], halo_recv.at[stage % 2, 1 + c])
            update(stage, far_z, r0)
            if stage < 2:
                send_far(stage + 1, c)
            else:
                pl.when(c >= 1)(lambda: remaining(pl.multiple_of(r0 - PAD, PAD), CHUNK))

        sweep(inner)
        for z in range(2, depth):
            wrap(states[stage + 1], z)
        settle(state.at[:, near_halo, pl.ds(PAD, rows)], halo_recv.at[stage % 2, 0])
        sweep(lambda c, r0: update(stage, near_z, r0))
        wrap(states[stage + 1], near_z)
        if stage < 2:
            send_near(stage + 1)
        else:

            def ready(c, r0):
                for z in early:
                    update(3, z, r0)
                rim(near_z, r0)

            sweep(ready)
            result = pack(paired(settled, early_first, depth - 2), [None] * groups)
            for g in range(groups):
                begun[g] = result[g]
        sweep(edge, chunks if stage < 2 else chunks - 1)
        if stage == 2:
            finish_rows([(PAD, rows - CHUNK - 2 * PAD)])
            edge(chunks - 1, rows - CHUNK)
        wrap(states[stage + 1], far_z)
        for level in range(levels):
            if min(level, 2) == stage:
                if level == 0:
                    pl.semaphore_wait(relays.at[0, 0], 1)
                else:
                    heard(level)
                if level + 1 < levels:
                    relay(level + 1)
        if stage == 1:
            pl.when(n > 0)(lambda: ahead_copy.start())

    remaining(rows - PAD, PAD)
    remaining(0, PAD)
    finish_rows([(rows - CHUNK - PAD, CHUNK + PAD), (0, PAD)])
    spec = transform([begun[g] for g in range(groups + 1)])

    def jump_copy(index, tile, target):
        return pltpu.make_async_remote_copy(
            src_ref=jumps.at[tile],
            dst_ref=gathered.at[index],
            send_sem=jump_send,
            recv_sem=jump_recv,
            device_id=target,
            device_id_type=MESH,
        )

    def others(act):
        def body(dt, carry):
            t = n + dt
            t = jnp.where(t >= times_n, t - times_n, t)
            for ds in reversed(range(spaces)):
                where = s + ds
                where = jnp.where(where >= spaces, where - spaces, where)
                run = functools.partial(act, t, where)
                if ds == 0:
                    pl.when(dt > 0)(run)
                else:
                    run()
            return carry

        if times_n <= 8:
            for dt in sorted(range(times_n), key=lambda d: -min(d, times_n - d)):
                body(dt, 0)
        else:
            lax.fori_loop(0, times_n, body, 0)

    sent = lambda t, where: jump_copy(
        n * spaces + s, lax.rem(t, pair) * spaces + where, (t, where)
    )

    @pl.when(n < times_n - 1)
    def _():
        ahead_copy.wait_recv()
        jumps[...] = spec - ahead[...]
        others(lambda t, where: sent(t, where).start())
        gathered[n * spaces + s] = jumps[me]

    whole = pl.ds(PAD, rows)
    send(y4.at[:, far_z, whole], late.at[1 - parity], 3, 1, far_to)
    send(y4.at[:, near_z, whole], late.at[parity], 3, 0, near_to)

    def finish_edge(c, r0):
        here = pl.ds(r0, CHUNK)
        for side in range(2):
            layer = [late[side, f, here] for f in range(fields)]
            for f, value in enumerate(reach(layer, -1.0 if side else 1.0)):
                at = f * depth + side * (depth - 1)
                fine[at, here] = fine[at, here] + weigh(3) * value

    pl.when(n < times_n - 1)(
        lambda: settle(gathered.at[pl.ds(0, (times_n - 1) * spaces - 1)], jump_recv)
    )
    pl.when(n == times_n - 1)(lambda: settle(gathered.at[pl.ds(0, (times_n - 1) * spaces)], jump_recv))

    width = depth * spaces * keep_x
    half = depth * slot
    steps = times_n - 1
    part = lax.broadcasted_iota(jnp.int32, (1, LANES), 1) // half

    def turned(values, move):
        move = move % LANES
        return pltpu.roll(values, move, 1) if move else values

    def joined(blocks):
        total = None
        for i, block in enumerate(blocks):
            total = block if total is None else jnp.where(part == i, block, total)
        return total

    place_of = lax.rem(lax.broadcasted_iota(jnp.int32, (1, 1, LANES), 2), half) // slot
    line_of = lax.broadcasted_iota(jnp.int32, (1, height, 1), 1) // share
    raw = [
        jnp.stack([gathered[m * spaces + k] for m in range(steps)], axis=0) for k in range(spaces)
    ]

    def slid(values, move, axis):
        move = move % values.shape[axis]
        return pltpu.roll(values, move, axis) if move else values

    def rim_values(values):
        total = None
        for f in range(0, fields, per):
            g, at = rim_place(f)
            moved = slid(slid(values, -(at - f % per * depth) * slot, 2), (f // per - g) * share, 1)
            total = moved if total is None else jnp.where(line_of == f // per, moved, total)
        return total

    reached = [rim_values(values) for values in raw]
    slabs = []
    for k in range(spaces):
        from_below = jnp.where(place_of == 0, reached[(k - 1) % spaces], 0.0)
        from_above = slid(reached[(k + 1) % spaces], (depth - 2) * slot, 2)
        from_above = jnp.where(place_of == depth - 1, from_above, 0.0)
        slabs.append((raw[k] + (from_below + from_above)).reshape(steps * height, LANES))
    lined = [
        jnp.concatenate(
            [
                joined([turned(slabs[at + i], (i - fp) * half) for i in range(per)])
                for at in range(0, spaces, per)
            ],
            axis=1,
        )
        for fp in range(per)
    ]
    fresh = times(jnp.concatenate(lined, axis=0), entry("zf"))
    gains = [(sym[me, fp, 0], sym[me, fp, 1]) for fp in range(per)]
    weight = jnp.where(lax.rem(lane, keep_x) == 0, 1.0, 2.0)
    zero = jnp.zeros((height, width), jnp.float32)
    held = [(zero, zero)] * per
    sizes_of = [jnp.zeros((1, LANES), jnp.float32)]
    corrections[0] = jnp.zeros((per, height, 2 * width), jnp.float32)
    for m in range(steps):
        size = None
        for fp in range(per):
            at = (fp * steps + m) * height
            re = held[fp][0] + fresh[at : at + height, :width]
            im = held[fp][1] + fresh[at : at + height, width:]
            gain_re, gain_im = gains[fp]
            re, im = gain_re * re - gain_im * im, gain_re * im + gain_im * re
            held[fp] = (re, im)
            corrections[m + 1, fp, :, :width] = re
            corrections[m + 1, fp, :, width:] = im
            square = re * re + im * im
            size = square if size is None else size + square
        sizes_of.append(jnp.sum(size * weight, axis=0, keepdims=True))
    back = times(
        jnp.concatenate([corrections[base + j, fp] for j in range(pair) for fp in range(per)], axis=0),
        entry("zi"),
    )
    column = jnp.sum(jnp.concatenate(sizes_of, axis=0), axis=1, keepdims=True)
    shape = (times_n, LANES)
    diagonal = lax.broadcasted_iota(jnp.int32, shape, 0) == lax.broadcasted_iota(jnp.int32, shape, 1)
    squares = jnp.sum(jnp.where(diagonal, column, 0.0), axis=0, keepdims=True) * (
        1.0 / (depth * spaces * rows * cols)
    )
    last = lax.broadcasted_iota(jnp.int32, (height, LANES), 0) == used
    for j in range(pair):
        for k in range(spaces):
            at = k * half
            tile, inside = at // LANES * LANES, at % LANES
            piece = joined(
                [
                    turned(
                        back[(j * per + fp) * height : (j * per + fp + 1) * height, tile : tile + LANES],
                        fp * half - inside,
                    )
                    for fp in range(per)
                ]
            )
            pieces[j * spaces + k] = jnp.where(last, squares, piece)

    def mode_copy(dj, dk):
        j, k = lax.rem(place + dj, pair), lax.rem(s + dk, spaces)
        return pltpu.make_async_remote_copy(
            src_ref=pieces.at[j * spaces + k],
            dst_ref=modes.at[me],
            send_sem=mode_send,
            recv_sem=mode_recv,
            device_id=(base + j, k),
            device_id_type=MESH,
        )

    sharers = [(dj, dk) for dj in reversed(range(pair)) for dk in reversed(range(spaces)) if dj + dk]
    for dj, dk in sharers:
        mode_copy(dj, dk).start()
    modes[me] = pieces[me]
    settle(late.at[parity], halo_recv.at[1, 1])
    settle(late.at[1 - parity], halo_recv.at[1, 0])
    sweep(finish_edge)
    settle(modes.at[pl.ds(0, owners - 1)], mode_recv)
    spectrum[...] = modes[...].reshape(owners * height, LANES)

    pl.when(n < times_n - 1)(lambda: settle(gathered.at[pl.ds(0, times_n * spaces - 1)], jump_send))

    @pl.when(n > 0)
    def _():
        ahead_copy.wait_send()

    for stage in range(4):
        settle(states[stage].at[:, pl.ds(0, 2), pl.ds(PAD, rows)], halo_send.at[stage])
    settle(modes.at[pl.ds(0, owners - 1)], mode_send)


def finish(
    sizes, places, fine, table, spectrum, out, slice_out, total_out, ends, slice_held, total_held, sems
):
    times_n, spaces, fields, depth, rows, cols = sizes
    keep_x = cols // 16
    slot = 2 * keep_x
    layers = fields * depth
    slots = LANES // slot
    groups, _, owners, _, used, height = layout(fields, depth, rows, cols, times_n, spaces)
    n = lax.axis_index("tm")
    lane = lax.broadcasted_iota(jnp.int32, (1, LANES), 1)
    found = spectrum[...]
    total = None
    for o in range(owners):
        row = found[o * height + used : o * height + used + 1]
        total = row if total is None else total + row
    cells = fields * depth * spaces * rows * cols

    def norm(values, count):
        return jnp.sqrt(jnp.sum(values, axis=1, keepdims=True) * (1.0 / count) + epsilon)

    copies = []
    planes = under_deep(
        entry_of(table, places, "yi"), jnp.concatenate([found, swap(found, keep_x)], axis=0)
    )
    for g in range(groups):
        plane = planes[g * rows : (g + 1) * rows]
        count = min(slots, layers - g * slots) // 2
        shifted = [
            plane if p == 0 else pltpu.roll(plane, LANES - 2 * p * slot, 1) for p in range(count)
        ]
        fix = times_deep(jnp.concatenate(shifted, axis=0), entry_of(table, places, "xi"))
        for p in range(count):
            for i in range(2):
                l = g * slots + 2 * p + i
                ends[l] = fine[l] + fix[p * rows : (p + 1) * rows, i * cols : (i + 1) * cols]
        held = pl.ds(g * slots, 2 * count)
        copies.append(pltpu.make_async_copy(ends.at[held], out.at[held], sems.at[2 + g]))
        copies[-1].start()
        if g == 0:
            slice_held[0] = norm(jnp.where(lane == n, total, 0.0), cells)[0, 0]
            total_held[0] = norm(total, cells * times_n)[0, 0]
            small = [
                pltpu.make_async_copy(slice_held, slice_out, sems.at[0]),
                pltpu.make_async_copy(total_held, total_out, sems.at[1]),
            ]
            for copy in small:
                copy.start()
            copies += small
    for copy in copies:
        copy.wait()


def solution(mesh):
    times_n, spaces = mesh.shape["tm"], mesh.shape["space"]

    def step(starts, source):
        _, fields, depth, rows, cols = starts.shape
        places, packed, gains = tables(fields, depth, rows, cols, times_n, spaces)
        constants = [packed, gains]
        operands = [starts, source] + [jnp.asarray(c) for c in constants]
        groups, _, owners, _, _, height = layout(fields, depth, rows, cols, times_n, spaces)
        slot = cols // 16 * 2
        per = LANES // (slot * depth)
        chunks = rows // CHUNK
        devices = times_n * spaces
        state = pltpu.VMEM((fields, depth + 2, rows + 2 * PAD, cols), jnp.float32)
        dma = pltpu.SemaphoreType.DMA
        layer_shape = (fields * depth, rows, cols)
        held = pl.pallas_call(
            functools.partial(kernel, (times_n, spaces, fields, depth, rows, cols), places),
            out_shape=(
                pltpu.VMEM(layer_shape, jnp.float32),
                pltpu.VMEM(packed.shape, jnp.bfloat16),
                pltpu.VMEM((owners * height, LANES), jnp.float32),
            ),
            in_specs=[pl.BlockSpec(memory_space=pltpu.HBM)] * (2 + len(constants)),
            out_specs=(pl.BlockSpec(memory_space=pltpu.VMEM),) * 3,
            scratch_shapes=[
                state, state, state, state,
                pltpu.VMEM((fields, depth, rows, cols), jnp.float32),
                pltpu.VMEM((2, fields, rows, cols), jnp.float32),
                pltpu.VMEM((2, fields, rows, cols), jnp.float32),
                pltpu.VMEM((groups + 1, rows, LANES), jnp.float32),
                pltpu.VMEM(gains.shape, jnp.float32),
                *[pltpu.VMEM((owners, height, LANES), jnp.float32)] * 3,
                pltpu.VMEM((devices, height, LANES), jnp.float32),
                pltpu.VMEM((times_n, per, height, depth * spaces * slot), jnp.float32),
                *[pltpu.VMEM((owners, height, LANES), jnp.float32)] * 2,
                dma((4,)), dma((2,)),
                dma((4,)), dma((2, 1 + chunks)), dma((2,)), dma, dma, dma, dma,
                pltpu.SemaphoreType.REGULAR(((times_n - 1).bit_length(), 2)),
            ],
            compiler_params=pltpu.CompilerParams(
                collective_id=0, has_side_effects=True, vmem_limit_bytes=VMEM_BYTES
            ),
        )(*[pltpu.with_memory_space_constraint(a, pltpu.HBM) for a in operands])
        out, slice_norm, total_norm = pl.pallas_call(
            functools.partial(finish, (times_n, spaces, fields, depth, rows, cols), places),
            out_shape=(
                jax.ShapeDtypeStruct(layer_shape, jnp.float32),
                jax.ShapeDtypeStruct((1,), jnp.float32),
                jax.ShapeDtypeStruct((1,), jnp.float32),
            ),
            in_specs=[pl.BlockSpec(memory_space=pltpu.VMEM)] * 3,
            out_specs=[pl.BlockSpec(memory_space=pltpu.HBM)] * 3,
            scratch_shapes=[
                pltpu.VMEM(layer_shape, jnp.float32),
                pltpu.SMEM((1,), jnp.float32), pltpu.SMEM((1,), jnp.float32), dma((2 + groups,)),
            ],
            compiler_params=pltpu.CompilerParams(vmem_limit_bytes=VMEM_BYTES // 2),
        )(*[pltpu.with_memory_space_constraint(a, pltpu.VMEM) for a in held])
        return out.reshape(starts.shape), slice_norm, total_norm

    return jax.shard_map(
        step,
        mesh=mesh,
        in_specs=(P("tm", None, "space", None, None), P(None, "space", None, None)),
        out_specs=(P("tm", None, "space", None, None), P("tm"), P()),
        check_vma=False,
    )
```

```python
import functools
import math

import jax
import jax.numpy as jnp
import numpy as np
from jax import lax
from jax.experimental import pallas as pl
from jax.experimental.pallas import tpu as pltpu
from jax.sharding import PartitionSpec as P

viscosity = 0.08
diffusivity = 0.05
compress_rate = 0.25
time_step = 0.5
diffusion_number = 0.08
advect_xaxis = 0.2
advect_yaxis = 0.15
advect_zaxis = 0.1
epsilon = 1e-06
MESH = pl.DeviceIdType.MESH
PAD = 8
CHUNK = 16
LANES = 128
SUBLANES = 8
PAIR = 2
VMEM_BYTES = 32 * 1024 * 1024


def layout(fields, depth, rows, cols, times_n, spaces):
    keep_y, keep_x = rows // 8, cols // 16
    groups = -(-fields * depth // (LANES // (2 * keep_x)))
    pair = PAIR if times_n % PAIR == 0 else 1
    owners = spaces * pair
    share = 2 * keep_y // owners
    used = groups * share
    height = -(-max(used + 1, used + share) // SUBLANES) * SUBLANES
    return groups, pair, owners, share, used, height


def tables(fields, depth, rows, cols, times_n, spaces):
    groups, pair, owners, share, used, height = layout(fields, depth, rows, cols, times_n, spaces)
    keep_y, keep_x = rows // 8, cols // 16
    slot = 2 * keep_x
    full = depth * spaces
    k = np.arange(keep_x)
    x = np.arange(cols)
    ax = 2 * math.pi / cols * ((x[:, None] * k[None, :]) % cols)
    weight = np.where(k == 0, 1.0, 2.0) / (full * rows * cols)
    xf = np.zeros((2 * cols, LANES))
    xi = np.zeros((LANES, 2 * cols))
    for i in range(2):
        at = i * slot
        xf[i * cols : (i + 1) * cols, at : at + keep_x] = np.cos(ax)
        xf[i * cols : (i + 1) * cols, at + keep_x : at + slot] = -np.sin(ax)
        xi[at : at + keep_x, i * cols : (i + 1) * cols] = (np.cos(ax) * weight).T
        xi[at + keep_x : at + slot, i * cols : (i + 1) * cols] = (-np.sin(ax) * weight).T
    ky = np.arange(2 * keep_y)
    ky = np.where(ky < keep_y, ky, ky - 2 * keep_y)
    y = np.arange(rows)
    ay = 2 * math.pi / rows * ((ky[:, None] * y[None, :]) % rows)
    kz = np.arange(full)
    width = full * keep_x
    block = owners * height
    yf = np.zeros((block, (groups + 1) * 2 * rows))
    yi = np.zeros((groups * rows, 2 * block))
    for g in range(groups + 1):
        for at in range(2 * keep_y):
            row = at // share * height + g * share + at % share
            yf[row, g * 2 * rows : (g + 1) * 2 * rows] = np.concatenate([np.cos(ay[at]), np.sin(ay[at])])
    for g in range(groups):
        for at in range(2 * keep_y):
            row = at // share * height + g * share + at % share
            yi[g * rows : (g + 1) * rows, row] = np.cos(ay[at])
            yi[g * rows : (g + 1) * rows, block + row] = -np.sin(ay[at])
    zf = np.zeros((full * slot, 2 * width))
    for z in range(full):
        a = 2 * math.pi / full * ((kz * z) % full)
        for kk in range(keep_x):
            row = z * slot + kk
            re = kz * keep_x + kk
            im = re + width
            zf[row, re] = np.cos(a)
            zf[row, im] = -np.sin(a)
            zf[row + keep_x, re] = np.sin(a)
            zf[row + keep_x, im] = np.cos(a)
    zi = np.zeros((2 * width, full * slot))
    for z in range(full):
        a = 2 * math.pi / full * ((kz * z) % full)
        for kk in range(keep_x):
            re = kz * keep_x + kk
            im = re + width
            col = z * slot + kk
            zi[re, col] = np.cos(a)
            zi[im, col] = -np.sin(a)
            zi[re, col + keep_x] = np.sin(a)
            zi[im, col + keep_x] = np.cos(a)
    tz = 2 * math.pi / full * kz
    ty = 2 * math.pi / rows * ky
    tx = 2 * math.pi / cols * k
    live = (ky != -keep_y).astype(np.float64)[:, None, None]
    real = 1.0 + diffusion_number * (
        (2 * np.cos(ty) - 2)[:, None, None]
        + (2 * np.cos(tz) - 2)[None, :, None]
        + (2 * np.cos(tx) - 2)[None, None, :]
    )
    imag = -(
        advect_yaxis * np.sin(ty)[:, None, None]
        + advect_zaxis * np.sin(tz)[None, :, None]
        + advect_xaxis * np.sin(tx)[None, None, :]
    )
    symbol = (real + 1j * imag) * live
    symbol = symbol.reshape(owners, share, width)
    per = LANES // (slot * depth)
    gains = np.zeros((owners, per, 2, height, width), np.float32)
    for f in range(fields):
        at = f // per * share
        gains[:, f % per, 0, at : at + share] = symbol.real
        gains[:, f % per, 1, at : at + share] = symbol.imag
    held = {
        "xf": halves(xf, 1), "yf": halves(yf, 1), "zf": halves(zf, 1), "zi": halves(zi, 1),
        "yi": halves(yi, 1, True), "xi": halves(xi, 0, True),
    }
    places, at, blocks = {}, 0, []
    for name, table in held.items():
        height, wide = table.shape
        places[name] = (at, height, wide // LANES)
        blocks += [table[:, i : i + LANES] for i in range(0, wide, LANES)]
        at += height * (wide // LANES)
    return places, np.concatenate(blocks, axis=0), gains


def halves(table, axis, twice=False):
    high = table.astype(jnp.bfloat16)
    low = (table - high.astype(np.float64)).astype(jnp.bfloat16)
    return np.concatenate([high, high, low] if twice else [high, low], axis=axis)


def split(values):
    high = values.astype(jnp.bfloat16)
    return high, (values - high.astype(jnp.float32)).astype(jnp.bfloat16)


def dot(a, b):
    return jnp.dot(a, b, preferred_element_type=jnp.float32)


def times(values, table):
    high, low = split(values)
    wide = table.shape[1] // 2
    if wide > LANES:
        stacked = dot(jnp.concatenate([high, low], axis=0), table[:, :wide])
        tall = values.shape[0]
        return stacked[:tall] + stacked[tall:] + dot(high, table[:, wide:])
    both = dot(high, table)
    return both[:, :wide] + dot(low, table[:, :wide]) + both[:, wide:]


def times_deep(values, table):
    high, low = split(values)
    deep = 2 * values.shape[1]
    return dot(jnp.concatenate([high, low], axis=1), table[:deep]) + dot(high, table[deep:])


def under(table, values):
    high, low = split(values)
    deep, wide = values.shape
    both = dot(table[:, :deep], jnp.concatenate([high, low], axis=1))
    return both[:, :wide] + both[:, wide:] + dot(table[:, deep:], high)


def under_deep(table, values):
    high, low = split(values)
    deep = 2 * values.shape[0]
    return dot(table[:, :deep], jnp.concatenate([high, low], axis=0)) + dot(table[:, deep:], high)


def entry_of(table, places, name):
    at, height, wide = places[name]
    return jnp.concatenate([table[pl.ds(at + i * height, height)] for i in range(wide)], axis=1)


def swap(values, keep_x):
    lane = lax.broadcasted_iota(jnp.int32, (1, LANES), 1)
    first = lax.rem(lane, 2 * keep_x) < keep_x
    return jnp.where(first, pltpu.roll(values, LANES - keep_x, 1), -pltpu.roll(values, keep_x, 1))


def kernel(
    sizes, places, starts, source, tables_h, sym_h,
    fine, table, spectrum,
    y1, y2, y3, y4, src, rims, late, begun, sym,
    own, jumps, ahead, gathered, corrections, pieces, modes,
    load_sem, table_sem, halo_send, halo_recv, ahead_sems, jump_send, jump_recv,
    mode_send, mode_recv, relays,
):
    times_n, spaces, fields, depth, rows, cols = sizes
    keep_y, keep_x = rows // 8, cols // 16
    slot = 2 * keep_x
    layers = fields * depth
    slots = LANES // slot
    per = LANES // (slot * depth)
    groups, pair, owners, share, used, height = layout(fields, depth, rows, cols, times_n, spaces)
    chunks = rows // CHUNK
    n = lax.axis_index("tm")
    s = lax.axis_index("space")
    place = lax.rem(n, pair)
    me = place * spaces + s
    base = n - place
    up = lax.rem(s + 1, spaces)
    down = lax.rem(s + spaces - 1, spaces)

    barrier = pltpu.get_barrier_semaphore()

    def near(distance, act):
        for side, target in enumerate((n - distance, n + distance)):
            pl.when((target >= 0) & (target < times_n))(functools.partial(act, side, target))

    def enter(target, where):
        pl.semaphore_signal(barrier, inc=1, device_id=(target, where), device_id_type=MESH)

    for offset in range(1, spaces):
        enter(n, lax.rem(s + offset, spaces))
    enter(n + 1 - 2 * lax.rem(n, 2), s)
    near(2, lambda side, target: enter(target, s))
    edges = [
        pltpu.make_async_copy(
            starts.at[0, :, z], y1.at[:, z + 1, pl.ds(PAD, rows)], load_sem.at[min(z, 1)]
        )
        for z in (0, depth - 1)
    ]
    for copy in edges:
        copy.start()
    loads = [
        pltpu.make_async_copy(
            starts.at[0, :, pl.ds(1, depth - 2)],
            y1.at[:, pl.ds(2, depth - 2), pl.ds(PAD, rows)],
            load_sem.at[2],
        ),
        pltpu.make_async_copy(tables_h, table, table_sem.at[0]),
        pltpu.make_async_copy(source, src, load_sem.at[3]),
        pltpu.make_async_copy(sym_h, sym, table_sem.at[1]),
    ]
    for copy in loads:
        copy.start()
    for copy in edges:
        copy.wait()
    beside = jnp.where(n > 1, 1, 0) + jnp.where(n < times_n - 2, 1, 0)
    pl.semaphore_wait(barrier, spaces + beside)

    def relay(level):
        near(
            2**level,
            lambda side, target: pl.semaphore_signal(
                relays.at[level, side], inc=1, device_id=(target, s), device_id_type=MESH
            ),
        )

    def greet():
        pl.semaphore_signal(
            relays.at[0, 0], inc=1, device_id=(n + 1 - 2 * lax.rem(n, 2), s), device_id_type=MESH
        )

    def heard(level):
        near(2**level, lambda side, target: pl.semaphore_wait(relays.at[level, 1 - side], 1))

    levels = (times_n - 1).bit_length()

    states = [y1, y2, y3, y4]

    parity = lax.rem(s, 2)
    far_to, near_to = jnp.where(parity == 0, down, up), jnp.where(parity == 0, up, down)
    far_z = jnp.where(parity == 0, 1, depth)
    near_z = depth + 1 - far_z
    step = 1 - 2 * parity
    far_halo, near_halo = far_z - step, near_z + step

    def settle(held, sem):
        pltpu.make_async_copy(held, held, sem).wait()

    def span(chunk):
        return pl.ds(pl.multiple_of(PAD + chunk * CHUNK, PAD), CHUNK)

    def send(src_ref, dst_ref, stage, index, target):
        pltpu.make_async_remote_copy(
            src_ref=src_ref,
            dst_ref=dst_ref,
            send_sem=halo_send.at[stage],
            recv_sem=halo_recv.at[stage % 2, index],
            device_id=(n, target),
            device_id_type=MESH,
        ).start()

    def send_near(stage):
        here, state = pl.ds(PAD, rows), states[stage]
        send(state.at[:, near_z, here], state.at[:, depth + 1 - near_halo, here], stage, 0, near_to)

    def send_far(stage, chunk):
        here, state = span(chunk), states[stage]
        send(
            state.at[:, far_z, here], state.at[:, depth + 1 - far_halo, here], stage, 1 + chunk, far_to
        )

    def send_first(c, carry):
        send_far(0, c)
        return carry

    lax.fori_loop(0, chunks, send_first, 0)
    send_near(0)
    greet()

    lane = lax.broadcasted_iota(jnp.int32, (1, LANES), 1)
    swapped = functools.partial(swap, keep_x=keep_x)

    entry = functools.partial(entry_of, table, places)

    def pack(pairs, result):
        stacked = jnp.concatenate(
            [jnp.concatenate([left, right], axis=1) for _, _, left, right in pairs], axis=0
        )
        packed = times(stacked, entry("xf"))
        result = list(result)
        for i, (g, at, _, _) in enumerate(pairs):
            tall = packed.shape[0] // len(pairs)
            piece = packed[i * tall : (i + 1) * tall]
            if not (isinstance(at, int) and at == 0):
                piece = pltpu.roll(piece, at * slot, 1)
            result[g] = piece if result[g] is None else result[g] + piece
        return result

    def transform(result):
        both = jnp.concatenate([part for t in result for part in (t, swapped(t))], axis=0)
        at, tall, wide = places["yf"]
        blocks = wide // 2
        held = len(result) * 2 * rows // LANES
        columns = [i * blocks + j for i in range(2) for j in range(held)]
        matrix = jnp.concatenate([table[pl.ds(at + i * tall, tall)] for i in columns], axis=1)
        return under(matrix, both).reshape(owners, height, LANES)

    def paired(layer_of, first_of, count):
        return [
            (f // per, f % per * depth + z, layer_of(f, z), layer_of(f, z + 1))
            for f in range(fields)
            for z in (first_of + i for i in range(0, count, 2))
        ]

    def rim_place(f):
        if f // per == groups - 1 and fields % per:
            return groups - 1, fields % per * depth
        return groups, f % per * depth + 2 * (f // per)

    loads[0].wait()
    loads[1].wait()
    def wrap(state, z):
        for f in range(fields):
            state[f, z, pl.ds(0, PAD)] = state[f, z, pl.ds(rows, PAD)]
            state[f, z, pl.ds(PAD + rows, PAD)] = state[f, z, pl.ds(PAD, PAD)]

    for z in range(1, depth + 1):
        wrap(y1, z)
    for f in range(fields):
        for z in (0, depth + 1):
            y4[f, z, pl.ds(PAD, rows)] = jnp.zeros((rows, cols), jnp.float32)

    own[...] = transform(
        pack(paired(lambda f, z: y1[f, z + 1, pl.ds(PAD, rows)], 0, depth), [None] * groups)
    )
    ahead_copy = pltpu.make_async_remote_copy(
        src_ref=own,
        dst_ref=ahead,
        send_sem=ahead_sems.at[0],
        recv_sem=ahead_sems.at[1],
        device_id=(jnp.maximum(n - 1, 0), s),
        device_id_type=MESH,
    )


    shift = viscosity - diffusivity

    def reach(layer, sign):
        factor = (viscosity + sign * 0.5 * advect_zaxis) + (sign * 0.5) * layer[2]
        result = [factor * layer[f] for f in range(3)]
        result[2] = result[2] + (sign * 0.5) * layer[3]
        return result + [(sign * 0.5 * compress_rate) * layer[2], (factor - shift) * layer[4]]

    def weigh(stage):
        return time_step / 6.0 * (1.0, 2.0, 2.0, 1.0)[stage]

    loads[2].wait()
    loads[3].wait()

    def update(stage, z, r0, size=CHUNK):
        state = states[stage]
        mid, xm, xp, ym, yp = [], [], [], [], []
        rolled = size + 2 * PAD
        for f in range(fields):
            wide = state[f, z, pl.ds(r0, rolled)]
            centre = wide[PAD : PAD + size]
            mid.append(centre)
            ym.append(pltpu.roll(wide, 1, 0)[PAD : PAD + size])
            yp.append(pltpu.roll(wide, rolled - 1, 0)[PAD : PAD + size])
            xm.append(pltpu.roll(centre, 1, 1))
            xp.append(pltpu.roll(centre, cols - 1, 1))
        sides = [(xm, 0, 1.0, advect_xaxis), (xp, 0, -1.0, advect_xaxis)]
        sides += [(ym, 1, 1.0, advect_yaxis), (yp, 1, -1.0, advect_yaxis)]
        here = pl.ds(pl.multiple_of(r0 + PAD, PAD), size)
        for offset, sign in ((-1, 1.0), (1, -1.0)):
            held = [state[f, z + offset, here] for f in range(fields)]
            sides.append((held, 2, sign, advect_zaxis))
        factors = [
            (viscosity + sign * 0.5 * speed) + (sign * 0.5) * side[axis]
            for side, axis, sign, speed in sides
        ]
        rates = []
        for f in range(fields):
            forcing = src[f, z - 1, pl.ds(r0, size)]
            if f == 3:
                total = None
                for side, axis, sign, _ in sides:
                    if total is None:
                        total = side[axis]
                    else:
                        total = total + side[axis] if sign > 0 else total - side[axis]
                total = total * (0.5 * compress_rate)
            else:
                gain = viscosity if f < 3 else diffusivity
                total = (-6.0 * gain) * mid[f]
                push = None
                for factor, (side, axis, sign, _) in zip(factors, sides):
                    total = total + (factor if f < 3 else factor - shift) * side[f]
                    if axis == f:
                        term = (sign * 0.5) * side[3]
                        push = term if push is None else push + term
                if push is not None:
                    total = total + push
            rates.append(total + forcing)
        share_of = weigh(stage)
        for f in range(fields):
            at = f * depth + z - 1
            here = pl.ds(r0, size)
            begin = y1[f, z, pl.ds(pl.multiple_of(r0 + PAD, 8), size)]
            done = begin if stage == 0 else fine[at, here]
            fine[at, here] = done + share_of * rates[f]
            if stage < 3:
                later = states[stage + 1]
                step = (0.5, 0.5, 1.0)[stage] * time_step
                value = begin + step * rates[f]
                later[f, z, pl.ds(pl.multiple_of(r0 + PAD, 8), size)] = value

    def sweep(act, count=chunks):
        def body(c, carry):
            act(c, pl.multiple_of(c * CHUNK, CHUNK))
            return carry

        lax.fori_loop(0, count, body, 0)

    def rim(z, r0, size=CHUNK):
        side = jnp.where(z == depth, 1, 0)
        sign = jnp.where(z == depth, 1.0, -1.0)
        layer = [y4[f, z, pl.ds(pl.multiple_of(r0 + PAD, PAD), size)] for f in range(fields)]
        for f, value in enumerate(reach(layer, sign)):
            rims[side, f, pl.ds(r0, size)] = weigh(3) * value

    early = [near_z - step * k for k in range(depth - 2)]
    late_layers = [far_z, far_z + step]
    early_first = jnp.where(parity == 0, 2, 0)
    late_first = jnp.where(parity == 0, 0, depth - 2)

    def settled(f, z):
        return fine[f * depth + z]

    def remaining(r0, size):
        for z in late_layers:
            update(3, z, r0, size)
        rim(far_z, r0, size)

    def finish_rows(spans):
        def of(ref, *index):
            return jnp.concatenate([ref[*index, pl.ds(r0, size)] for r0, size in spans], axis=0)

        pairs = paired(lambda f, z: of(fine, f * depth + z), late_first, 2)
        pairs += [(*rim_place(f), of(rims, 1, f), of(rims, 0, f)) for f in range(fields)]
        result = pack(pairs, [of(begun, g) for g in range(groups)] + [None])
        for g in range(groups + 1):
            at = 0
            for r0, size in spans:
                begun[g, pl.ds(r0, size)] = result[g][at : at + size]
                at += size

    for stage in range(3):
        state = states[stage]

        def inner(c, r0):
            for z in range(2, depth):
                update(stage, z, r0)

        def edge(c, r0):
            settle(state.at[:, far_halo, span(c)], halo_recv.at[stage % 2, 1 + c])
            update(stage, far_z, r0)
            if stage < 2:
                send_far(stage + 1, c)
            else:
                pl.when(c >= 1)(lambda: remaining(pl.multiple_of(r0 - PAD, PAD), CHUNK))

        sweep(inner)
        for z in range(2, depth):
            wrap(states[stage + 1], z)
        settle(state.at[:, near_halo, pl.ds(PAD, rows)], halo_recv.at[stage % 2, 0])
        sweep(lambda c, r0: update(stage, near_z, r0))
        wrap(states[stage + 1], near_z)
        if stage < 2:
            send_near(stage + 1)
        else:

            def ready(c, r0):
                for z in early:
                    update(3, z, r0)
                rim(near_z, r0)

            sweep(ready)
            result = pack(paired(settled, early_first, depth - 2), [None] * groups)
            for g in range(groups):
                begun[g] = result[g]
        for c in range(chunks if stage < 2 else chunks - 1):
            edge(c, c * CHUNK)
        if stage == 2:
            finish_rows([(PAD, rows - CHUNK - 2 * PAD)])
            edge(chunks - 1, rows - CHUNK)
        wrap(states[stage + 1], far_z)
        for level in range(levels):
            if min(level, 2) == stage:
                if level == 0:
                    pl.semaphore_wait(relays.at[0, 0], 1)
                else:
                    heard(level)
                if level + 1 < levels:
                    relay(level + 1)
        if stage == 1:
            pl.when(n > 0)(lambda: ahead_copy.start())

    remaining(rows - PAD, PAD)
    remaining(0, PAD)
    finish_rows([(rows - CHUNK - PAD, CHUNK + PAD), (0, PAD)])
    spec = transform([begun[g] for g in range(groups + 1)])

    def jump_copy(index, tile, target):
        return pltpu.make_async_remote_copy(
            src_ref=jumps.at[tile],
            dst_ref=gathered.at[index],
            send_sem=jump_send,
            recv_sem=jump_recv,
            device_id=target,
            device_id_type=MESH,
        )

    def others(act):
        def body(dt, carry):
            t = n + dt
            t = jnp.where(t >= times_n, t - times_n, t)
            for ds in reversed(range(spaces)):
                where = s + ds
                where = jnp.where(where >= spaces, where - spaces, where)
                run = functools.partial(act, t, where)
                if ds == 0:
                    pl.when(dt > 0)(run)
                else:
                    run()
            return carry

        if times_n <= 8:
            for dt in sorted(range(times_n), key=lambda d: -min(d, times_n - d)):
                body(dt, 0)
        else:
            lax.fori_loop(0, times_n, body, 0)

    sent = lambda t, where: jump_copy(
        n * spaces + s, lax.rem(t, pair) * spaces + where, (t, where)
    )

    @pl.when(n < times_n - 1)
    def _():
        ahead_copy.wait_recv()
        jumps[...] = spec - ahead[...]
        others(lambda t, where: sent(t, where).start())
        gathered[n * spaces + s] = jumps[me]

    whole = pl.ds(PAD, rows)
    send(y4.at[:, far_z, whole], late.at[1 - parity], 3, 1, far_to)
    send(y4.at[:, near_z, whole], late.at[parity], 3, 0, near_to)

    def finish_edge(c, r0):
        here = pl.ds(r0, CHUNK)
        for side in range(2):
            layer = [late[side, f, here] for f in range(fields)]
            for f, value in enumerate(reach(layer, -1.0 if side else 1.0)):
                at = f * depth + side * (depth - 1)
                fine[at, here] = fine[at, here] + weigh(3) * value

    pl.when(n < times_n - 1)(
        lambda: settle(gathered.at[pl.ds(0, (times_n - 1) * spaces - 1)], jump_recv)
    )
    pl.when(n == times_n - 1)(lambda: settle(gathered.at[pl.ds(0, (times_n - 1) * spaces)], jump_recv))

    width = depth * spaces * keep_x
    half = depth * slot
    steps = times_n - 1
    part = lax.broadcasted_iota(jnp.int32, (1, LANES), 1) // half

    def turned(values, move):
        move = move % LANES
        return pltpu.roll(values, move, 1) if move else values

    def joined(blocks):
        total = None
        for i, block in enumerate(blocks):
            total = block if total is None else jnp.where(part == i, block, total)
        return total

    place_of = lax.rem(lax.broadcasted_iota(jnp.int32, (1, 1, LANES), 2), half) // slot
    line_of = lax.broadcasted_iota(jnp.int32, (1, height, 1), 1) // share
    raw = [
        jnp.stack([gathered[m * spaces + k] for m in range(steps)], axis=0) for k in range(spaces)
    ]

    def slid(values, move, axis):
        move = move % values.shape[axis]
        return pltpu.roll(values, move, axis) if move else values

    def rim_values(values):
        total = None
        for f in range(0, fields, per):
            g, at = rim_place(f)
            moved = slid(slid(values, -(at - f % per * depth) * slot, 2), (f // per - g) * share, 1)
            total = moved if total is None else jnp.where(line_of == f // per, moved, total)
        return total

    reached = [rim_values(values) for values in raw]
    slabs = []
    for k in range(spaces):
        from_below = jnp.where(place_of == 0, reached[(k - 1) % spaces], 0.0)
        from_above = slid(reached[(k + 1) % spaces], (depth - 2) * slot, 2)
        from_above = jnp.where(place_of == depth - 1, from_above, 0.0)
        slabs.append((raw[k] + (from_below + from_above)).reshape(steps * height, LANES))
    lined = [
        jnp.concatenate(
            [
                joined([turned(slabs[at + i], (i - fp) * half) for i in range(per)])
                for at in range(0, spaces, per)
            ],
            axis=1,
        )
        for fp in range(per)
    ]
    fresh = times(jnp.concatenate(lined, axis=0), entry("zf"))
    gains = [(sym[me, fp, 0], sym[me, fp, 1]) for fp in range(per)]
    weight = jnp.where(lax.rem(lane, keep_x) == 0, 1.0, 2.0)
    zero = jnp.zeros((height, width), jnp.float32)
    held = [(zero, zero)] * per
    sizes_of = [jnp.zeros((1, LANES), jnp.float32)]
    corrections[0] = jnp.zeros((per, height, 2 * width), jnp.float32)
    for m in range(steps):
        size = None
        for fp in range(per):
            at = (fp * steps + m) * height
            re = held[fp][0] + fresh[at : at + height, :width]
            im = held[fp][1] + fresh[at : at + height, width:]
            gain_re, gain_im = gains[fp]
            re, im = gain_re * re - gain_im * im, gain_re * im + gain_im * re
            held[fp] = (re, im)
            corrections[m + 1, fp, :, :width] = re
            corrections[m + 1, fp, :, width:] = im
            square = re * re + im * im
            size = square if size is None else size + square
        sizes_of.append(jnp.sum(size * weight, axis=0, keepdims=True))
    back = times(
        jnp.concatenate([corrections[base + j, fp] for j in range(pair) for fp in range(per)], axis=0),
        entry("zi"),
    )
    column = jnp.sum(jnp.concatenate(sizes_of, axis=0), axis=1, keepdims=True)
    shape = (times_n, LANES)
    diagonal = lax.broadcasted_iota(jnp.int32, shape, 0) == lax.broadcasted_iota(jnp.int32, shape, 1)
    squares = jnp.sum(jnp.where(diagonal, column, 0.0), axis=0, keepdims=True) * (
        1.0 / (depth * spaces * rows * cols)
    )
    last = lax.broadcasted_iota(jnp.int32, (height, LANES), 0) == used
    for j in range(pair):
        for k in range(spaces):
            at = k * half
            tile, inside = at // LANES * LANES, at % LANES
            piece = joined(
                [
                    turned(
                        back[(j * per + fp) * height : (j * per + fp + 1) * height, tile : tile + LANES],
                        fp * half - inside,
                    )
                    for fp in range(per)
                ]
            )
            pieces[j * spaces + k] = jnp.where(last, squares, piece)

    def mode_copy(dj, dk):
        j, k = lax.rem(place + dj, pair), lax.rem(s + dk, spaces)
        return pltpu.make_async_remote_copy(
            src_ref=pieces.at[j * spaces + k],
            dst_ref=modes.at[me],
            send_sem=mode_send,
            recv_sem=mode_recv,
            device_id=(base + j, k),
            device_id_type=MESH,
        )

    sharers = [(dj, dk) for dj in reversed(range(pair)) for dk in reversed(range(spaces)) if dj + dk]
    for dj, dk in sharers:
        mode_copy(dj, dk).start()
    modes[me] = pieces[me]
    settle(late.at[parity], halo_recv.at[1, 1])
    settle(late.at[1 - parity], halo_recv.at[1, 0])
    sweep(finish_edge)
    settle(modes.at[pl.ds(0, owners - 1)], mode_recv)
    spectrum[...] = modes[...].reshape(owners * height, LANES)

    pl.when(n < times_n - 1)(lambda: settle(gathered.at[pl.ds(0, times_n * spaces - 1)], jump_send))

    @pl.when(n > 0)
    def _():
        ahead_copy.wait_send()

    for stage in range(4):
        settle(states[stage].at[:, pl.ds(0, 2), pl.ds(PAD, rows)], halo_send.at[stage])
    settle(modes.at[pl.ds(0, owners - 1)], mode_send)


def finish(
    sizes, places, fine, table, spectrum, out, slice_out, total_out, ends, slice_held, total_held, sems
):
    times_n, spaces, fields, depth, rows, cols = sizes
    keep_x = cols // 16
    slot = 2 * keep_x
    layers = fields * depth
    slots = LANES // slot
    groups, _, owners, _, used, height = layout(fields, depth, rows, cols, times_n, spaces)
    n = lax.axis_index("tm")
    lane = lax.broadcasted_iota(jnp.int32, (1, LANES), 1)
    found = spectrum[...]
    total = None
    for o in range(owners):
        row = found[o * height + used : o * height + used + 1]
        total = row if total is None else total + row
    cells = fields * depth * spaces * rows * cols

    def norm(values, count):
        return jnp.sqrt(jnp.sum(values, axis=1, keepdims=True) * (1.0 / count) + epsilon)

    copies = []
    planes = under_deep(
        entry_of(table, places, "yi"), jnp.concatenate([found, swap(found, keep_x)], axis=0)
    )
    for g in range(groups):
        plane = planes[g * rows : (g + 1) * rows]
        count = min(slots, layers - g * slots) // 2
        shifted = [
            plane if p == 0 else pltpu.roll(plane, LANES - 2 * p * slot, 1) for p in range(count)
        ]
        fix = times_deep(jnp.concatenate(shifted, axis=0), entry_of(table, places, "xi"))
        for p in range(count):
            for i in range(2):
                l = g * slots + 2 * p + i
                ends[l] = fine[l] + fix[p * rows : (p + 1) * rows, i * cols : (i + 1) * cols]
        held = pl.ds(g * slots, 2 * count)
        copies.append(pltpu.make_async_copy(ends.at[held], out.at[held], sems.at[2 + g]))
        copies[-1].start()
        if g == 0:
            slice_held[0] = norm(jnp.where(lane == n, total, 0.0), cells)[0, 0]
            total_held[0] = norm(total, cells * times_n)[0, 0]
            small = [
                pltpu.make_async_copy(slice_held, slice_out, sems.at[0]),
                pltpu.make_async_copy(total_held, total_out, sems.at[1]),
            ]
            for copy in small:
                copy.start()
            copies += small
    for copy in copies:
        copy.wait()


def solution(mesh):
    times_n, spaces = mesh.shape["tm"], mesh.shape["space"]

    def step(starts, source):
        _, fields, depth, rows, cols = starts.shape
        places, packed, gains = tables(fields, depth, rows, cols, times_n, spaces)
        constants = [packed, gains]
        operands = [starts, source] + [jnp.asarray(c) for c in constants]
        groups, _, owners, _, _, height = layout(fields, depth, rows, cols, times_n, spaces)
        slot = cols // 16 * 2
        per = LANES // (slot * depth)
        chunks = rows // CHUNK
        devices = times_n * spaces
        state = pltpu.VMEM((fields, depth + 2, rows + 2 * PAD, cols), jnp.float32)
        dma = pltpu.SemaphoreType.DMA
        layer_shape = (fields * depth, rows, cols)
        held = pl.pallas_call(
            functools.partial(kernel, (times_n, spaces, fields, depth, rows, cols), places),
            out_shape=(
                pltpu.VMEM(layer_shape, jnp.float32),
                pltpu.VMEM(packed.shape, jnp.bfloat16),
                pltpu.VMEM((owners * height, LANES), jnp.float32),
            ),
            in_specs=[pl.BlockSpec(memory_space=pltpu.HBM)] * (2 + len(constants)),
            out_specs=(pl.BlockSpec(memory_space=pltpu.VMEM),) * 3,
            scratch_shapes=[
                state, state, state, state,
                pltpu.VMEM((fields, depth, rows, cols), jnp.float32),
                pltpu.VMEM((2, fields, rows, cols), jnp.float32),
                pltpu.VMEM((2, fields, rows, cols), jnp.float32),
                pltpu.VMEM((groups + 1, rows, LANES), jnp.float32),
                pltpu.VMEM(gains.shape, jnp.float32),
                *[pltpu.VMEM((owners, height, LANES), jnp.float32)] * 3,
                pltpu.VMEM((devices, height, LANES), jnp.float32),
                pltpu.VMEM((times_n, per, height, depth * spaces * slot), jnp.float32),
                *[pltpu.VMEM((owners, height, LANES), jnp.float32)] * 2,
                dma((4,)), dma((2,)),
                dma((4,)), dma((2, 1 + chunks)), dma((2,)), dma, dma, dma, dma,
                pltpu.SemaphoreType.REGULAR(((times_n - 1).bit_length(), 2)),
            ],
            compiler_params=pltpu.CompilerParams(
                collective_id=0, has_side_effects=True, vmem_limit_bytes=VMEM_BYTES
            ),
        )(*[pltpu.with_memory_space_constraint(a, pltpu.HBM) for a in operands])
        out, slice_norm, total_norm = pl.pallas_call(
            functools.partial(finish, (times_n, spaces, fields, depth, rows, cols), places),
            out_shape=(
                jax.ShapeDtypeStruct(layer_shape, jnp.float32),
                jax.ShapeDtypeStruct((1,), jnp.float32),
                jax.ShapeDtypeStruct((1,), jnp.float32),
            ),
            in_specs=[pl.BlockSpec(memory_space=pltpu.VMEM)] * 3,
            out_specs=[pl.BlockSpec(memory_space=pltpu.HBM)] * 3,
            scratch_shapes=[
                pltpu.VMEM(layer_shape, jnp.float32),
                pltpu.SMEM((1,), jnp.float32), pltpu.SMEM((1,), jnp.float32), dma((2 + groups,)),
            ],
            compiler_params=pltpu.CompilerParams(vmem_limit_bytes=VMEM_BYTES // 2),
        )(*[pltpu.with_memory_space_constraint(a, pltpu.VMEM) for a in held])
        return out.reshape(starts.shape), slice_norm, total_norm

    return jax.shard_map(
        step,
        mesh=mesh,
        in_specs=(P("tm", None, "space", None, None), P(None, "space", None, None)),
        out_specs=(P("tm", None, "space", None, None), P("tm"), P()),
        check_vma=False,
    )
```
